32 devices in a mesh: seq: 16 (over z, y, core), fsdp: 2 (over x).
Axes of the slice: x: 2, y: 2, z: 4, core: 2. Of those that a mesh axis runs over, the one named last changes fastest.
Arguments:
- inputs: bfloat16 [2, 2048, 2048], P('fsdp', 'seq'), may hold values from -10 to 10
- routes: int32 [2, 2048, 8], P('fsdp', 'seq'), may hold values from 0 to 15, all different within a row; in each aligned block of 128 rows (0 to 127, 128 to 255, ..., all dimensions but the last counted through in order) at most 80 rows name the same one
- w_qkv: bfloat16 [2048, 6144], P(('seq', 'fsdp')), may hold values from -1 to 1
- w_out: bfloat16 [2048, 2048], P(('seq', 'fsdp')), may hold values from -0.375 to 0.375
- w_router: bfloat16 [2048, 16], P(('seq', 'fsdp')), may hold values from -2.5 to 2.5
- norm_gains: bfloat16 [2048, 4], P(('seq', 'fsdp')), may hold values from 0.5 to 1.5
- w_gate: bfloat16 [16, 2048, 1024], P('seq', None, 'fsdp'), may hold values from -0.125 to 0.125
- w_up: bfloat16 [16, 2048, 1024], P('seq', None, 'fsdp'), may hold values from -0.125 to 0.125
- w_down: bfloat16 [16, 2048, 1024], P('seq', None, 'fsdp'), may hold values from -0.75 to 0.75
- cotangent: bfloat16 [2, 2048, 2048], P('fsdp', 'seq'), may hold values from -6 to 6
Outputs:
- result: bfloat16 [2, 2048, 2048], P('fsdp', 'seq')
- grad_inputs: float32 [2, 2048, 2048], P('fsdp', 'seq')
- grad_qkv: float32 [2048, 6144], P(('seq', 'fsdp'))
- grad_proj: float32 [2048, 2048], P(('seq', 'fsdp'))
- grad_router: float32 [2048, 16], P(('seq', 'fsdp'))
- grad_gains: float32 [2048, 4], P(('seq', 'fsdp'))
- grad_gate: float32 [16, 2048, 1024], P('seq', None, 'fsdp')
- grad_up: float32 [16, 2048, 1024], P('seq', None, 'fsdp')
- grad_down: float32 [16, 2048, 1024], P('seq', None, 'fsdp')
The draws below stay inside these ranges and needn't reach their ends.
Inputs may be any that keep to these rules, and one draw needn't show every extreme that they name: `routes`: each row names 8 different experts. In the rows of one device (aligned blocks of 128 rows of a sequence) no expert is named by more than 80 rows, a bound that some block reaches.
All inputs are finite; a program needn't handle non-finite values.
Results may differ from the reference program's by a relative error of at most 0.024.
The reference program's roundings to bfloat16 on the way count: a program that leaves them out, or rounds other values in their place, can miss the bound.
Values may be sent and summed in bfloat16 or wider, within the bound.
A program may use at most 256 MiB of HBM per device.

```python
import math
from functools import partial
import jax
import jax.numpy as jnp
import numpy as np
from jax import lax

D = 2048
HEADS = 16
HDIM = 128
FF = 1024
TOPK = 8
TOK_DEV = 128
EXPERTS = 16
SEQLEN = 2048
SEQS = 2
CAP = 80
N_SEQ = 16


def draw_inputs(key, part):
    drawn_key = jax.random.fold_in(key, 1)
    return jax.random.truncated_normal(drawn_key, -6.0, 6.0, (SEQS, SEQLEN, D), jnp.float32).astype(jnp.bfloat16)


def draw_w_qkv(key, part):
    drawn_part = jax.random.truncated_normal(jax.random.fold_in(key, 11), -4.0, 4.0, (D, 3 * D), jnp.float32) / math.sqrt(D)
    return drawn_part.astype(jnp.bfloat16)


def draw_w_router(key, part):
    drawn_part = jax.random.truncated_normal(jax.random.fold_in(key, 21), -4.0, 4.0, (D, EXPERTS), jnp.float32) / math.sqrt(D // 8)
    return drawn_part.astype(jnp.bfloat16)


def draw_norm_gains(key, part):
    return (1.0 + 0.1 * jax.random.truncated_normal(jax.random.fold_in(key, 33), -5.0, 5.0, (D, 4), jnp.float32)).astype(jnp.bfloat16)


def with_spikes(array, key, source, target, shards_of, factor):
    owner, partner = [(jnp.arange(array.shape[axis_at]) // (array.shape[axis_at] // shards_of)).reshape([-1 if axis == axis_at else 1 for axis in range(array.ndim)]) for axis_at in (source, target)]
    chosen = jax.random.permutation(key, shards_of)[partner]
    strong = (owner == chosen) | (owner == (partner + shards_of // 2) % shards_of)
    return jnp.where(strong, factor * array, array)


def level_of(stream_key, extent, shards, smallest, high):
    factor_of, own = 1.0, jax.random.fold_in(stream_key, 6)
    for position, blocks in shards:
        draws = jnp.exp(jax.random.uniform(jax.random.fold_in(own, position), (blocks,), jnp.float32, smallest / len(shards), high / len(shards)))
        factor_of = factor_of * jnp.repeat(draws, extent[position] // blocks).reshape([-1 if axis == position else 1 for axis in range(len(extent))])
    return factor_of


def shared_out(rng, own, number, rows, amount, top, reach, skew):
    ranking = jax.random.permutation(rng, amount)
    heavy_load, common = portions_of(amount, rows * top, reach, skew, True), portions_of(amount, rows * top, reach, skew, False)
    places = jnp.arange(amount)

    def named(tallies, offset_by):
        used = int((tallies > 0).sum())
        fixed = max(1, used // 4)
        passed = fixed + (places - fixed + offset_by * (used - fixed)) % max(1, amount - fixed)
        return jnp.zeros((amount,), jnp.int32).at[ranking[jnp.where(places < fixed, places, passed)]].set(jnp.asarray(tallies, jnp.int32))

    tallies = jnp.where(number % 4 == 0, named(heavy_load, number // 4), named(common, number - number // 4 - 1))
    mixed = jax.random.permutation(jax.random.fold_in(own, 3), amount)
    source_of, taker = mixed[0:amount // 2 * 2:2], mixed[1:amount // 2 * 2:2]
    margin = jnp.minimum(tallies[source_of] - 1, reach - tallies[taker]) // 2
    margin = jnp.where((source_of == ranking[0]) | (taker == ranking[0]) | (tallies[taker] == 0), 0, jnp.maximum(margin, 0))
    passed = jax.random.randint(jax.random.fold_in(own, 4), (amount // 2,), 0, 1 << 20) % (margin + 1)
    tallies = tallies.at[source_of].add(-passed).at[taker].add(passed)
    labels = jnp.searchsorted(jnp.cumsum(tallies), jnp.arange(rows * top), side="right").astype(jnp.int32)
    listing = labels.reshape(top, rows).T
    listing = listing[jax.random.permutation(jax.random.fold_in(own, 1), rows)]
    offset_by = jax.random.randint(jax.random.fold_in(own, 2), (rows, 1), 0, top)
    return jnp.take_along_axis(listing, (jnp.arange(top)[None, :] + offset_by) % top, axis=1)


def portions_of(number_of, total, most, lean, full):
    weights = [(1 << 20) // math.isqrt(grade ** lean) + 1 for grade in range(1, number_of + 1)]
    largest = most if full else min(most, max(-(-total // number_of), total * weights[0] // sum(weights)))
    least = 1 if total - largest >= number_of - 1 else 0
    counts, surplus = [largest] + [least] * (number_of - 1), total - largest - least * (number_of - 1)
    while surplus > 0:
        candidates = [i for i in range(1, number_of) if counts[i] < largest] or [i for i in range(1, number_of) if counts[i] < most]
        whole, remaining = sum([weights[i] for i in candidates]), surplus
        for i in candidates:
            extra = min(most - counts[i], max(1, remaining * weights[i] // whole), surplus)
            counts[i] = counts[i] + extra
            surplus = surplus - extra
    return np.array(counts)


def centred(rng, shape, scale, reach, cuts=(), kind=jnp.bfloat16):
    level = level_of(rng, shape, cuts, -0.22, 0.18) if cuts else 1.0
    drawn = jax.random.normal(rng, shape, jnp.float32) * scale * level
    return jnp.minimum(jnp.maximum(drawn, -reach), reach).astype(kind)


def heavy_noise(rng, shape, scale, most, pieces, heavy, held_as=jnp.bfloat16):
    array = scale * jax.random.normal(rng, shape, jnp.float32)
    if pieces:
        array = array * level_of(rng, shape, pieces, -0.22, 0.18)
    return jnp.clip(with_spikes(array, jax.random.fold_in(rng, 3), *heavy), -most, most).astype(held_as)


def setup_inputs(seed: int = 0) -> dict:
    arg_keys = jax.random.split(jax.random.key(seed), 11)
    inputs = draw_inputs(jax.random.fold_in(arg_keys[10], 71), 0)
    routes_keys = jax.random.split(jax.random.fold_in(arg_keys[1], 1), SEQS * SEQLEN // TOK_DEV)
    routes_turns = jax.random.permutation(jax.random.fold_in(arg_keys[1], 3), SEQS * SEQLEN // TOK_DEV)
    routes = jax.vmap(lambda own, number: shared_out(jax.random.fold_in(arg_keys[1], 2), own, number, TOK_DEV, EXPERTS, TOPK, CAP, 1))(routes_keys, routes_turns).reshape((SEQS, SEQLEN, TOPK))
    w_qkv = draw_w_qkv(jax.random.fold_in(arg_keys[10], 71), 0)
    w_out = centred(arg_keys[3], (D, D), (D // 8) ** -0.5, 0.375, ((0, 32),))
    w_router = draw_w_router(jax.random.fold_in(arg_keys[10], 71), 0)
    norm_gains = draw_norm_gains(jax.random.fold_in(arg_keys[10], 71), 0)
    w_gate = centred(arg_keys[6], (EXPERTS, D, FF), D ** -0.5, 0.125, ((0, 16), (2, 2)))
    w_up = centred(arg_keys[7], (EXPERTS, D, FF), D ** -0.5, 0.125, ((0, 16), (2, 2)))
    w_down = centred(arg_keys[8], (EXPERTS, D, FF), (FF // 16) ** -0.5, 0.75, ((0, 16), (2, 2)))
    cotangent = heavy_noise(arg_keys[9], (SEQS, SEQLEN, D), 1.0, 6.0, ((0, 2), (1, 16)), (1, 2, 16, 2.0))
    return {"inputs": inputs, "routes": routes, "w_qkv": w_qkv, "w_out": w_out, "w_router": w_router, "norm_gains": norm_gains, "w_gate": w_gate, "w_up": w_up, "w_down": w_down, "cotangent": cotangent}


EPS = 1e-05
NEG = -1e+30
HIGH = lax.Precision.HIGHEST

@jax.custom_vjp
def low(v):
    return lax.optimization_barrier(v.astype(jnp.bfloat16)).astype(jnp.float32)

@jax.custom_vjp
def low_back(v):
    return v

def low_keep(v):
    return (low(v), None)

def low_pass(kept, grad):
    return (grad,)

def back_keep(v):
    return (v, None)

def back_low(kept, grad):
    return (low(grad),)
low.defvjp(low_keep, low_pass)
low_back.defvjp(back_keep, back_low)

def normalize(values, gain):
    return values * lax.rsqrt(lax.optimization_barrier(jnp.mean(values * values, -1, keepdims=True)) + EPS) * gain

def rotate(values, positions):
    half = values.shape[-1] // 2
    freqs = 10000.0 ** (-jnp.arange(half, dtype=jnp.float32) / half)
    angles = positions.astype(jnp.float32)[:, None] * freqs[None, :]
    cosine = jnp.concatenate([jnp.cos(angles), jnp.cos(angles)], -1)[:, None, :]
    sine = jnp.concatenate([jnp.sin(angles), jnp.sin(angles)], -1)[:, None, :]
    turned = jnp.concatenate([-values[..., half:], values[..., :half]], -1)
    return values * cosine + turned * sine

def prepare(mixed, gain_query, gain_key, positions):
    width = gain_query.shape[0]
    shaped = (mixed.shape[0], HEADS, width // HEADS)
    queries = normalize(mixed[:, :width], gain_query).reshape(shaped)
    key_rows = normalize(mixed[:, width:2 * width], gain_key).reshape(shaped)
    value_rows = mixed[:, 2 * width:].reshape(shaped)
    return (rotate(queries, positions), rotate(key_rows, positions), value_rows)

def route_weights(logits, routes):
    top = lax.optimization_barrier(jnp.max(logits, -1, keepdims=True))
    expd = jnp.exp(logits - top)
    probs = expd / lax.optimization_barrier(jnp.sum(expd, -1, keepdims=True))
    return jnp.take_along_axis(probs, routes, 1)

def arrange(block_routes, experts, capacity):
    flat = block_routes.reshape(-1)
    onehot = (flat[:, None] == jnp.arange(experts, dtype=jnp.int32)[None, :]).astype(jnp.int32)
    before = jnp.cumsum(onehot, 0) - onehot
    places = lax.optimization_barrier(jnp.sum(before * onehot, 1))
    slot = (flat * capacity + places).astype(jnp.int32)
    entries = flat.shape[0]
    entry = jnp.zeros((experts * capacity,), jnp.int32).at[slot].set(jnp.arange(entries, dtype=jnp.int32))
    filled = jnp.zeros((experts * capacity,), jnp.int32).at[slot].set(1)
    return (slot, entry, filled)

def pick_rows(table, index):
    return table[index]

def attention(queries, key_rows, value_rows):
    length = queries.shape[0]
    block = min(512, length)
    factor = HDIM ** (-0.5)

    def one_block(index):
        start = index * block
        part = lax.dynamic_slice_in_dim(queries, start, block, 0)
        scores = jnp.einsum('qhd,khd->hqk', part, key_rows, precision=HIGH) * factor
        scores = low_back(scores)
        query_pos = start + jnp.arange(block, dtype=jnp.int32)
        allowed = jnp.arange(length, dtype=jnp.int32)[None, :] <= query_pos[:, None]
        scores = jnp.where(allowed[None], scores, NEG)
        top = lax.optimization_barrier(jnp.max(scores, -1, keepdims=True))
        expd = jnp.exp(scores - top)
        probs = low(expd / lax.optimization_barrier(jnp.sum(expd, -1, keepdims=True)))
        return jnp.einsum('hqk,khd->qhd', probs, value_rows, precision=HIGH)
    blocks = lax.map(jax.checkpoint(one_block), jnp.arange(length // block, dtype=jnp.int32))
    return blocks.reshape(queries.shape)

def one_sequence(params, sequence, seq_routes, slot, entry, filled):
    w_qkv, w_out, w_router, norm_gains, w_gate, w_up, w_down = params
    length = sequence.shape[0]
    width = sequence.shape[1]
    positions = jnp.arange(length, dtype=jnp.int32)
    hidden_one = low(normalize(sequence, norm_gains[:, 0]))
    mixed = low_back(jnp.dot(hidden_one, w_qkv, precision=HIGH))
    queries, key_rows, value_rows = prepare(mixed, norm_gains[:, 1], norm_gains[:, 2], positions)
    queries = low_back(low(queries))
    key_rows = low_back(low(key_rows))
    value_rows = low_back(low(value_rows))
    attended = low_back(low(attention(queries, key_rows, value_rows))).reshape(length, width)
    attn_out = low_back(jnp.dot(attended, w_out, precision=HIGH))
    middle = sequence + attn_out
    hidden_two = low(normalize(middle, norm_gains[:, 3]))
    logits = low_back(jnp.dot(hidden_two, w_router, precision=HIGH))
    weights = route_weights(logits, seq_routes)
    blocks = slot.shape[0]
    experts = w_gate.shape[0]
    capacity = entry.shape[1] // experts
    grouped = hidden_two.reshape(blocks, -1, width)
    picked = jax.vmap(pick_rows)(grouped, entry // TOPK)
    picked = low_back(jnp.where(filled[..., None] > 0, picked, 0.0))
    expert_rows = picked.reshape(blocks, experts, capacity, width).transpose(1, 0, 2, 3).reshape(experts, blocks * capacity, width)
    gate_act = low_back(jnp.einsum('erd,edf->erf', expert_rows, w_gate, precision=HIGH))
    up_act = low_back(jnp.einsum('erd,edf->erf', expert_rows, w_up, precision=HIGH))
    inner = low(jax.nn.silu(gate_act) * up_act)
    produced = low_back(low(jnp.einsum('erf,edf->erd', inner, w_down, precision=HIGH)))
    produced = produced.reshape(experts, blocks, capacity, width).transpose(1, 0, 2, 3).reshape(blocks, experts * capacity, width)
    chosen = jax.vmap(pick_rows)(produced, slot).reshape(length, TOPK, width)
    moe = jnp.einsum('tk,tkd->td', weights, chosen, precision=HIGH)
    return middle + moe

def reference(inputs, routes, w_qkv, w_out, w_router, norm_gains, w_gate, w_up, w_down, cotangent):
    block_routes = routes.reshape(SEQS * N_SEQ, TOK_DEV, TOPK)
    slot, entry, filled = jax.vmap(partial(arrange, experts=EXPERTS, capacity=CAP))(block_routes)
    slot = slot.reshape(SEQS, N_SEQ, -1)
    entry = entry.reshape(SEQS, N_SEQ, -1)
    filled = filled.reshape(SEQS, N_SEQ, -1)

    def forward(sequences, *params):

        def step(carry, items):
            sequence, seq_routes, seq_slot, seq_entry, seq_filled = items
            return (carry, one_sequence(params, sequence, seq_routes, seq_slot, seq_entry, seq_filled))
        unused, outputs = lax.scan(jax.checkpoint(step), jnp.zeros((), jnp.float32), (sequences, routes, slot, entry, filled))
        return outputs
    weights32 = [w.astype(jnp.float32) for w in (w_qkv, w_out, w_router, norm_gains, w_gate, w_up, w_down)]
    result32, backward = jax.vjp(forward, inputs.astype(jnp.float32), *weights32)
    grads = backward(cotangent.astype(jnp.float32))
    return (result32.astype(jnp.bfloat16), grads[0], grads[1], grads[2], grads[3], grads[4], grads[5], grads[6], grads[7])
```

```python
from functools import partial

import jax
import jax.numpy as jnp
from jax import lax
from jax.experimental import pallas as pl
from jax.experimental.pallas import tpu as pltpu
from jax.sharding import PartitionSpec as P

HEADS = 16
TOPK = 8
EPS = 1e-05
NEG = -1e30
F32 = jnp.float32
BF16 = jnp.bfloat16
MESH = pl.DeviceIdType.MESH
PIECES = 2
ANY = pl.BlockSpec(memory_space=pl.ANY)
VMEM = pl.BlockSpec(memory_space=pltpu.VMEM)
MATMUL = (((1,), (0,)), ((), ()))
BY_LAST = (((1,), (1,)), ((), ()))
BY_FIRST = (((0,), (0,)), ((), ()))


def dot(a, b, dims):
    return lax.dot_general(a, b, dims, preferred_element_type=F32)


class Ring:
    def __init__(self, n, f):
        self.n, self.f = n, f
        self.chips = n // 2
        self.half = self.chips // 2
        self.pairs_minor = f == 2
        self.me = lax.axis_index("seq")
        self.mine = lax.axis_index("fsdp")
        chip = self.me // 2
        self.core = self.me % 2
        if self.pairs_minor:
            along, side = chip // 2, chip % 2
        else:
            along, side = chip % self.half, chip // self.half
        self.pos = along + side * (self.chips - 1 - 2 * along)
        self.right = self.at(self.pos + 1)
        self.left = self.at(self.pos + self.chips - 1)
        self.mate = self.me + 1 - 2 * self.core

    def at(self, place, other=False):
        place = lax.rem(place + self.chips, self.chips)
        side = place // self.half
        along = place + side * (self.chips - 1 - 2 * place)
        chip = along * 2 + side if self.pairs_minor else side * self.half + along
        core = 1 - self.core if other else self.core
        return chip * 2 + core

    def peer(self, step):
        return lax.rem(self.me + step, self.n)

    def beside(self, step):
        return lax.rem(self.mine + step, self.f)


def greet(ring, everyone, beside):
    barrier = pltpu.get_barrier_semaphore()
    count = 0
    if everyone:
        for step in range(1, ring.n):
            pl.semaphore_signal(
                barrier, inc=1, device_id={"seq": ring.peer(step)}, device_id_type=MESH
            )
        count += ring.n - 1
    else:
        for other in (ring.right, ring.left, ring.mate):
            pl.semaphore_signal(barrier, inc=1, device_id={"seq": other}, device_id_type=MESH)
        count += 3
    if beside:
        for step in range(1, ring.f):
            pl.semaphore_signal(
                barrier, inc=1, device_id={"fsdp": ring.beside(step)}, device_id_type=MESH
            )
        count += ring.f - 1
    pl.semaphore_wait(barrier, count)


def remote(src, dst, send, recv, where):
    return pltpu.make_async_remote_copy(
        src_ref=src,
        dst_ref=dst,
        send_sem=send,
        recv_sem=recv,
        device_id=where,
        device_id_type=MESH,
    )


class Gather:
    def __init__(self, ring, own, out, sems):
        self.ring, self.own, self.out = ring, own, out
        self.send, self.recv, self.mate_send, self.mate_recv, self.keep = sems
        self.piece = own.shape[0] // (2 * PIECES)

    @staticmethod
    def semaphores(n):
        hops = n // 2 - 1
        kind = pltpu.SemaphoreType.DMA
        return [
            kind((2, hops, PIECES)),
            kind((2, hops, PIECES)),
            kind((2, hops + 1, PIECES)),
            kind((2, hops + 1, PIECES)),
            kind((1,)),
        ]

    def rows(self, way, s):
        return pl.ds((way * PIECES + s) * self.piece, self.piece)

    def hop(self, way, step, s, first):
        ring = self.ring
        chunk = ring.at(ring.pos - step if way == 0 else ring.pos + step)
        rows = self.rows(way, s)
        there = self.out.at[chunk, rows]
        return remote(
            self.own.at[rows] if first else there,
            there,
            self.send.at[way, step, s],
            self.recv.at[way, step, s],
            {"seq": ring.right if way == 0 else ring.left},
        )

    def share(self, way, step, s, first):
        ring = self.ring
        chunk = ring.at(ring.pos - step if way == 0 else ring.pos + step)
        rows = self.rows(way, s)
        there = self.out.at[chunk, rows]
        return remote(
            self.own.at[rows] if first else there,
            there,
            self.mate_send.at[way, step, s],
            self.mate_recv.at[way, step, s],
            {"seq": ring.mate},
        )

    def local(self):
        return pltpu.make_async_copy(self.own, self.out.at[self.ring.me], self.keep.at[0])

    def begin(self):
        for s in range(PIECES):
            for way in (0, 1):
                self.hop(way, 0, s, True).start()
        for s in range(PIECES):
            for way in (0, 1):
                self.share(way, 0, s, True).start()
        self.local().start()

    def run(self):
        hops = self.ring.chips - 1

        def body(step, carry):
            for s in range(PIECES):
                for way in (0, 1):
                    self.hop(way, step - 1, s, False).wait_recv()
                    self.hop(way, step, s, False).start()
                    self.share(way, step, s, False).start()
            return carry

        lax.fori_loop(1, hops, body, 0)
        for s in range(PIECES):
            for way in (0, 1):
                self.hop(way, hops - 1, s, False).wait_recv()
                self.share(way, hops, s, False).start()

    def finish(self):
        hops = self.ring.chips - 1

        def body(step, carry):
            for s in range(PIECES):
                for way in (0, 1):
                    self.hop(way, step, s, False).wait_send()
                    self.share(way, step, s, False).wait()
            return carry

        lax.fori_loop(0, hops, body, 0)
        for s in range(PIECES):
            for way in (0, 1):
                self.share(way, hops, s, False).wait()
        self.local().wait()


class Scatter:
    def __init__(self, ring, part, tok, width, buffers, sems):
        self.ring, self.part, self.tok, self.width = ring, part, tok, width
        self.mate_out, self.mate_in, self.own, self.going, self.coming = buffers
        self.send, self.recv, self.mate_send, self.mate_recv = sems
        self.piece = tok // (2 * PIECES)

    @staticmethod
    def buffers(n, tok, width):
        chips = n // 2
        return [
            pltpu.VMEM((chips, tok, width), BF16),
            pltpu.VMEM((chips, tok, width), BF16),
            pltpu.VMEM((2, tok, width), F32),
            pltpu.VMEM((chips - 1, tok, width), BF16),
            pltpu.VMEM((chips - 1, tok, width), BF16),
        ]

    @staticmethod
    def semaphores(n):
        chips = n // 2
        kind = pltpu.SemaphoreType.DMA
        return [
            kind((2, chips - 1, PIECES)),
            kind((2, chips - 1, PIECES)),
            kind((chips,)),
            kind((chips,)),
        ]

    def rows(self, way, s):
        return pl.ds((way * PIECES + s) * self.piece, self.piece)

    def exchange(self, i):
        return remote(
            self.mate_out.at[i],
            self.mate_in.at[i],
            self.mate_send.at[i],
            self.mate_recv.at[i],
            {"seq": self.ring.mate},
        )

    def hop(self, way, i, s):
        ring = self.ring
        rows = self.rows(way, s)
        return remote(
            self.going.at[i, rows],
            self.coming.at[i, rows],
            self.send.at[way, i, s],
            self.recv.at[way, i, s],
            {"seq": ring.right if way == 0 else ring.left},
        )

    def produce(self, i):
        ring = self.ring
        half = self.tok // 2
        places = (ring.pos - 1 - i, ring.pos + 1 + i)
        for way in (0, 1):
            chunk = ring.at(places[way] + ring.chips, True)
            self.part(chunk, way, self.mate_out, i)
        self.exchange(i).start()
        slot = lax.rem(i, 2)
        for way in (0, 1):
            chunk = ring.at(places[way] + ring.chips)
            self.part(chunk, way, self.own, slot)

    def step(self, i, first):
        self.exchange(i).wait_recv()
        slot = lax.rem(i, 2)
        for s in range(PIECES):
            for way in (0, 1):
                rows = self.rows(way, s)
                value = self.own[slot, rows] + self.mate_in[i, rows].astype(F32)
                if not first:
                    self.hop(way, i - 1, s).wait_recv()
                    value = value + self.coming[i - 1, rows].astype(F32)
                self.going[i, rows] = value.astype(BF16)
                self.hop(way, i, s).start()

    def run(self, finish):
        last = self.ring.chips - 1
        self.produce(0)
        self.produce(1)
        self.step(0, True)

        def body(i, carry):
            self.produce(i + 1)
            self.step(i, False)
            return carry

        lax.fori_loop(1, last, body, 0)
        self.exchange(last).wait_recv()
        slot = last % 2
        for s in range(PIECES):
            for way in (0, 1):
                rows = self.rows(way, s)
                self.hop(way, last - 1, s).wait_recv()
                value = self.own[slot, rows] + self.mate_in[last, rows].astype(F32)
                value = value + self.coming[last - 1, rows].astype(F32)
                finish(rows, value)

    def close(self):
        last = self.ring.chips - 1

        def body(i, carry):
            self.exchange(i).wait_send()
            for s in range(PIECES):
                for way in (0, 1):
                    self.hop(way, i, s).wait_send()
            return carry

        lax.fori_loop(0, last, body, 0)
        self.exchange(last).wait_send()


def first_kernel(n, f, *refs):
    own, by_head, out_rows, small, routes = refs[:5]
    own_all, w_head, w_out_head, small_all, routes_all = refs[5:10]
    sems = refs[10:15]
    send, recv, beside_send, beside_recv, keep, wide_send, wide_recv = refs[15:]
    ring = Ring(n, f)
    greet(ring, True, True)
    gather = Gather(ring, own, own_all, sems)

    def push(kind, step):
        there = ring.peer(step)
        source, target = [
            (by_head.at[there], w_head.at[ring.me, ring.mine]),
            (small, small_all.at[ring.me, ring.mine]),
            (routes, routes_all.at[ring.me]),
        ][kind]
        return remote(
            source, target, send.at[kind, step], recv.at[kind, step], {"seq": there}
        )

    def wide(step):
        return remote(
            out_rows,
            w_out_head.at[ring.mine],
            wide_send.at[step],
            wide_recv.at[step],
            {"fsdp": ring.beside(step)},
        )

    def aside(kind, step, over, first):
        origin = lax.rem(ring.me + n - step, n)
        block = [w_head, small_all][kind].at[origin, ring.mine]
        source = [by_head.at[ring.me], small][kind] if first else block
        return remote(
            source,
            block,
            beside_send.at[kind, step, over],
            beside_recv.at[kind, step, over],
            {"fsdp": ring.beside(over)},
        )

    gather.begin()
    copies = [
        pltpu.make_async_copy(by_head.at[ring.me], w_head.at[ring.me, ring.mine], keep.at[0]),
        pltpu.make_async_copy(small, small_all.at[ring.me, ring.mine], keep.at[1]),
        pltpu.make_async_copy(routes, routes_all.at[ring.me], keep.at[2]),
        pltpu.make_async_copy(out_rows, w_out_head.at[ring.mine], keep.at[3]),
    ]
    for copy in copies:
        copy.start()
    for step in range(1, n):
        for kind in (1, 0, 2):
            push(kind, step).start()
    for over in range(1, f):
        aside(1, 0, over, True).start()
        aside(0, 0, over, True).start()
        wide(over).start()
    for step in range(1, n):
        for kind in (1, 0):
            push(kind, step).wait_recv()
            for over in range(1, f):
                aside(kind, step, over, False).start()
    gather.run()
    gather.finish()
    for step in range(1, n):
        push(2, step).wait_recv()
        for kind in (0, 1, 2):
            push(kind, step).wait_send()
    for step in range(n):
        for kind in (0, 1):
            for over in range(1, f):
                aside(kind, step, over, False).wait()
    for over in range(1, f):
        wide(over).wait()
    for copy in copies:
        copy.wait()


def first_gather(n, f, own, by_head, out_rows, small, routes):
    tok, width = own.shape
    kind = pltpu.SemaphoreType.DMA
    shape = jax.ShapeDtypeStruct
    return pl.pallas_call(
        partial(first_kernel, n, f),
        out_shape=[
            shape((n, tok, width), BF16),
            shape((n, f) + by_head.shape[1:], BF16),
            shape((f,) + out_rows.shape, BF16),
            shape((n, f) + small.shape, BF16),
            shape((n,) + routes.shape, jnp.int32),
        ],
        in_specs=[VMEM] * 5,
        out_specs=[ANY] * 5,
        scratch_shapes=Gather.semaphores(n)
        + [kind((3, n)), kind((3, n)), kind((2, n, f)), kind((2, n, f)), kind((4,))]
        + [kind((f,)), kind((f,))],
        compiler_params=pltpu.CompilerParams(
            collective_id=0, has_side_effects=True, vmem_limit_bytes=32 << 20
        ),
        name="first_gather",
    )(own, by_head, out_rows, small, routes)


def spread_kernel(n, f, block, out, send, recv, keep):
    ring = Ring(n, f)
    greet(ring, True, False)

    def push(step):
        return remote(
            block, out.at[ring.me], send.at[step], recv.at[step], {"seq": ring.peer(step)}
        )

    local = pltpu.make_async_copy(block, out.at[ring.me], keep.at[0])
    for step in range(1, n):
        push(step).start()
    local.start()
    for step in range(1, n):
        push(step).wait()
    local.wait()


def spread(n, f, block, ident):
    kind = pltpu.SemaphoreType.DMA
    return pl.pallas_call(
        partial(spread_kernel, n, f),
        out_shape=jax.ShapeDtypeStruct((n,) + block.shape, block.dtype),
        in_specs=[VMEM],
        out_specs=VMEM,
        scratch_shapes=[kind((n,)), kind((n,)), kind((1,))],
        compiler_params=pltpu.CompilerParams(
            collective_id=ident, has_side_effects=True, vmem_limit_bytes=16 << 20
        ),
        name="spread",
    )(block)


def blocks_of(length):
    block = min(512, length)
    return block, length // block


def attention_kernel(factor, q_ref, k_ref, v_ref, out_ref, exact_ref, sums_ref):
    length, head = q_ref.shape
    block, count = blocks_of(length)
    rows = lax.broadcasted_iota(jnp.int32, (block, block), 0)
    cols = lax.broadcasted_iota(jnp.int32, (block, block), 1)

    def outer(i, carry):
        here = pl.ds(pl.multiple_of(i * block, block), block)
        part = q_ref[here, :]

        def inner(j, state, masked):
            top, total, acc = state
            there = pl.ds(pl.multiple_of(j * block, block), block)
            scores = dot(part, k_ref[there, :], BY_LAST) * factor
            if masked:
                scores = jnp.where(cols <= rows, scores, NEG)
            new = jnp.maximum(top, jnp.max(scores, -1, keepdims=True))
            scale = jnp.exp(top - new)
            expd = jnp.exp(scores - new)
            total = total * scale + jnp.sum(expd, -1, keepdims=True)
            acc = acc * scale + dot(expd.astype(BF16), v_ref[there, :], MATMUL)
            return new, total, acc

        state = (
            jnp.full((block, 1), NEG, F32),
            jnp.zeros((block, 1), F32),
            jnp.zeros((block, head), F32),
        )
        state = lax.fori_loop(0, i, lambda j, s: inner(j, s, False), state)
        top, total, acc = inner(i, state, True)
        exact = acc / total
        exact_ref[here, :] = exact
        out_ref[here, :] = exact.astype(BF16)
        sums_ref[here, :] = top + jnp.log(total)
        return carry

    lax.fori_loop(0, count, outer, 0)


def attention(queries, keys, values, factor):
    length, head = queries.shape
    shape = jax.ShapeDtypeStruct
    return pl.pallas_call(
        partial(attention_kernel, factor),
        out_shape=[
            shape((length, head), BF16),
            shape((length, head), F32),
            shape((length, 1), F32),
        ],
        in_specs=[VMEM] * 3,
        out_specs=[VMEM] * 3,
        compiler_params=pltpu.CompilerParams(vmem_limit_bytes=32 << 20),
        cost_estimate=pl.CostEstimate(
            flops=2 * length * length * head,
            transcendentals=length * length // 2,
            bytes_accessed=8 * length * head,
        ),
        name="attention",
    )(queries, keys, values)


def attention_back_kernel(
    factor, q_ref, k_ref, v_ref, d_ref, sums_ref, delta_ref, dq_ref, dk_ref, dv_ref
):
    length, head = q_ref.shape
    block, count = blocks_of(length)
    rows = lax.broadcasted_iota(jnp.int32, (block, block), 0)
    cols = lax.broadcasted_iota(jnp.int32, (block, block), 1)
    dq_ref[...] = jnp.zeros_like(dq_ref)

    def outer(j, carry):
        there = pl.ds(pl.multiple_of(j * block, block), block)
        keys = k_ref[there, :]
        values = v_ref[there, :]

        def inner(i, state, masked):
            d_keys, d_values = state
            here = pl.ds(pl.multiple_of(i * block, block), block)
            part = q_ref[here, :]
            d_part = d_ref[here, :]
            scores = dot(keys, part, BY_LAST) * factor
            if masked:
                scores = jnp.where(rows <= cols, scores, NEG)
            probs = jnp.exp(scores - sums_ref[:, here])
            d_probs = dot(values, d_part, BY_LAST)
            d_scores = (probs * (d_probs - delta_ref[:, here])).astype(BF16)
            d_values = d_values + dot(probs.astype(BF16), d_part, MATMUL)
            d_keys = d_keys + dot(d_scores, part, MATMUL)
            dq_ref[here, :] += dot(d_scores, keys, BY_FIRST)
            return d_keys, d_values

        zero = jnp.zeros((block, head), F32)
        state = inner(j, (zero, zero), True)
        state = lax.fori_loop(j + 1, count, lambda i, s: inner(i, s, False), state)
        dk_ref[there, :] = state[0] * factor
        dv_ref[there, :] = state[1]
        return carry

    lax.fori_loop(0, count, outer, 0)
    dq_ref[...] = dq_ref[...] * factor


def attention_back(queries, keys, values, d_out, sums, delta, factor):
    length, head = queries.shape
    shape = jax.ShapeDtypeStruct((length, head), F32)
    return pl.pallas_call(
        partial(attention_back_kernel, factor),
        out_shape=[shape] * 3,
        in_specs=[VMEM] * 6,
        out_specs=[VMEM] * 3,
        compiler_params=pltpu.CompilerParams(vmem_limit_bytes=32 << 20),
        cost_estimate=pl.CostEstimate(
            flops=5 * length * length * head,
            transcendentals=length * length // 2,
            bytes_accessed=20 * length * head,
        ),
        name="attention_back",
    )(queries, keys, values, d_out, sums, delta)


def wide_store(target, slot, rows, left, right, dims):
    width = target.shape[-1]
    tile = min(512, width)
    for start in range(0, width, tile):
        cols = slice(start, start + tile)
        other = right[cols, :] if dims == BY_LAST else right[:, cols]
        target[slot, rows, cols] = dot(left, other, dims).astype(target.dtype)


def middle_kernel(n, f, *refs):
    attended, w_out, tokens, gain, router, routes = refs[:6]
    middle, hidden_all, probs_ref, weights_here = refs[6:10]
    hidden, outgoing = refs[10:12]
    buffers, scatter_sems = refs[12:17], refs[17:21]
    gather_sems = refs[21:26]
    send, recv, keep = refs[26:]
    ring = Ring(n, f)
    tok, width = tokens.shape
    half = tok // 2
    greet(ring, True, False)

    def part(chunk, way, target, slot):
        rows = pl.ds(way * half, half)
        wide_store(target, slot, rows, attended[chunk, rows, :], w_out, MATMUL)

    scatter = Scatter(ring, part, tok, width, buffers, scatter_sems)

    def finish(rows, value):
        value = tokens[rows, :].astype(F32) + value
        middle[rows, :] = value
        inverse = lax.rsqrt(jnp.mean(value * value, -1, keepdims=True) + EPS)
        hidden[rows, :] = (value * inverse * gain[...]).astype(BF16)

    scatter.run(finish)
    gather = Gather(ring, hidden, hidden_all, gather_sems)
    gather.begin()
    logits = dot(router[...], hidden[...], BY_LAST)
    expd = jnp.exp(logits - jnp.max(logits, 0, keepdims=True))
    probs = expd / jnp.sum(expd, 0, keepdims=True)
    probs_ref[...] = probs
    experts = lax.broadcasted_iota(jnp.int32, probs.shape, 0)
    named = jnp.zeros(probs.shape, F32)
    for k in range(routes.shape[0]):
        named = named + jnp.where(routes[k : k + 1, :] == experts, 1.0, 0.0)
    weights = probs * named
    for e in range(n):
        outgoing[e] = jnp.broadcast_to(weights[e : e + 1, :], (8, tok))

    def push(step):
        there = ring.peer(step)
        return remote(
            outgoing.at[there],
            weights_here.at[ring.me],
            send.at[step],
            recv.at[step],
            {"seq": there},
        )

    local = pltpu.make_async_copy(outgoing.at[ring.me], weights_here.at[ring.me], keep.at[0])
    for step in range(1, n):
        push(step).start()
    local.start()
    gather.run()
    scatter.close()
    gather.finish()
    for step in range(1, n):
        push(step).wait()
    local.wait()


def middle_stage(n, f, attended, w_out, tokens, gain, router, routes):
    tok, width = tokens.shape
    experts = router.shape[0]
    kind = pltpu.SemaphoreType.DMA
    shape = jax.ShapeDtypeStruct
    return pl.pallas_call(
        partial(middle_kernel, n, f),
        out_shape=[
            shape((tok, width), F32),
            shape((n, tok, width), BF16),
            shape((experts, tok), F32),
            shape((n, 8, tok), F32),
        ],
        in_specs=[VMEM] * 6,
        out_specs=[VMEM, ANY, VMEM, ANY],
        scratch_shapes=[pltpu.VMEM((tok, width), BF16), pltpu.VMEM((n, 8, tok), F32)]
        + Scatter.buffers(n, tok, width)
        + Scatter.semaphores(n)
        + Gather.semaphores(n)
        + [kind((n,)), kind((n,)), kind((1,))],
        compiler_params=pltpu.CompilerParams(
            collective_id=1, has_side_effects=True, vmem_limit_bytes=56 << 20
        ),
        name="middle_stage",
    )(attended, w_out, tokens, gain, router, routes)


def back_kernel(n, f, *refs):
    pick, d_rows, d_weight, probs, router, upstream, middle, gain = refs[:8]
    d_middle, d_attn_all, d_logits_all, gain_two = refs[8:12]
    d_attn, d_logits, arrived = refs[12:15]
    buffers, scatter_sems = refs[15:20], refs[20:24]
    gather_sems = refs[24:29]
    send, recv, keep = refs[29:]
    ring = Ring(n, f)
    tok, width = upstream.shape
    half = tok // 2
    greet(ring, True, False)

    def push(step):
        there = ring.peer(step)
        return remote(
            d_weight.at[there],
            arrived.at[ring.me],
            send.at[0, step],
            recv.at[0, step],
            {"seq": there},
        )

    local = pltpu.make_async_copy(d_weight.at[ring.me], arrived.at[ring.me], keep.at[0])
    for step in range(1, n):
        push(step).start()
    local.start()

    def part(chunk, way, target, slot):
        rows = pl.ds(way * half, half)
        wide_store(target, slot, rows, pick[chunk, rows, :], d_rows.at[chunk], MATMUL)

    scatter = Scatter(ring, part, tok, width, buffers, scatter_sems)

    def finish(rows, value):
        d_middle[rows, :] = value

    scatter.run(finish)
    for step in range(1, n):
        push(step).wait()
    local.wait()
    gate = probs[...]
    d_gate = jnp.concatenate([arrived[e, 0:1, :] for e in range(n)], 0)
    d_gate = gate * (d_gate - jnp.sum(gate * d_gate, 0, keepdims=True))
    d_logits[...] = d_gate.astype(BF16)
    d_hidden = d_middle[...] + dot(d_gate.astype(BF16), router[...], BY_FIRST)
    value = middle[...]
    inverse = lax.rsqrt(jnp.mean(value * value, -1, keepdims=True) + EPS)
    inner = jnp.mean(value * gain[...] * d_hidden, -1, keepdims=True)
    gain_two[...] = jnp.sum(value * inverse * d_hidden, 0, keepdims=True)
    d_value = inverse * gain[...] * d_hidden - value * (inverse * inverse * inverse) * inner
    d_value = upstream[...].astype(F32) + d_value
    d_middle[...] = d_value
    d_attn[...] = d_value.astype(BF16)
    gather = Gather(ring, d_attn, d_attn_all, gather_sems)
    gather.begin()

    def publish(step):
        return remote(
            d_logits,
            d_logits_all.at[ring.me],
            send.at[1, step],
            recv.at[1, step],
            {"seq": ring.peer(step)},
        )

    kept = pltpu.make_async_copy(d_logits, d_logits_all.at[ring.me], keep.at[1])
    for step in range(1, n):
        publish(step).start()
    kept.start()
    gather.run()
    scatter.close()
    gather.finish()
    for step in range(1, n):
        publish(step).wait()
    kept.wait()


def back_stage(n, f, pick, d_rows, d_weight, probs, router, upstream, middle, gain):
    tok, width = upstream.shape
    experts = router.shape[0]
    kind = pltpu.SemaphoreType.DMA
    shape = jax.ShapeDtypeStruct
    return pl.pallas_call(
        partial(back_kernel, n, f),
        out_shape=[
            shape((tok, width), F32),
            shape((n, tok, width), BF16),
            shape((n, experts, tok), BF16),
            shape((1, width), F32),
        ],
        in_specs=[VMEM] * 8,
        out_specs=[VMEM, ANY, ANY, VMEM],
        scratch_shapes=[
            pltpu.VMEM((tok, width), BF16),
            pltpu.VMEM((experts, tok), BF16),
            pltpu.VMEM((n, 8, tok), F32),
        ]
        + Scatter.buffers(n, tok, width)
        + Scatter.semaphores(n)
        + Gather.semaphores(n)
        + [kind((2, n)), kind((2, n)), kind((2,))],
        compiler_params=pltpu.CompilerParams(
            collective_id=2, has_side_effects=True, vmem_limit_bytes=60 << 20
        ),
        name="back_stage",
    )(pick, d_rows, d_weight, probs, router, upstream, middle, gain)


def result_kernel(n, f, *refs):
    pick, produced, weights, middle = refs[:4]
    result = refs[4]
    buffers, scatter_sems = refs[5:10], refs[10:14]
    ring = Ring(n, f)
    tok, width = middle.shape
    half = tok // 2
    greet(ring, False, False)

    def part(chunk, way, target, slot):
        rows = pl.ds(way * half, half)
        tile = min(512, width)
        for start in range(0, width, tile):
            cols = slice(start, start + tile)
            value = dot(pick[chunk, rows, :], produced[chunk, :, cols], MATMUL)
            target[slot, rows, cols] = (value * weights[chunk, rows, :]).astype(target.dtype)

    scatter = Scatter(ring, part, tok, width, buffers, scatter_sems)

    def finish(rows, value):
        result[rows, :] = (middle[rows, :] + value).astype(BF16)

    scatter.run(finish)
    scatter.close()


def result_stage(n, f, pick, produced, weights, middle):
    tok, width = middle.shape
    return pl.pallas_call(
        partial(result_kernel, n, f),
        out_shape=jax.ShapeDtypeStruct((tok, width), BF16),
        in_specs=[VMEM] * 4,
        out_specs=VMEM,
        scratch_shapes=Scatter.buffers(n, tok, width) + Scatter.semaphores(n),
        compiler_params=pltpu.CompilerParams(
            collective_id=3, has_side_effects=True, vmem_limit_bytes=56 << 20
        ),
        name="result_stage",
    )(pick, produced, weights, middle)


def last_kernel(n, f, *refs):
    d_mixed, w_head, qkv_part, tokens, gain, d_middle, gain_two, gain_head = refs[:8]
    d_inputs, qkv_rows, gains_out = refs[8:11]
    beside_rows, summed, gain_rows, gain_in, gain_side = refs[11:16]
    buffers, scatter_sems = refs[16:21], refs[21:25]
    side_send, side_recv, send, recv, keep = refs[25:]
    ring = Ring(n, f)
    tok, width = tokens.shape
    half = tok // 2
    slice_width = width // n
    greet(ring, True, True)

    def side(step):
        there = ring.beside(step)
        return remote(
            qkv_part.at[there],
            beside_rows.at[step - 1],
            side_send.at[0, step],
            side_recv.at[0, step],
            {"fsdp": there},
        )

    for step in range(1, f):
        side(step).start()

    def part(chunk, way, target, slot):
        rows = pl.ds(way * half, half)
        wide_store(target, slot, rows, d_mixed[chunk, rows, :], w_head, BY_LAST)

    scatter = Scatter(ring, part, tok, width, buffers, scatter_sems)

    def finish(rows, value):
        d_inputs[rows, :] = value

    def push(step):
        there = ring.peer(step)
        return remote(
            summed.at[there],
            qkv_rows.at[ring.me],
            send.at[0, step],
            recv.at[0, step],
            {"seq": there},
        )

    local = pltpu.make_async_copy(summed.at[ring.me], qkv_rows.at[ring.me], keep.at[0])
    for step in range(1, f):
        side(step).wait_recv()
    for block in range(n):
        value = qkv_part[ring.mine, block].astype(F32)
        for step in range(1, f):
            value = value + beside_rows[step - 1, block].astype(F32)
        summed[block] = value.astype(BF16)
    for step in range(1, n):
        push(step).start()
    local.start()
    scatter.run(finish)
    value = tokens[...].astype(F32)
    grad = d_inputs[...]
    inverse = lax.rsqrt(jnp.mean(value * value, -1, keepdims=True) + EPS)
    inner = jnp.mean(value * gain[...] * grad, -1, keepdims=True)
    gain_rows[...] = jnp.zeros_like(gain_rows)
    gain_rows[0:1, :] = jnp.sum(value * inverse * grad, 0, keepdims=True)
    gain_rows[1:2, :] = gain_two[...]

    def gains(step):
        there = ring.peer(step)
        cols = pl.ds(pl.multiple_of(there * slice_width, slice_width), slice_width)
        return remote(
            gain_rows.at[:, cols],
            gain_in.at[ring.me],
            send.at[1, step],
            recv.at[1, step],
            {"seq": there},
        )

    mine = pl.ds(pl.multiple_of(ring.me * slice_width, slice_width), slice_width)
    kept = pltpu.make_async_copy(gain_rows.at[:, mine], gain_in.at[ring.me], keep.at[1])
    for step in range(1, n):
        gains(step).start()
    kept.start()
    d_value = inverse * gain[...] * grad - value * (inverse * inverse * inverse) * inner
    d_inputs[...] = d_middle[...] + d_value
    for step in range(1, n):
        gains(step).wait()
    kept.wait()
    total = gain_head[...]
    for device in range(n):
        total = total + gain_in[device]
    gain_side[0] = total

    def sums(step):
        return remote(
            gain_side.at[0],
            gain_side.at[step],
            side_send.at[1, step],
            side_recv.at[1, step],
            {"fsdp": ring.beside(step)},
        )

    for step in range(1, f):
        sums(step).start()
    for step in range(1, f):
        sums(step).wait()
        total = total + gain_side[step]
    gains_out[...] = total
    scatter.close()
    for step in range(1, f):
        side(step).wait_send()
    for step in range(1, n):
        push(step).wait()
    local.wait()


def last_stage(n, f, d_mixed, w_head, qkv_part, tokens, gain, d_middle, gain_two, gain_head):
    tok, width = tokens.shape
    rows, across = qkv_part.shape[2:]
    kind = pltpu.SemaphoreType.DMA
    shape = jax.ShapeDtypeStruct
    return pl.pallas_call(
        partial(last_kernel, n, f),
        out_shape=[
            shape((tok, width), F32),
            shape((n, rows, across), BF16),
            shape((8, width // n), F32),
        ],
        in_specs=[VMEM] * 8,
        out_specs=[VMEM] * 3,
        scratch_shapes=[
            pltpu.VMEM((max(f - 1, 1), n, rows, across), BF16),
            pltpu.VMEM((n, rows, across), BF16),
            pltpu.VMEM((8, width), F32),
            pltpu.VMEM((n, 8, width // n), F32),
            pltpu.VMEM((f, 8, width // n), F32),
        ]
        + Scatter.buffers(n, tok, width)
        + Scatter.semaphores(n)
        + [kind((2, f)), kind((2, f)), kind((2, n)), kind((2, n)), kind((2,))],
        compiler_params=pltpu.CompilerParams(
            collective_id=4, has_side_effects=True, vmem_limit_bytes=60 << 20
        ),
        name="last_stage",
    )(d_mixed, w_head, qkv_part, tokens, gain, d_middle, gain_two, gain_head)


def angles_of(length, head_size):
    half = head_size // 2
    freqs = 10000.0 ** (-jnp.arange(half, dtype=F32) / half)
    angles = jnp.arange(length, dtype=jnp.int32).astype(F32)[:, None] * freqs[None, :]
    cosine = jnp.concatenate([jnp.cos(angles), jnp.cos(angles)], -1)
    sine = jnp.concatenate([jnp.sin(angles), jnp.sin(angles)], -1)
    return cosine, sine


def turn(values):
    half = values.shape[-1] // 2
    return jnp.concatenate([-values[..., half:], values[..., :half]], -1)


def turn_back(values):
    half = values.shape[-1] // 2
    return jnp.concatenate([values[..., half:], -values[..., :half]], -1)


def shift_fsdp(values, step, f):
    if step == 0:
        return values
    return lax.ppermute(values, "fsdp", [(i, (i + step) % f) for i in range(f)])


def shards(n, f, inputs, routes, w_qkv, w_out, w_router, norm_gains, w_gate, w_up, w_down, cotangent):
    tokens_low = inputs[0]
    upstream_low = cotangent[0]
    local_routes = routes[0].T
    me = lax.axis_index("seq")
    mine = lax.axis_index("fsdp")
    tok, width = tokens_low.shape
    length = tok * n
    head_size = width // HEADS
    across = 3 * head_size
    rows = w_qkv.shape[0]
    experts = n * w_gate.shape[0]
    capacity = min(tok, 5 * tok * TOPK // (4 * experts))
    factor = head_size ** (-0.5)

    by_head = w_qkv.reshape(rows, 3, HEADS, head_size).transpose(2, 0, 1, 3)
    by_head = by_head.reshape(HEADS, rows, across)
    small = jnp.concatenate([w_router, norm_gains], 1)
    small = jnp.pad(small, ((0, 0), (0, 128 - small.shape[1])))
    tokens_all, w_head, w_out_head, small_all, routes_all = first_gather(
        n, f, tokens_low, by_head, w_out, small, local_routes
    )
    gates = [shift_fsdp(w_gate[0], j, f) for j in range(f)]
    ups = [shift_fsdp(w_up[0], j, f) for j in range(f)]
    downs = [shift_fsdp(w_down[0], j, f) for j in range(f)]
    tokens_all = tokens_all.reshape(length, width)
    w_head = w_head.reshape(width, across)
    w_out_head = w_out_head.reshape(head_size, width)
    small_all = small_all.reshape(width, 128)
    router = small_all[:, :experts].T
    gains = small_all[:, experts : experts + 4].astype(F32).T
    upstream_low, _ = lax.optimization_barrier((upstream_low, tokens_all))
    upstream_all = lax.all_gather(upstream_low, "seq", axis=0, tiled=False)

    tokens_all32 = tokens_all.astype(F32)
    inverse_one = lax.rsqrt(jnp.mean(tokens_all32 * tokens_all32, -1, keepdims=True) + EPS)
    hidden_one = (tokens_all32 * inverse_one * gains[0:1]).astype(BF16)
    mixed = dot(hidden_one, w_head, MATMUL)
    raw_q = mixed[:, :head_size]
    raw_k = mixed[:, head_size : 2 * head_size]
    squares = jnp.stack([jnp.sum(raw_q * raw_q, -1), jnp.sum(raw_k * raw_k, -1)])
    squares = jnp.sum(spread(n, f, squares.reshape(-1, 128), 5), 0).reshape(2, length)
    inverses = lax.rsqrt(squares / width + EPS)
    inverse_q, inverse_k = inverses[0][:, None], inverses[1][:, None]
    own = lax.dynamic_slice_in_dim(gains, me * head_size, head_size, 1)
    gain_q, gain_k = own[1:2], own[2:3]
    cosine, sine = angles_of(length, head_size)
    normed_q = raw_q * inverse_q * gain_q
    normed_k = raw_k * inverse_k * gain_k
    queries = (normed_q * cosine + turn(normed_q) * sine).astype(BF16)
    keys = (normed_k * cosine + turn(normed_k) * sine).astype(BF16)
    values = mixed[:, 2 * head_size :].astype(BF16)
    attended, exact, sums = attention(queries, keys, values, factor)

    middle, hidden_all, gate_probs, weights_here = middle_stage(
        n,
        f,
        attended.reshape(n, tok, head_size),
        w_out_head,
        tokens_low,
        gains[3:4],
        router,
        local_routes,
    )

    weights_here = weights_here[:, 0, :]
    here = jnp.any(routes_all == me, 1)
    count = here.astype(jnp.int32)
    place = jnp.cumsum(count, 1) - count
    place = jnp.where(here, place, -1)
    slots = jnp.arange(capacity, dtype=jnp.int32)
    pick = slots[None, :, None] == place[:, None, :]
    pick_low = pick.astype(BF16)
    pick_back = (slots[None, None, :] == place[:, :, None]).astype(BF16)
    take = (((2,), (1,)), ((0,), (0,)))
    expert_rows = lax.dot_general(pick_low, hidden_all, take, preferred_element_type=F32)
    expert_rows = expert_rows.astype(BF16).reshape(n * capacity, width)
    upstream_rows = lax.dot_general(pick_low, upstream_all, take, preferred_element_type=F32)
    row_weight = jnp.sum(jnp.where(pick, weights_here[:, None, :], 0.0), -1)
    d_produced = (row_weight[..., None] * upstream_rows).astype(BF16).reshape(n * capacity, width)
    produced = 0.0
    inners, keeps = [], []
    for j in range(f):
        gate_act = dot(expert_rows, gates[j], MATMUL)
        up_act = dot(expert_rows, ups[j], MATMUL)
        sigma = jax.nn.sigmoid(gate_act)
        silu = gate_act * sigma
        inner = (silu * up_act).astype(BF16)
        produced = produced + dot(inner, downs[j], BY_LAST)
        inners.append(inner)
        keeps.append((gate_act, up_act, sigma, silu))
    produced = produced.astype(BF16).reshape(n, capacity, width)
    d_weight_rows = jnp.sum(produced.astype(F32) * upstream_rows, -1)
    d_weight_tok = jnp.sum(jnp.where(pick, d_weight_rows[..., None], 0.0), 1)
    d_weight_tok = jnp.broadcast_to(d_weight_tok[:, None, :], (n, 8, tok))
    d_rows = 0.0
    backs = []
    for j in range(f):
        gate_act, up_act, sigma, silu = keeps[j]
        d_inner = dot(d_produced, downs[j], MATMUL)
        d_gate = (d_inner * up_act * sigma * (1.0 + gate_act * (1.0 - sigma))).astype(BF16)
        d_up = (d_inner * silu).astype(BF16)
        d_rows = d_rows + dot(d_gate, gates[j], BY_LAST) + dot(d_up, ups[j], BY_LAST)
        backs.append((d_gate, d_up))
    d_rows = d_rows.astype(BF16).reshape(n, capacity, width)

    d_middle, d_attn_all, d_logits_all, gain_two = back_stage(
        n,
        f,
        pick_back,
        d_rows,
        d_weight_tok,
        gate_probs,
        router,
        upstream_low,
        middle,
        gains[3:4],
    )
    result = result_stage(n, f, pick_back, produced, weights_here[:, :, None], middle)

    grads = []
    for left, right in (
        (lambda j: expert_rows, lambda j: backs[j][0]),
        (lambda j: expert_rows, lambda j: backs[j][1]),
        (lambda j: d_produced, lambda j: inners[j]),
    ):
        total = dot(left(0), right(0), BY_FIRST)
        for j in range(1, f):
            part = dot(left(j), right(j), BY_FIRST).astype(BF16)
            total = total + shift_fsdp(part, f - j, f).astype(F32)
        grads.append(total[None])

    d_attn_all = d_attn_all.reshape(length, width)
    d_attended = dot(d_attn_all, w_out_head, BY_LAST).astype(BF16)
    delta = jnp.sum(d_attended.astype(F32) * exact, -1)[None, :]
    d_queries, d_keys, d_values = attention_back(
        queries, keys, values, d_attended, sums.reshape(1, length), delta, factor
    )
    d_q = d_queries.astype(BF16).astype(F32)
    d_k = d_keys.astype(BF16).astype(F32)
    d_q = d_q * cosine + turn_back(d_q * sine)
    d_k = d_k * cosine + turn_back(d_k * sine)
    inners = jnp.stack(
        [jnp.sum(raw_q * gain_q * d_q, -1), jnp.sum(raw_k * gain_k * d_k, -1)]
    )
    inners = jnp.sum(spread(n, f, inners.reshape(-1, 128), 6), 0).reshape(2, length) / width
    d_raw_q = inverse_q * gain_q * d_q - raw_q * (inverse_q**3) * inners[0][:, None]
    d_raw_k = inverse_k * gain_k * d_k - raw_k * (inverse_k**3) * inners[1][:, None]
    gain_query = jnp.sum(raw_q * inverse_q * d_q, 0)
    gain_key = jnp.sum(raw_k * inverse_k * d_k, 0)
    d_mixed = jnp.concatenate(
        [d_raw_q.astype(BF16), d_raw_k.astype(BF16), d_values.astype(BF16)], 1
    )
    qkv_part = dot(hidden_one, d_mixed, BY_FIRST).astype(BF16)
    qkv_part = qkv_part.reshape(n, f, rows, across).transpose(1, 0, 2, 3)
    zero = jnp.zeros((head_size,), F32)
    gain_head = jnp.stack([zero, zero, gain_query, gain_key, zero, zero, zero, zero])
    grad_inputs, qkv_rows, gains_own = last_stage(
        n,
        f,
        d_mixed.reshape(n, tok, across),
        w_head,
        qkv_part,
        tokens_low,
        gains[0:1],
        d_middle,
        gain_two,
        gain_head,
    )
    grad_qkv = (
        qkv_rows.reshape(HEADS, rows, 3, head_size)
        .transpose(1, 2, 0, 3)
        .reshape(rows, 3 * width)
        .astype(F32)
    )
    own_hidden = lax.dynamic_slice_in_dim(hidden_all, me * head_size, head_size, 2)
    proj_part = dot(attended, d_attn_all, BY_FIRST)
    router_part = jnp.einsum(
        "ntc,nkt->ck", own_hidden, d_logits_all, preferred_element_type=F32
    )
    both = jnp.concatenate([proj_part, router_part], 1).reshape(f, rows, width + experts)
    total = lax.dynamic_index_in_dim(both, mine, 0, keepdims=False)
    for j in range(1, f):
        part = lax.dynamic_index_in_dim(both, (mine + j) % f, 0, keepdims=False)
        total = total + shift_fsdp(part.astype(BF16), j, f).astype(F32)
    gains_out = jnp.stack([gains_own[0], gains_own[2], gains_own[3], gains_own[1]], 1)
    grad_gains = lax.dynamic_slice_in_dim(gains_out, mine * rows, rows, 0)
    return (
        result[None],
        grad_inputs[None],
        grad_qkv,
        total[:, :width],
        total[:, width:],
        grad_gains,
        *grads,
    )


def solution(mesh):
    tokens = P("fsdp", "seq", None)
    split = P(("seq", "fsdp"), None)
    expert = P("seq", None, "fsdp")
    return jax.shard_map(
        partial(shards, mesh.shape["seq"], mesh.shape["fsdp"]),
        mesh=mesh,
        in_specs=(tokens, tokens, split, split, split, split, expert, expert, expert, tokens),
        out_specs=(tokens, tokens, split, split, split, split, expert, expert, expert),
        check_vma=False,
    )
```

```python
from functools import partial

import jax
import jax.numpy as jnp
from jax import lax
from jax.experimental import pallas as pl
from jax.experimental.pallas import tpu as pltpu
from jax.sharding import PartitionSpec as P


HEADS = 16
TOPK = 8
EPS = 1e-05
NEG = -1e30
F32 = jnp.float32
BF16 = jnp.bfloat16
MESH = pl.DeviceIdType.MESH
PIECES = 2
ANY = pl.BlockSpec(memory_space=pl.ANY)
VMEM = pl.BlockSpec(memory_space=pltpu.VMEM)
MATMUL = (((1,), (0,)), ((), ()))
BY_LAST = (((1,), (1,)), ((), ()))
BY_FIRST = (((0,), (0,)), ((), ()))


def dot(a, b, dims):
    return lax.dot_general(a, b, dims, preferred_element_type=F32)


class Ring:
    def __init__(self, n, f):
        self.n, self.f = n, f
        self.chips = n // 2
        self.half = self.chips // 2
        self.pairs_minor = f == 2
        self.me = lax.axis_index("seq")
        self.mine = lax.axis_index("fsdp")
        chip = self.me // 2
        self.core = self.me % 2
        if self.pairs_minor:
            along, side = chip // 2, chip % 2
        else:
            along, side = chip % self.half, chip // self.half
        self.pos = along + side * (self.chips - 1 - 2 * along)
        self.right = self.at(self.pos + 1)
        self.left = self.at(self.pos + self.chips - 1)
        self.mate = self.me + 1 - 2 * self.core
        self.sign = 1 - 2 * self.core
        self.onward = self.at(self.pos + self.sign + self.chips)

    def at(self, place, other=False):
        place = lax.rem(place + self.chips, self.chips)
        side = place // self.half
        along = place + side * (self.chips - 1 - 2 * place)
        chip = along * 2 + side if self.pairs_minor else side * self.half + along
        core = 1 - self.core if other else self.core
        return chip * 2 + core

    def peer(self, step):
        return lax.rem(self.me + step, self.n)

    def beside(self, step):
        return lax.rem(self.mine + step, self.f)


def greet(ring, everyone, beside):
    barrier = pltpu.get_barrier_semaphore()
    count = 0
    if everyone:
        for step in range(1, ring.n):
            pl.semaphore_signal(
                barrier, inc=1, device_id={"seq": ring.peer(step)}, device_id_type=MESH
            )
        count += ring.n - 1
    else:
        for other in (ring.right, ring.left, ring.mate):
            pl.semaphore_signal(barrier, inc=1, device_id={"seq": other}, device_id_type=MESH)
        count += 3
    if beside:
        for step in range(1, ring.f):
            pl.semaphore_signal(
                barrier, inc=1, device_id={"fsdp": ring.beside(step)}, device_id_type=MESH
            )
        count += ring.f - 1
    pl.semaphore_wait(barrier, count)


def remote(src, dst, send, recv, where):
    return pltpu.make_async_remote_copy(
        src_ref=src,
        dst_ref=dst,
        send_sem=send,
        recv_sem=recv,
        device_id=where,
        device_id_type=MESH,
    )


class Gather:
    def __init__(self, ring, own, out, sems):
        self.ring, self.own, self.out = ring, own, out
        self.send, self.recv, self.mate_send, self.mate_recv, self.keep = sems
        self.piece = own.shape[0] // (2 * PIECES)
        self.last = ring.chips - 1

    @staticmethod
    def semaphores(n):
        hops = n // 2 - 1
        kind = pltpu.SemaphoreType.DMA
        return [
            kind((2, hops, PIECES)),
            kind((2, hops, PIECES)),
            kind((2, hops + 1, PIECES)),
            kind((2, hops + 1, PIECES)),
            kind((1,)),
        ]

    def rows(self, way, s):
        return pl.ds((way * PIECES + s) * self.piece, self.piece)

    def hop(self, way, step, s, first):
        ring = self.ring
        chunk = ring.at(ring.pos - step if way == 0 else ring.pos + step)
        rows = self.rows(way, s)
        there = self.out.at[chunk, rows]
        return remote(
            self.own.at[rows] if first else there,
            there,
            self.send.at[way, step, s],
            self.recv.at[way, step, s],
            {"seq": ring.right if way == 0 else ring.left},
        )

    def share(self, way, step, s, first):
        ring = self.ring
        chunk = ring.at(ring.pos - step if way == 0 else ring.pos + step)
        rows = self.rows(way, s)
        there = self.out.at[chunk, rows]
        return remote(
            self.own.at[rows] if first else there,
            there,
            self.mate_send.at[way, step, s],
            self.mate_recv.at[way, step, s],
            {"seq": ring.mate},
        )

    def local(self):
        return pltpu.make_async_copy(self.own, self.out.at[self.ring.me], self.keep.at[0])

    def begin(self):
        for s in range(PIECES):
            for way in (0, 1):
                self.hop(way, 0, s, True).start()
        for s in range(PIECES):
            for way in (0, 1):
                self.share(way, 0, s, True).start()
        self.local().start()

    def pass_on(self, i):
        for s in range(PIECES):
            for way in (0, 1):
                self.hop(way, i, s, False).wait_recv()

                @pl.when(i + 1 < self.ring.chips - 1)
                def _():
                    self.hop(way, i + 1, s, False).start()

                self.share(way, i + 1, s, False).start()

    def run(self):
        def body(step, carry):
            self.pass_on(step)
            return carry

        lax.fori_loop(0, self.ring.chips - 1, body, 0)

    def finish(self):
        hops = self.ring.chips - 1

        def body(step, carry):
            for s in range(PIECES):
                for way in (0, 1):
                    self.hop(way, step, s, False).wait_send()
                    self.share(way, step, s, False).wait()
            return carry

        lax.fori_loop(0, hops, body, 0)
        for s in range(PIECES):
            for way in (0, 1):
                self.share(way, hops, s, False).wait()
        self.local().wait()


class Scatter:
    def __init__(self, ring, part, tok, width, buffers, sems):
        self.ring, self.part, self.tok, self.width = ring, part, tok, width
        self.mate_out, self.mate_in, self.own, self.going, self.coming = buffers
        self.send, self.recv, self.mate_send, self.mate_recv = sems
        self.piece = tok // (2 * PIECES)

    @staticmethod
    def buffers(n, tok, width):
        chips = n // 2
        return [
            pltpu.VMEM((chips, tok, width), BF16),
            pltpu.VMEM((chips, tok, width), BF16),
            pltpu.VMEM((2, tok, width), F32),
            pltpu.VMEM((chips - 1, tok, width), BF16),
            pltpu.VMEM((chips - 1, tok, width), BF16),
        ]

    @staticmethod
    def semaphores(n):
        chips = n // 2
        kind = pltpu.SemaphoreType.DMA
        return [
            kind((2, chips - 1, PIECES)),
            kind((2, chips - 1, PIECES)),
            kind((chips,)),
            kind((chips,)),
        ]

    def rows(self, way, s):
        return pl.ds((way * PIECES + s) * self.piece, self.piece)

    def exchange(self, i):
        return remote(
            self.mate_out.at[i],
            self.mate_in.at[i],
            self.mate_send.at[i],
            self.mate_recv.at[i],
            {"seq": self.ring.mate},
        )

    def hop(self, way, i, s):
        ring = self.ring
        rows = self.rows(way, s)
        return remote(
            self.going.at[i, rows],
            self.coming.at[i, rows],
            self.send.at[way, i, s],
            self.recv.at[way, i, s],
            {"seq": ring.right if way == 0 else ring.left},
        )

    def produce(self, i):
        ring = self.ring
        half = self.tok // 2
        places = (ring.pos - 1 - i, ring.pos + 1 + i)
        for way in (0, 1):
            chunk = ring.at(places[way] + ring.chips, True)
            self.part(chunk, way, self.mate_out, i)
        self.exchange(i).start()
        slot = lax.rem(i, 2)
        for way in (0, 1):
            chunk = ring.at(places[way] + ring.chips)
            self.part(chunk, way, self.own, slot)

    def step(self, i, first):
        self.exchange(i).wait_recv()
        slot = lax.rem(i, 2)
        for s in range(PIECES):
            for way in (0, 1):
                rows = self.rows(way, s)
                value = self.own[slot, rows] + self.mate_in[i, rows].astype(F32)
                if not first:
                    self.hop(way, i - 1, s).wait_recv()
                    value = value + self.coming[i - 1, rows].astype(F32)
                self.going[i, rows] = value.astype(BF16)
                self.hop(way, i, s).start()

    def run(self, finish, between=None):
        last = self.ring.chips - 1
        self.produce(0)
        self.produce(1)
        self.step(0, True)

        def body(i, carry):
            self.produce(i + 1)
            self.step(i, False)
            return carry

        if between is None:
            lax.fori_loop(1, last, body, 0)
        else:
            lax.fori_loop(1, last // 2 + 1, body, 0)
            between()
            lax.fori_loop(last // 2 + 1, last, body, 0)
        self.exchange(last).wait_recv()
        slot = last % 2
        for s in range(PIECES):
            for way in (0, 1):
                rows = self.rows(way, s)
                self.hop(way, last - 1, s).wait_recv()
                value = self.own[slot, rows] + self.mate_in[last, rows].astype(F32)
                value = value + self.coming[last - 1, rows].astype(F32)
                finish(rows, value)

    def close(self):
        last = self.ring.chips - 1

        def body(i, carry):
            self.exchange(i).wait_send()
            for s in range(PIECES):
                for way in (0, 1):
                    self.hop(way, i, s).wait_send()
            return carry

        lax.fori_loop(0, last, body, 0)
        self.exchange(last).wait_send()


class Walk:
    def __init__(self, ring, own, out, sems):
        self.ring, self.own, self.out = ring, own, out
        self.send, self.recv, self.share_send, self.share_recv, self.keep = sems
        self.piece = own.shape[0] // PIECES
        self.last = ring.chips - 1

    @staticmethod
    def semaphores(n):
        kind = pltpu.SemaphoreType.DMA
        return [kind((n // 2, PIECES)) for _ in range(4)] + [kind((1,))]

    def block(self, i):
        ring = self.ring
        return ring.at(ring.pos - ring.sign * i + 2 * ring.chips)

    def hop(self, i, s, first=False):
        rows = pl.ds(s * self.piece, self.piece)
        there = self.out.at[self.block(i), rows]
        return remote(
            self.own.at[rows] if first else there,
            there,
            self.send.at[i, s],
            self.recv.at[i, s],
            {"seq": self.ring.onward},
        )

    def share(self, i, s, first=False):
        rows = pl.ds(s * self.piece, self.piece)
        there = self.out.at[self.block(i), rows]
        return remote(
            self.own.at[rows] if first else there,
            there,
            self.share_send.at[i, s],
            self.share_recv.at[i, s],
            {"seq": self.ring.mate},
        )

    def local(self):
        return pltpu.make_async_copy(self.own, self.out.at[self.ring.me], self.keep.at[0])

    def begin(self):
        for s in range(PIECES):
            self.hop(0, s, True).start()
        for s in range(PIECES):
            self.share(0, s, True).start()
        self.local().start()

    def pass_on(self, i):
        for s in range(PIECES):
            self.hop(i, s).wait_recv()

            @pl.when(i + 1 < self.last)
            def _():
                self.hop(i + 1, s).start()

            self.share(i + 1, s).start()

    def finish(self):
        def body(i, carry):
            for s in range(PIECES):
                self.hop(i, s).wait_send()
                self.share(i, s).wait()
            return carry

        lax.fori_loop(0, self.last, body, 0)
        for s in range(PIECES):
            self.share(self.last, s).wait()
        self.local().wait()


class Fold:
    def __init__(self, ring, part, buffers, sems):
        self.ring, self.part = ring, part
        self.mate_out, self.mate_in, self.own, self.going, self.coming = buffers
        self.swap_send, self.swap_recv, self.send, self.recv = sems
        self.piece = self.own.shape[0] // PIECES
        self.last = ring.chips - 1

    @staticmethod
    def buffers(n, tok, width):
        chips = n // 2
        return [
            pltpu.VMEM((2, tok, width), BF16),
            pltpu.VMEM((chips, tok, width), BF16),
            pltpu.VMEM((tok, width), F32),
            pltpu.VMEM((2, tok, width), BF16),
            pltpu.VMEM((chips - 1, tok, width), BF16),
        ]

    @staticmethod
    def semaphores(n):
        chips = n // 2
        kind = pltpu.SemaphoreType.DMA
        return [kind((chips,)), kind((chips,)), kind((chips, PIECES)), kind((chips, PIECES))]

    def swap(self, i):
        return remote(
            self.mate_out.at[lax.rem(i, 2)],
            self.mate_in.at[i],
            self.swap_send.at[i],
            self.swap_recv.at[i],
            {"seq": self.ring.mate},
        )

    def hop(self, i, s):
        rows = pl.ds(s * self.piece, self.piece)
        return remote(
            self.going.at[lax.rem(i, 2), rows],
            self.coming.at[i, rows],
            self.send.at[i, s],
            self.recv.at[i, s],
            {"seq": self.ring.onward},
        )

    def produce(self, i):
        ring = self.ring

        @pl.when(i >= 2)
        def _():
            self.swap(i - 2).wait_send()

        slot = lax.rem(i, 2)
        there = ring.at(ring.pos + ring.sign * (1 + i) + 2 * ring.chips, True)
        self.part(there, self.mate_out.at[slot])
        self.swap(i).start()
        here = ring.at(ring.pos - ring.sign * (1 + i) + 2 * ring.chips)
        self.part(here, self.own)

    def step(self, i):
        self.swap(i).wait_recv()

        @pl.when(i >= 2)
        def _():
            for s in range(PIECES):
                self.hop(i - 2, s).wait_send()

        for s in range(PIECES):
            rows = pl.ds(s * self.piece, self.piece)

            @pl.when(i > 0)
            def _():
                self.hop(i - 1, s).wait_recv()
                self.own[rows, :] = self.own[rows, :] + self.coming[i - 1, rows].astype(F32)

            value = self.own[rows, :] + self.mate_in[i, rows].astype(F32)
            self.going[lax.rem(i, 2), rows] = value.astype(BF16)
            self.hop(i, s).start()

    def run(self, finish, filler, after):
        last = self.last

        def body(i, carry):
            self.produce(i)
            self.step(i)
            after(i)
            filler(i)
            return carry

        lax.fori_loop(1, last, body, 0)
        self.produce(last)
        filler(last)
        self.swap(last).wait_recv()
        for s in range(PIECES):
            rows = pl.ds(s * self.piece, self.piece)
            self.hop(last - 1, s).wait_recv()
            value = self.own[rows, :] + self.mate_in[last, rows].astype(F32)
            finish(rows, value + self.coming[last - 1, rows].astype(F32))

    def close(self):
        last = self.last
        for s in range(PIECES):
            self.hop(last - 2, s).wait_send()
            self.hop(last - 1, s).wait_send()
        self.swap(last - 1).wait_send()
        self.swap(last).wait_send()


class Stored:
    def __init__(self, ring, parts, buffers, sems):
        self.ring, self.parts = ring, parts
        self.near, self.mate_in, self.going, self.coming = buffers
        self.swap_send, self.swap_recv, self.send, self.recv, self.load_sem = sems
        self.piece = self.near.shape[1] // PIECES
        self.last = ring.chips - 1

    @staticmethod
    def buffers(n, tok, width):
        chips = n // 2
        return [
            pltpu.VMEM((2, tok, width), BF16),
            pltpu.VMEM((chips, tok, width), BF16),
            pltpu.VMEM((2, tok, width), BF16),
            pltpu.VMEM((chips - 1, tok, width), BF16),
        ]

    @staticmethod
    def semaphores(n):
        chips = n // 2
        kind = pltpu.SemaphoreType.DMA
        return [
            kind((chips,)),
            kind((chips,)),
            kind((chips, PIECES)),
            kind((chips, PIECES)),
            kind((2,)),
        ]

    def swap(self, i):
        ring = self.ring
        there = ring.at(ring.pos + ring.sign * (1 + i) + 2 * ring.chips, True)
        return remote(
            self.parts.at[there],
            self.mate_in.at[i],
            self.swap_send.at[i],
            self.swap_recv.at[i],
            {"seq": ring.mate},
        )

    def load(self, i):
        ring = self.ring
        here = ring.at(ring.pos - ring.sign * (1 + i) + 2 * ring.chips)
        slot = lax.rem(i, 2)
        return pltpu.make_async_copy(
            self.parts.at[here], self.near.at[slot], self.load_sem.at[slot]
        )

    def hop(self, i, s):
        rows = pl.ds(s * self.piece, self.piece)
        return remote(
            self.going.at[lax.rem(i, 2), rows],
            self.coming.at[i, rows],
            self.send.at[i, s],
            self.recv.at[i, s],
            {"seq": self.ring.onward},
        )

    def begin(self):
        self.load(0).start()

        def body(i, carry):
            self.swap(i).start()
            return carry

        lax.fori_loop(0, self.last + 1, body, 0)

    def step(self, i):
        self.load(i).wait()
        self.load(i + 1).start()
        self.swap(i).wait_recv()
        slot = lax.rem(i, 2)

        @pl.when(i >= 2)
        def _():
            for s in range(PIECES):
                self.hop(i - 2, s).wait_send()

        for s in range(PIECES):
            rows = pl.ds(s * self.piece, self.piece)
            value = self.near[slot, rows].astype(F32) + self.mate_in[i, rows].astype(F32)
            self.going[slot, rows] = value.astype(BF16)

            @pl.when(i > 0)
            def _():
                self.hop(i - 1, s).wait_recv()
                total = self.near[slot, rows].astype(F32) + self.mate_in[i, rows].astype(F32)
                total = total + self.coming[i - 1, rows].astype(F32)
                self.going[slot, rows] = total.astype(BF16)

            self.hop(i, s).start()

    def close(self, finish):
        last = self.last
        self.load(last).wait()
        self.swap(last).wait_recv()
        for s in range(PIECES):
            rows = pl.ds(s * self.piece, self.piece)
            self.hop(last - 1, s).wait_recv()
            value = self.near[last % 2, rows].astype(F32) + self.mate_in[last, rows].astype(F32)
            finish(rows, value + self.coming[last - 1, rows].astype(F32))
            self.hop(last - 2, s).wait_send()
            self.hop(last - 1, s).wait_send()

        def body(i, carry):
            self.swap(i).wait_send()
            return carry

        lax.fori_loop(0, last + 1, body, 0)


def first_kernel(n, f, *refs):
    own, by_head, small, routes, w_out, w_gate, w_up = refs[:7]
    hidden_all, mixed, w_head, router, gains, routes_all, gate_near, up_near, out_all = refs[7:16]
    near, small_all, out_rows = refs[16:19]
    sems, out_sems = refs[19:24], refs[24:29]
    send, recv, beside_send, beside_recv, keep = refs[29:34]
    wide_send, wide_recv, row_send, row_recv, out_sem = refs[34:]
    ring = Ring(n, f)
    experts = router.shape[0]
    tok, width = own.shape
    rows = small.shape[0]
    hops = ring.chips - 1
    piece = width // ring.chips
    greet(ring, True, True)
    gather = Gather(ring, own, near, sems)
    gather_out = Gather(ring, out_rows, out_all, out_sems)
    out_mine = pl.ds(pl.multiple_of(ring.mine * rows, rows), rows)

    def push(kind, step):
        there = ring.peer(step)
        source, target = [
            (by_head.at[there], w_head.at[ring.me, ring.mine]),
            (small, small_all.at[ring.me, ring.mine]),
            (routes, routes_all.at[ring.me]),
        ][kind]
        return remote(
            source, target, send.at[kind, step], recv.at[kind, step], {"seq": there}
        )

    def aside(kind, step, over, first):
        origin = lax.rem(ring.me + n - step, n)
        block = [w_head, small_all][kind].at[origin, ring.mine]
        source = [by_head.at[ring.me], small][kind] if first else block
        return remote(
            source,
            block,
            beside_send.at[kind, step, over],
            beside_recv.at[kind, step, over],
            {"fsdp": ring.beside(over)},
        )

    def row(over):
        return remote(
            w_out,
            out_rows.at[out_mine],
            row_send.at[over],
            row_recv.at[over],
            {"fsdp": ring.beside(over)},
        )

    def wide(kind, part, over):
        these = pl.ds(part * piece, piece)
        return remote(
            [w_gate, w_up][kind].at[these],
            [gate_near, up_near][kind].at[over - 1, these],
            wide_send.at[kind, part, over],
            wide_recv.at[kind, part, over],
            {"fsdp": ring.beside(over)},
        )

    gather.begin()
    for over in range(1, f):
        row(over).start()
    copies = [
        pltpu.make_async_copy(by_head.at[ring.me], w_head.at[ring.me, ring.mine], keep.at[0]),
        pltpu.make_async_copy(small, small_all.at[ring.me, ring.mine], keep.at[1]),
        pltpu.make_async_copy(routes, routes_all.at[ring.me], keep.at[2]),
        pltpu.make_async_copy(w_out, out_rows.at[out_mine], keep.at[3]),
    ]
    for copy in copies:
        copy.start()
    for step in range(1, n):
        for kind in (1, 0, 2):
            push(kind, step).start()
    for over in range(1, f):
        aside(1, 0, over, True).start()
        aside(0, 0, over, True).start()
        for kind in (0, 1):
            wide(kind, 0, over).start()
    copies[3].wait()
    for over in range(1, f):
        row(over).wait_recv()
    gather_out.begin()
    each = -(-(n - 1) // (hops - 1))
    for i in range(hops):
        gather.pass_on(i)
        gather_out.pass_on(i)
        if i:
            for step in range((i - 1) * each + 1, min(i * each, n - 1) + 1):
                for kind in (1, 0):
                    push(kind, step).wait_recv()
                    for over in range(1, f):
                        aside(kind, step, over, False).start()
        for over in range(1, f):
            for kind in (0, 1):
                wide(kind, i + 1, over).start()
    gather.finish()
    for copy in copies[:3]:
        copy.wait()
    for step in range(1, n):
        push(2, step).wait_recv()
        for kind in (0, 1, 2):
            push(kind, step).wait_send()
    for step in range(n):
        for kind in (0, 1):
            for over in range(1, f):
                aside(kind, step, over, False).wait()

    lanes = lax.broadcasted_iota(jnp.int32, (32, small.shape[1]), 1)
    places = lax.broadcasted_iota(jnp.int32, (32, small.shape[1]), 0)
    chosen = jnp.where(lanes == places, 1.0, 0.0).astype(BF16)
    for c in range(n):
        for x in range(f):
            start = (c * f + x) * rows
            flipped = dot(chosen, small_all[c, x], BY_LAST)
            router[:, start : start + rows] = flipped[0:experts, :].astype(BF16)
            gains[:, start : start + rows] = flipped[experts : experts + 8, :]

    def out(c):
        return pltpu.make_async_copy(near.at[c], hidden_all.at[c], out_sem.at[c])

    def project(c, carry):
        value = near[c].astype(F32)
        inverse = lax.rsqrt(jnp.mean(value * value, -1, keepdims=True) + EPS)
        near[c] = (value * inverse * gains[0:1, :]).astype(BF16)
        out(c).start()
        here = pl.ds(pl.multiple_of(c * tok, tok), tok)
        total = jnp.zeros((tok, w_head.shape[3]), F32)
        for k in range(n):
            for x in range(f):
                start = (k * f + x) * rows
                if (k * f + x) % (256 // rows):
                    continue
                wide_rows = 256 // rows
                if wide_rows <= f:
                    right = w_head[k, x : x + wide_rows]
                else:
                    right = w_head[k : k + wide_rows // f]
                right = right.reshape(256, w_head.shape[3])
                total = total + dot(near[c, :, start : start + 256], right, MATMUL)
        mixed[here, :] = total
        return carry

    lax.fori_loop(0, n, project, 0)
    for c in range(n):
        out(c).wait()
    gather_out.finish()
    for over in range(1, f):
        row(over).wait_send()
        for kind in (0, 1):
            for part in range(ring.chips):
                wide(kind, part, over).wait()


def first_gather(n, f, own, by_head, small, routes, w_out, w_gate, w_up):
    tok, width = own.shape
    experts = by_head.shape[0]
    kind = pltpu.SemaphoreType.DMA
    shape = jax.ShapeDtypeStruct
    return pl.pallas_call(
        partial(first_kernel, n, f),
        out_shape=[
            shape((n, tok, width), BF16),
            shape((n * tok, by_head.shape[2]), F32),
            shape((n, f) + by_head.shape[1:], BF16),
            shape((experts, width), BF16),
            shape((8, width), F32),
            shape((n,) + routes.shape, jnp.int32),
            shape((max(f - 1, 1),) + w_up.shape, BF16),
            shape((max(f - 1, 1),) + w_up.shape, BF16),
            shape((n, f * w_out.shape[0], w_out.shape[1]), BF16),
        ],
        in_specs=[VMEM] * 5 + [ANY] * 2,
        out_specs=[ANY] + [VMEM] * 4 + [ANY] * 4,
        scratch_shapes=[
            pltpu.VMEM((n, tok, width), BF16),
            pltpu.VMEM((n, f) + small.shape, BF16),
            pltpu.VMEM((f * w_out.shape[0], w_out.shape[1]), BF16),
        ]
        + Gather.semaphores(n)
        + Gather.semaphores(n)
        + [kind((3, n)), kind((3, n)), kind((2, n, f)), kind((2, n, f)), kind((4,))]
        + [kind((2, n // 2, f)), kind((2, n // 2, f)), kind((f,)), kind((f,)), kind((n,))],
        compiler_params=pltpu.CompilerParams(
            collective_id=0, has_side_effects=True, vmem_limit_bytes=56 << 20
        ),
        name="first_gather",
    )(own, by_head, small, routes, w_out, w_gate, w_up)


def blocks_of(length):
    block = min(512, length)
    return block, length // block


def across_lanes(value):
    ones = jnp.ones((8, value.shape[1]), F32)
    total = lax.dot_general(
        ones, value, BY_LAST, precision=lax.Precision.HIGHEST, preferred_element_type=F32
    )
    return total[0:1, :]


def to_column(table, index, lanes):
    rows = lax.broadcasted_iota(jnp.int32, (table.shape[0], lanes), 0)
    chosen = jnp.where(rows == index, 1.0, 0.0)
    return lax.dot_general(
        table, chosen, BY_FIRST, precision=lax.Precision.HIGHEST, preferred_element_type=F32
    )


def half_turn(value, first_sign):
    half = value.shape[1] // 2
    lanes = lax.broadcasted_iota(jnp.int32, value.shape, 1)
    sign = jnp.where(lanes < half, first_sign, -first_sign)
    return pltpu.roll(value, half, 1) * sign


class Spread:
    def __init__(self, ring, block, out, sems):
        self.ring, self.block, self.out = ring, block, out
        self.send, self.recv, self.keep = sems

    @staticmethod
    def semaphores(n):
        kind = pltpu.SemaphoreType.DMA
        return [kind((n,)), kind((n,)), kind((1,))]

    def push(self, step):
        return remote(
            self.block,
            self.out.at[self.ring.me],
            self.send.at[step],
            self.recv.at[step],
            {"seq": self.ring.peer(step)},
        )

    def local(self):
        return pltpu.make_async_copy(self.block, self.out.at[self.ring.me], self.keep.at[0])

    def begin(self):
        for step in range(1, self.ring.n):
            self.push(step).start()
        self.local().start()

    def finish(self):
        for step in range(1, self.ring.n):
            self.push(step).wait()
        self.local().wait()

    def total(self):
        total = self.out[0]
        for device in range(1, self.ring.n):
            total = total + self.out[device]
        return total


def attention_kernel(n, f, factor, *refs):
    mixed, tables, starts, gains, upstream = refs[:5]
    q_ref, k_ref, v_ref, out_ref, exact_ref, sums_ref, squares = refs[5:12]
    cosine, sine, upstream_all = refs[12:15]
    partial_sums, arrived = refs[15:17]
    sems, walk_sems = refs[17:20], refs[20:]
    ring = Ring(n, f)
    length, head = q_ref.shape
    width = head * n
    block, count = blocks_of(length)
    greet(ring, True, False)
    walk = Gather(ring, upstream, upstream_all, walk_sems)
    walk.begin()
    last = walk.last
    tok = tables.shape[1]

    def measure(b, carry):
        here = pl.ds(pl.multiple_of(b * block, block), block)
        for kind in (0, 1):
            raw = mixed[here, kind * head : (kind + 1) * head]
            partial_sums[pl.ds(kind * count + b, 1), :] = across_lanes(raw * raw)
        v_ref[here, :] = mixed[here, 2 * head :].astype(BF16)
        return carry

    lax.fori_loop(0, count, measure, 0)
    spread = Spread(ring, partial_sums, arrived, sems)
    spread.begin()

    def angles(c, carry):
        here = pl.ds(pl.multiple_of(c * tok, tok), tok)
        cosine[here, :] = starts[0, c] * tables[0] - starts[1, c] * tables[1]
        sine[here, :] = starts[1, c] * tables[0] + starts[0, c] * tables[1]
        return carry

    lax.fori_loop(0, n, angles, 0)
    spread.finish()
    squares[...] = spread.total()
    walk.pass_on(0)

    def prepare(b, carry):
        here = pl.ds(pl.multiple_of(b * block, block), block)
        for kind, target in ((0, q_ref), (1, k_ref)):
            inverse = lax.rsqrt(to_column(squares[...], kind * count + b, head) / width + EPS)
            raw = mixed[here, kind * head : (kind + 1) * head]
            normed = raw * inverse * gains[kind + 1 : kind + 2, :]
            turned = half_turn(normed, -1.0)
            target[here, :] = (normed * cosine[here, :] + turned * sine[here, :]).astype(BF16)
        return carry

    lax.fori_loop(0, count, prepare, 0)
    rows = lax.broadcasted_iota(jnp.int32, (block, block), 0)
    cols = lax.broadcasted_iota(jnp.int32, (block, block), 1)

    def outer(i, carry):
        here = pl.ds(pl.multiple_of(i * block, block), block)
        part = q_ref[here, :]

        def inner(j, state, masked):
            top, total, acc = state
            there = pl.ds(pl.multiple_of(j * block, block), block)
            scores = dot(part, k_ref[there, :], BY_LAST) * factor
            if masked:
                scores = jnp.where(cols <= rows, scores, NEG)
            new = jnp.maximum(top, jnp.max(scores, -1, keepdims=True))
            scale = jnp.exp(top - new)
            expd = jnp.exp(scores - new)
            total = total * scale + jnp.sum(expd, -1, keepdims=True)
            acc = acc * scale + dot(expd.astype(BF16), v_ref[there, :], MATMUL)
            return new, total, acc

        state = (
            jnp.full((block, 1), NEG, F32),
            jnp.zeros((block, 1), F32),
            jnp.zeros((block, head), F32),
        )
        state = lax.fori_loop(0, i, lambda j, s: inner(j, s, False), state)
        top, total, acc = inner(i, state, True)
        exact = acc / total
        exact_ref[here, :] = exact
        out_ref[here, :] = exact.astype(BF16)
        column = jnp.broadcast_to(top + jnp.log(total), (block, 128))
        sums_ref[:, here] = jnp.transpose(column)[0:8, :]

        @pl.when((i > 0) & (i < last))
        def _():
            walk.pass_on(i)

        return carry

    lax.fori_loop(0, count, outer, 0)
    for i in range(count, last):
        walk.pass_on(i)
    walk.finish()


def attention(n, f, mixed, tables, starts, gains, upstream, factor):
    length, head = mixed.shape[0], mixed.shape[1] // 3
    block, count = blocks_of(length)
    shape = jax.ShapeDtypeStruct
    return pl.pallas_call(
        partial(attention_kernel, n, f, factor),
        out_shape=[
            shape((length, head), BF16),
            shape((length, head), BF16),
            shape((length, head), BF16),
            shape((length, head), BF16),
            shape((length, head), F32),
            shape((8, length), F32),
            shape((2 * count, block), F32),
            shape((length, head), F32),
            shape((length, head), F32),
            shape((n,) + upstream.shape, BF16),
        ],
        in_specs=[VMEM] * 5,
        out_specs=[VMEM] * 9 + [ANY],
        scratch_shapes=[
            pltpu.VMEM((2 * count, block), F32),
            pltpu.VMEM((n, 2 * count, block), F32),
        ]
        + Spread.semaphores(n)
        + Gather.semaphores(n),
        compiler_params=pltpu.CompilerParams(
            collective_id=5, has_side_effects=True, vmem_limit_bytes=40 << 20
        ),
        cost_estimate=pl.CostEstimate(
            flops=2 * length * length * head,
            transcendentals=length * length // 2,
            bytes_accessed=8 * length * head,
        ),
        name="attention",
    )(mixed, tables, starts, gains, upstream)


def attention_back_kernel(n, f, factor, *refs):
    q_ref, k_ref, v_ref, d_ref, sums_ref, exact, mixed, cosine, sine, gains, squares = refs[:11]
    d_attn = refs[11]
    far = refs[12:15]
    d_mixed, gain_head, d_attn_all, third, qkv_part = refs[15:20]
    dq_ref, dk_ref, dv_ref, delta, partial_sums, arrived = refs[20:26]
    near = refs[26:29]
    d_in, inner_in, hidden = near
    walk_sems, spread_sems, load_sem = refs[29:34], refs[34:37], refs[37]
    ring = Ring(n, f)
    length, head = q_ref.shape
    width = head * n
    block, count = blocks_of(length)
    greet(ring, True, False)
    walk = Gather(ring, d_attn, d_attn_all, walk_sems)
    walk.begin()
    last = walk.last
    loads = [
        pltpu.make_async_copy(source, target, load_sem.at[k])
        for k, (source, target) in enumerate(zip(far, near))
    ]
    for load in loads:
        load.start()
    dq_ref[...] = jnp.zeros_like(dq_ref)

    def measure(b, carry):
        here = pl.ds(pl.multiple_of(b * block, block), block)
        value = across_lanes(d_ref[here, :].astype(F32) * exact[here, :])
        delta[:, here] = jnp.broadcast_to(value, (8, block))
        return carry

    lax.fori_loop(0, count, measure, 0)
    rows = lax.broadcasted_iota(jnp.int32, (block, block), 0)
    cols = lax.broadcasted_iota(jnp.int32, (block, block), 1)

    def outer(j, carry):
        there = pl.ds(pl.multiple_of(j * block, block), block)
        keys = k_ref[there, :]
        values = v_ref[there, :]

        def inner(i, state, masked):
            d_keys, d_values = state
            here = pl.ds(pl.multiple_of(i * block, block), block)
            part = q_ref[here, :]
            d_part = d_ref[here, :]
            scores = dot(keys, part, BY_LAST) * factor
            if masked:
                scores = jnp.where(rows <= cols, scores, NEG)
            probs = jnp.exp(scores - sums_ref[0:1, here])
            d_probs = dot(values, d_part, BY_LAST)
            d_scores = (probs * (d_probs - delta[0:1, here])).astype(BF16)
            d_values = d_values + dot(probs.astype(BF16), d_part, MATMUL)
            d_keys = d_keys + dot(d_scores, part, MATMUL)
            dq_ref[here, :] += dot(d_scores, keys, BY_FIRST)
            return d_keys, d_values

        zero = jnp.zeros((block, head), F32)
        state = inner(j, (zero, zero), True)
        state = lax.fori_loop(j + 1, count, lambda i, s: inner(i, s, False), state)
        dk_ref[there, :] = state[0]
        dv_ref[there, :] = state[1]

        @pl.when((j >= 1) & (j < last + 1))
        def _():
            walk.pass_on(j - 1)

        return carry

    lax.fori_loop(0, count, outer, 0)

    def unturn(b, carry):
        here = pl.ds(pl.multiple_of(b * block, block), block)
        for kind, source in ((0, dq_ref), (1, dk_ref)):
            grad = (source[here, :] * factor).astype(BF16).astype(F32)
            grad = grad * cosine[here, :] + half_turn(grad * sine[here, :], 1.0)
            source[here, :] = grad
            raw = mixed[here, kind * head : (kind + 1) * head]
            partial_sums[pl.ds(kind * count + b, 1), :] = across_lanes(
                raw * gains[kind + 1 : kind + 2, :] * grad
            )
        return carry

    lax.fori_loop(0, count, unturn, 0)
    spread = Spread(ring, partial_sums, arrived, spread_sems)
    spread.begin()
    walk.pass_on(count - 1)
    units = third.shape[2]
    for load in loads:
        load.wait()

    def products(tile, tiles):
        size = d_in.shape[1] // tiles
        these = pl.ds(pl.multiple_of(tile * size, size), size)
        for j in range(1, f):
            part = slice(j * units, (j + 1) * units)
            third[j - 1, these, :] = dot(d_in[:, these], inner_in[:, part], BY_FIRST).astype(BF16)

    def some(tile, carry):
        products(tile, 8)
        return carry

    spread.finish()
    total = spread.total()
    gain_head[...] = jnp.zeros_like(gain_head)

    def close(b, carry):
        here = pl.ds(pl.multiple_of(b * block, block), block)
        for kind, source in ((0, dq_ref), (1, dk_ref)):
            index = kind * count + b
            inverse = lax.rsqrt(to_column(squares[...], index, head) / width + EPS)
            inner = to_column(total, index, head) / width
            raw = mixed[here, kind * head : (kind + 1) * head]
            grad = source[here, :]
            value = inverse * gains[kind + 1 : kind + 2, :] * grad
            value = value - raw * (inverse * inverse * inverse) * inner
            d_mixed[here, kind * head : (kind + 1) * head] = value.astype(BF16)
            gain_head[kind + 2 : kind + 3, :] += jnp.sum(raw * inverse * grad, 0, keepdims=True)
        d_mixed[here, 2 * head :] = dv_ref[here, :].astype(BF16)
        return carry

    lax.fori_loop(0, count, close, 0)
    walk.pass_on(count)
    chunks, beside, rows_each = qkv_part.shape[1], qkv_part.shape[0], qkv_part.shape[2]
    span = width // chunks

    def weigh(c, carry):
        these = pl.ds(pl.multiple_of(c * span, span), span)
        value = dot(hidden[:, these], d_mixed[...], BY_FIRST).astype(BF16)
        for x in range(beside):
            qkv_part[x, c] = value[x * rows_each : (x + 1) * rows_each]
        return carry

    lax.fori_loop(0, chunks, weigh, 0)
    for i in range(count + 1, last):
        walk.pass_on(i)
        if i == count + 1:
            lax.fori_loop(0, 8, some, 0)
    walk.finish()


def attention_back(
    n, f, queries, keys, values, d_out, sums, exact, mixed, cosine, sine, gains, squares,
    d_attn, d_in, inner_in, hidden, rows, factor
):
    length, head = queries.shape
    tok, width = d_attn.shape
    block, count = blocks_of(length)
    shape = jax.ShapeDtypeStruct
    units = inner_in.shape[1] // f
    grad = shape((max(f - 1, 1), width, units), BF16)
    return pl.pallas_call(
        partial(attention_back_kernel, n, f, factor),
        out_shape=[
            shape((length, 3 * head), BF16),
            shape((8, head), F32),
            shape((n, tok, width), BF16),
            grad,
            shape((f, n, rows, 3 * head), BF16),
        ],
        in_specs=[VMEM] * 12 + [ANY] * 3,
        out_specs=[VMEM, VMEM, ANY] + [VMEM] * 2,
        scratch_shapes=[pltpu.VMEM((length, head), F32)] * 3
        + [
            pltpu.VMEM((8, length), F32),
            pltpu.VMEM((2 * count, block), F32),
            pltpu.VMEM((n, 2 * count, block), F32),
            pltpu.VMEM(d_in.shape, BF16),
            pltpu.VMEM(inner_in.shape, BF16),
            pltpu.VMEM(hidden.shape, BF16),
        ]
        + Gather.semaphores(n)
        + Spread.semaphores(n)
        + [pltpu.SemaphoreType.DMA((3,))],
        compiler_params=pltpu.CompilerParams(
            collective_id=6, has_side_effects=True, vmem_limit_bytes=64 << 20
        ),
        name="attention_back",
    )(
        queries, keys, values, d_out, sums, exact, mixed, cosine, sine, gains, squares,
        d_attn, d_in, inner_in, hidden
    )


def core_kernel(n, f, *refs):
    attended, w_out, tokens, upstream, gain, router, routes, routes_all, upstream_all = refs[:9]
    shards_in = refs[9 : 9 + 3 * f]
    refs = refs[9 + 3 * f :]
    d_middle, middle, d_attn, d_attended, d_logits_all, gain_two = refs[:6]
    own_hidden, rows_out, d_out, inner_out, d_gate_out, d_up_out, moe_out = refs[6:13]
    refs = refs[13:]
    w_near, w_gate, w_up, w_down, by_token, d_logits, arrived, outgoing, weights_in = refs[:9]
    refs = refs[9:]
    ring_in, mate_near, d_mate_in, coming, going, d_mate_out, own, lift = refs[:8]
    refs = refs[8:]
    rows_now, lifted, d_now, inner_now, d_gate_now, d_up_now, moe_now, d_weight, places = refs[:9]
    refs = refs[9:]
    hop_send, hop_recv, share_send, share_recv, swap_send, swap_recv = refs[:6]
    sum_send, sum_recv, send, recv, keep, load_sem, lift_sem, stage_sem, own_sem = refs[6:]
    ring = Ring(n, f)
    tok, width = tokens.shape
    head = width // n
    chips = ring.chips
    last = chips - 1
    capacity = rows_now.shape[1] // 2
    hidden_units = w_gate.shape[1]
    piece = tok // PIECES
    sign = 1 - 2 * ring.core
    onward = ring.at(ring.pos + sign + chips)
    local_units = hidden_units // f

    loads = [pltpu.make_async_copy(w_out, w_near, keep.at[0])]
    for kind, target in enumerate((w_gate, w_up, w_down)):
        for j in range(f):
            cols = slice(j * local_units, (j + 1) * local_units)
            loads.append(
                pltpu.make_async_copy(
                    shards_in[kind * f + j], target.at[:, cols], load_sem.at[kind, j]
                )
            )
    for load in loads:
        load.start()

    def chunk_of(i, other):
        return ring.at(
            ring.pos + (sign * (1 + i) if other else -sign * (1 + i)) + 2 * chips, other
        )

    def lift_copy(i, other):
        slot = lax.rem(i, 2)
        return pltpu.make_async_copy(
            upstream_all.at[chunk_of(i, other)],
            lift.at[slot, other],
            lift_sem.at[slot, other],
        )

    lift_copy(0, 0).start()
    lift_copy(0, 1).start()
    greet(ring, True, False)

    def deal(step):
        cols = pl.ds(pl.multiple_of(ring.me * head, head), head)
        there = ring.peer(step)
        return remote(
            attended.at[there],
            by_token.at[:, cols],
            send.at[0, step],
            recv.at[0, step],
            {"seq": there},
        )

    for step in range(1, n):
        deal(step).start()
    mine = pl.ds(pl.multiple_of(ring.me * head, head), head)
    by_token[:, mine] = attended[ring.me]

    before = lax.broadcasted_iota(jnp.int32, (tok, tok), 0)
    after = lax.broadcasted_iota(jnp.int32, (tok, tok), 1)
    earlier = jnp.where(before < after, 1.0, 0.0).astype(BF16)
    for c in range(n):
        here = jnp.where(routes_all[c] == ring.me, 1.0, 0.0)
        here = jnp.sum(here, 0, keepdims=True)
        count = dot(jnp.broadcast_to(here, (8, tok)).astype(BF16), earlier, MATMUL)
        places[c] = jnp.where(jnp.broadcast_to(here, (8, tok)) > 0.5, count, -1.0)

    loads[0].wait()
    for step in range(1, n):
        deal(step).wait()
    tile = min(512, width)
    squares = jnp.zeros((tok, 1), F32)
    for start in range(0, width, tile):
        cols = slice(start, start + tile)
        value = tokens[:, cols].astype(F32) + dot(by_token[...], w_near[:, cols], MATMUL)
        middle[:, cols] = value
        squares = squares + jnp.sum(value * value, -1, keepdims=True)
    inverse = lax.rsqrt(squares / width + EPS)
    ring_in[last] = (middle[...] * inverse * gain[...]).astype(BF16)

    def hop(i, s):
        rows = pl.ds(s * piece, piece)
        source = lax.rem(i + last, chips)
        return remote(
            ring_in.at[source, rows],
            ring_in.at[i, rows],
            hop_send.at[i, s],
            hop_recv.at[i, s],
            {"seq": onward},
        )

    def share(i, s):
        rows = pl.ds(s * piece, piece)
        return remote(
            ring_in.at[i, rows],
            mate_near.at[i, rows],
            share_send.at[i, s],
            share_recv.at[i, s],
            {"seq": ring.mate},
        )

    for s in range(PIECES):
        hop(0, s).start()
    for s in range(PIECES):
        share(last, s).start()

    logits = dot(router[...], ring_in[last], BY_LAST)
    expd = jnp.exp(logits - jnp.max(logits, 0, keepdims=True))
    gate = expd / jnp.sum(expd, 0, keepdims=True)
    experts = lax.broadcasted_iota(jnp.int32, gate.shape, 0)
    named = jnp.zeros(gate.shape, F32)
    for k in range(routes.shape[0]):
        named = named + jnp.where(routes[k : k + 1, :] == experts, 1.0, 0.0)
    weights = gate * named
    for e in range(n):
        outgoing[e] = jnp.broadcast_to(weights[e : e + 1, :], (8, tok))

    def push(there):
        return remote(
            outgoing.at[there],
            weights_in.at[ring.me],
            send.at[1, there],
            recv.at[1, ring.me],
            {"seq": there},
        )

    def pushed(origin):
        return remote(
            outgoing.at[origin],
            weights_in.at[origin],
            send.at[1, origin],
            recv.at[1, origin],
            {"seq": origin},
        )

    for step in range(1, n):
        push(ring.peer(step)).start()
    weights_in[ring.me] = outgoing[ring.me]
    for load in loads[1:]:
        load.wait()

    def swap(i):
        return remote(
            d_mate_out.at[lax.rem(i, 2)],
            d_mate_in.at[i],
            swap_send.at[i],
            swap_recv.at[i],
            {"seq": ring.mate},
        )

    def sum_hop(i, s):
        rows = pl.ds(s * piece, piece)
        return remote(
            going.at[lax.rem(i, 2), rows],
            coming.at[i, rows],
            sum_send.at[i, s],
            sum_recv.at[i, s],
            {"seq": onward},
        )

    def sum_step(i):
        swap(i).wait_recv()

        @pl.when(i >= 2)
        def _():
            for s in range(PIECES):
                sum_hop(i - 2, s).wait_send()

        for s in range(PIECES):
            rows = pl.ds(s * piece, piece)

            @pl.when(i > 0)
            def _():
                sum_hop(i - 1, s).wait_recv()
                own[rows, :] = own[rows, :] + coming[i - 1, rows].astype(F32)

            value = own[rows, :] + d_mate_in[i, rows].astype(F32)
            going[lax.rem(i, 2), rows] = value.astype(BF16)
            sum_hop(i, s).start()

    def give(kind, target, other, slot):
        chunk = target
        source, sink = [
            (rows_now, rows_out),
            (d_now, d_out),
            (inner_now, inner_out),
            (d_gate_now, d_gate_out),
            (d_up_now, d_up_out),
            (moe_now, moe_out),
        ][kind]
        size = tok if kind == 5 else capacity
        return pltpu.make_async_copy(
            source.at[slot, pl.ds(other * size, size)],
            sink.at[chunk],
            stage_sem.at[slot, kind, other],
        )

    def keep_hidden(i, other):
        return pltpu.make_async_copy(
            (mate_near if other else ring_in).at[i, :, mine],
            own_hidden.at[chunk_of(i, other)],
            own_sem.at[other, i],
        )

    def report(there, slot, other):
        return remote(
            d_weight.at[slot, other],
            arrived.at[ring.me],
            send.at[2, there],
            recv.at[2, ring.me],
            {"seq": there},
        )

    def reported(origin):
        return remote(
            d_weight.at[0, 0],
            arrived.at[origin],
            send.at[2, origin],
            recv.at[2, origin],
            {"seq": origin},
        )

    def pass_on(i):
        for s in range(PIECES):
            hop(i, s).wait_recv()

            @pl.when(i < last - 1)
            def _():
                hop(i + 1, s).start()

            share(i, s).start()

    def work(i):
        slot = lax.rem(i, 2)
        chunks = (chunk_of(i, 0), chunk_of(i, 1))
        for s in range(PIECES):
            share(i, s).wait_recv()
        keep_hidden(i, 0).start()
        keep_hidden(i, 1).start()
        for other in (0, 1):
            lift_copy(i, other).wait()

        @pl.when(i < last)
        def _():
            lift_copy(i + 1, 0).start()
            lift_copy(i + 1, 1).start()
            pushed(chunks[0]).wait_recv()

        pushed(chunks[1]).wait_recv()

        @pl.when(i >= 2)
        def _():
            for kind in range(6):
                for other in (0, 1):
                    give(kind, chunks[other], other, slot).wait()
            swap(i - 2).wait_send()
            for other in (0, 1):
                report(chunk_of(i - 2, other), slot, other).wait_send()

        slots = lax.broadcasted_iota(jnp.int32, (capacity, tok), 0).astype(F32)
        picks, rates = [], []
        for other in (0, 1):
            rows = slice(other * capacity, (other + 1) * capacity)
            where = slots == jnp.broadcast_to(places[chunks[other], 0:1, :], (capacity, tok))
            pick = jnp.where(where, 1.0, 0.0)
            low = pick.astype(BF16)
            source = mate_near.at[i] if other else ring_in.at[i]
            share_of = weights_in[chunks[other], 0:1, :]
            rate = jnp.sum(jnp.where(where, share_of, 0.0), -1, keepdims=True)
            for start in range(0, width, tile):
                cols = slice(start, start + tile)
                rows_now[slot, rows, cols] = dot(low, source[:, cols], MATMUL).astype(BF16)
                picked = dot(low, lift[slot, other, :, cols], MATMUL)
                lifted[rows, cols] = picked.astype(BF16)
                d_now[slot, rows, cols] = (rate * picked).astype(BF16)
            picks.append((low, where))
            rates.append(rate)
        rate = jnp.concatenate(rates, 0)
        unit = min(256, hidden_units)
        for start in range(0, hidden_units, unit):
            cols = slice(start, start + unit)
            gate_act = dot(rows_now[slot], w_gate[:, cols], MATMUL)
            up_act = dot(rows_now[slot], w_up[:, cols], MATMUL)
            d_inner = dot(d_now[slot], w_down[:, cols], MATMUL)
            sigma = 1.0 / (1.0 + jnp.exp(-gate_act))
            silu = gate_act * sigma
            inner_now[slot, :, cols] = (silu * up_act).astype(BF16)
            d_gate_now[slot, :, cols] = (
                d_inner * up_act * sigma * (1.0 + gate_act * (1.0 - sigma))
            ).astype(BF16)
            d_up_now[slot, :, cols] = (d_inner * silu).astype(BF16)
        inner_product = jnp.zeros((2 * capacity, 1), F32)
        for start in range(0, width, tile):
            cols = slice(start, start + tile)
            produced = dot(inner_now[slot], w_down[cols, :], BY_LAST)
            produced = produced.astype(BF16).astype(F32)
            inner_product = inner_product + jnp.sum(
                produced * lifted[:, cols].astype(F32), -1, keepdims=True
            )
            scaled = (rate * produced).astype(BF16)
            d_rows = dot(d_gate_now[slot], w_gate[cols, :], BY_LAST)
            d_rows = (d_rows + dot(d_up_now[slot], w_up[cols, :], BY_LAST)).astype(BF16)
            for other in (0, 1):
                rows = slice(other * capacity, (other + 1) * capacity)
                low = picks[other][0]
                moe_now[slot, other * tok : (other + 1) * tok, cols] = dot(
                    low, scaled[rows], BY_FIRST
                ).astype(BF16)
                spread_rows = dot(low, d_rows[rows], BY_FIRST)
                if other:
                    d_mate_out[slot, :, cols] = spread_rows.astype(BF16)
                else:
                    own[:, cols] = spread_rows
        swap(i).start()
        for kind in range(6):
            for other in (0, 1):
                give(kind, chunks[other], other, slot).start()
        for other in (0, 1):
            rows = slice(other * capacity, (other + 1) * capacity)
            value = jnp.sum(
                jnp.where(picks[other][1], inner_product[rows], 0.0), 0, keepdims=True
            )
            d_weight[slot, other] = jnp.broadcast_to(value, (8, tok))
        report(chunks[1], slot, 1).start()

        @pl.when(i < last)
        def _():
            report(chunks[0], slot, 0).start()

    pass_on(0)
    work(0)

    def body(i, carry):
        @pl.when(i < last)
        def _():
            pass_on(i)

        sum_step(i - 1)
        work(i)
        return carry

    lax.fori_loop(1, chips, body, 0)
    arrived[ring.me] = d_weight[last % 2, 0]
    for step in range(1, n):
        reported(ring.peer(step)).wait_recv()
    gate_back = jnp.concatenate([arrived[e, 0:1, :] for e in range(n)], 0)
    gate_back = gate * (gate_back - jnp.sum(gate * gate_back, 0, keepdims=True))
    d_logits[...] = gate_back.astype(BF16)

    def publish(step):
        return remote(
            d_logits,
            d_logits_all.at[ring.me],
            send.at[4, step],
            recv.at[4, step],
            {"seq": ring.peer(step)},
        )

    kept = pltpu.make_async_copy(d_logits, d_logits_all.at[ring.me], keep.at[1])
    swap(last).wait_recv()
    for s in range(PIECES):
        rows = pl.ds(s * piece, piece)
        sum_hop(last - 1, s).wait_recv()
        value = own[rows, :] + d_mate_in[last, rows].astype(F32)
        own[rows, :] = value + coming[last - 1, rows].astype(F32)
    d_hidden = own[...] + dot(gate_back.astype(BF16), router[...], BY_FIRST)
    value = middle[...]
    inner = jnp.mean(value * gain[...] * d_hidden, -1, keepdims=True)
    gain_two[...] = jnp.sum(value * inverse * d_hidden, 0, keepdims=True)
    d_value = inverse * gain[...] * d_hidden - value * (inverse * inverse * inverse) * inner
    d_value = upstream[...].astype(F32) + d_value
    d_middle[...] = d_value
    d_attn[...] = d_value.astype(BF16)
    for start in range(0, width, tile):
        cols = slice(start, start + tile)
        by_token[:, cols] = dot(d_attn[...], w_near[cols, :], BY_LAST).astype(BF16)

    def deal_back(step):
        there = ring.peer(step)
        cols = pl.ds(pl.multiple_of(there * head, head), head)
        return remote(
            by_token.at[:, cols],
            d_attended.at[ring.me],
            send.at[3, step],
            recv.at[3, step],
            {"seq": there},
        )

    for step in range(1, n):
        deal_back(step).start()
    d_attended[ring.me] = by_token[:, mine]
    for step in range(1, n):
        publish(step).start()
    kept.start()

    for s in range(PIECES):
        share(last, s).wait_send()

    def settle(i, carry):
        for s in range(PIECES):
            hop(i, s).wait_send()
            share(i, s).wait_send()
        for other in (0, 1):
            keep_hidden(i, other).wait()
        return carry

    lax.fori_loop(0, last, settle, 0)
    for other in (0, 1):
        keep_hidden(last, other).wait()
    for s in range(PIECES):
        sum_hop(last - 2, s).wait_send()
        sum_hop(last - 1, s).wait_send()
    for i in (last - 1, last):
        swap(i).wait_send()
        for other in (0, 1):
            for kind in range(6):
                give(kind, chunk_of(i, other), other, i % 2).wait()
            if other or i < last:
                report(chunk_of(i, other), i % 2, other).wait_send()
    for step in range(1, n):
        push(ring.peer(step)).wait_send()
    for step in range(1, n):
        deal_back(step).wait()
        publish(step).wait()
    kept.wait()


def core_stage(
    n, f, attended, w_out, tokens, upstream, gain, router, routes, routes_all, upstream_all, halves
):
    tok, width = tokens.shape
    experts = router.shape[0]
    units = f * halves[0].shape[1]
    capacity = min(tok, 5 * tok * TOPK // (4 * experts))
    chips = n // 2
    kind = pltpu.SemaphoreType.DMA
    shape = jax.ShapeDtypeStruct
    rows = 2 * capacity
    return pl.pallas_call(
        partial(core_kernel, n, f),
        out_shape=[
            shape((tok, width), F32),
            shape((tok, width), F32),
            shape((tok, width), BF16),
            shape((n, tok, width // n), BF16),
            shape((n, experts, tok), BF16),
            shape((1, width), F32),
            shape((n, tok, width // n), BF16),
            shape((n, capacity, width), BF16),
            shape((n, capacity, width), BF16),
            shape((n, capacity, units), BF16),
            shape((n, capacity, units), BF16),
            shape((n, capacity, units), BF16),
            shape((n, tok, width), BF16),
        ],
        in_specs=[VMEM, ANY] + [VMEM] * 6 + [ANY] * (1 + 3 * f),
        out_specs=[VMEM] * 4 + [ANY, VMEM] + [ANY] * 7,
        scratch_shapes=[
            pltpu.VMEM((width, width), BF16),
            pltpu.VMEM((width, units), BF16),
            pltpu.VMEM((width, units), BF16),
            pltpu.VMEM((width, units), BF16),
            pltpu.VMEM((tok, width), BF16),
            pltpu.VMEM((experts, tok), BF16),
            pltpu.VMEM((n, 8, tok), F32),
            pltpu.VMEM((n, 8, tok), F32),
            pltpu.VMEM((n, 8, tok), F32),
            pltpu.VMEM((chips, tok, width), BF16),
            pltpu.VMEM((chips, tok, width), BF16),
            pltpu.VMEM((chips, tok, width), BF16),
            pltpu.VMEM((chips - 1, tok, width), BF16),
            pltpu.VMEM((2, tok, width), BF16),
            pltpu.VMEM((2, tok, width), BF16),
            pltpu.VMEM((tok, width), F32),
            pltpu.VMEM((2, 2, tok, width), BF16),
            pltpu.VMEM((2, rows, width), BF16),
            pltpu.VMEM((rows, width), BF16),
            pltpu.VMEM((2, rows, width), BF16),
            pltpu.VMEM((2, rows, units), BF16),
            pltpu.VMEM((2, rows, units), BF16),
            pltpu.VMEM((2, rows, units), BF16),
            pltpu.VMEM((2, 2 * tok, width), BF16),
            pltpu.VMEM((2, 2, 8, tok), F32),
            pltpu.VMEM((n, 8, tok), F32),
            kind((chips, PIECES)),
            kind((chips, PIECES)),
            kind((chips, PIECES)),
            kind((chips, PIECES)),
            kind((chips,)),
            kind((chips,)),
            kind((chips, PIECES)),
            kind((chips, PIECES)),
            kind((5, n)),
            kind((5, n)),
            kind((2,)),
            kind((3, f)),
            kind((2, 2)),
            kind((2, 6, 2)),
            kind((2, chips)),
        ],
        compiler_params=pltpu.CompilerParams(
            collective_id=1, has_side_effects=True, vmem_limit_bytes=67_000_000
        ),
        name="core_stage",
    )(attended, w_out, tokens, upstream, gain, router, routes, routes_all, upstream_all, *halves)


def last_kernel(n, f, *refs):
    d_mixed, w_head, qkv_part, tokens, gain, d_middle, gain_two, gain_head = refs[:8]
    middle, third, moe_part = refs[8:11]
    far_refs = refs[11:16]
    d_inputs, qkv_rows, gains_out, third_in, grads_out, result = refs[16:22]
    beside_rows, summed, gain_rows, gain_in, gain_side, stage = refs[22:28]
    near_refs = refs[28:33]
    rows_in, d_in, d_gate, d_up, inner_in = near_refs
    buffers, fold_sems = refs[33:38], refs[38:42]
    stored_buffers, stored_sems = refs[42:46], refs[46:51]
    side_send, side_recv, send, recv, keep, stage_sem, load_sem = refs[51:]
    ring = Ring(n, f)
    _, width = tokens.shape
    slice_width = width // n
    units = grads_out.shape[2]
    chips = ring.chips
    size = width // chips
    loads = [
        pltpu.make_async_copy(source if k < 2 else source.at[:, :units], target, load_sem.at[k])
        for k, (source, target) in enumerate(zip(far_refs, near_refs))
    ]
    greet(ring, True, True)

    def side(step):
        there = ring.beside(step)
        return remote(
            qkv_part.at[there],
            beside_rows.at[step - 1],
            side_send.at[0, step],
            side_recv.at[0, step],
            {"fsdp": there},
        )

    for step in range(1, f):
        side(step).start()

    def part(chunk, target):
        tile = min(512, width)
        for start in range(0, width, tile):
            cols = slice(start, start + tile)
            target[:, cols] = dot(d_mixed[chunk], w_head[cols, :], BY_LAST).astype(target.dtype)

    fold = Fold(ring, part, buffers, fold_sems)

    def finish(rows, value):
        d_inputs[rows, :] = value

    def store(i, which):
        these = pl.ds(pl.multiple_of(i * size, size), size)
        slot = lax.rem(i, 2)
        return pltpu.make_async_copy(
            stage.at[slot, which], grads_out.at[which, these], stage_sem.at[slot, which]
        )

    def filler(i):
        these = pl.ds(pl.multiple_of(i * size, size), size)
        slot = lax.rem(i, 2)
        pairs = ((rows_in, d_gate), (rows_in, d_up), (d_in, inner_in))
        for which, (left, right) in enumerate(pairs):

            @pl.when(i >= 2)
            def _():
                store(i - 2, which).wait()

            stage[slot, which] = dot(left[:, these], right[...], BY_FIRST)
            store(i, which).start()

    def push(step):
        there = ring.peer(step)
        return remote(
            summed.at[there],
            qkv_rows.at[ring.me],
            send.at[0, step],
            recv.at[0, step],
            {"seq": there},
        )

    local = pltpu.make_async_copy(summed.at[ring.me], qkv_rows.at[ring.me], keep.at[0])

    def far(step):
        return remote(
            third.at[step - 1],
            third_in.at[step - 1],
            side_send.at[2, step],
            side_recv.at[2, step],
            {"fsdp": ring.beside(f - step)},
        )

    for step in range(1, f):
        far(step).start()
    stored = Stored(ring, moe_part, stored_buffers, stored_sems)
    fold.produce(0)
    stored.begin()
    for load in loads:
        load.start()
    fold.step(0)
    stored.step(0)
    for load in loads:
        load.wait()
    filler(0)
    fold.run(finish, filler, stored.step)

    def settle(rows, value):
        result[rows, :] = (middle[rows, :] + value).astype(BF16)

    stored.close(settle)
    value = tokens[...].astype(F32)
    grad = d_inputs[...]
    inverse = lax.rsqrt(jnp.mean(value * value, -1, keepdims=True) + EPS)
    inner = jnp.mean(value * gain[...] * grad, -1, keepdims=True)
    gain_rows[...] = jnp.zeros_like(gain_rows)
    gain_rows[0:1, :] = jnp.sum(value * inverse * grad, 0, keepdims=True)
    gain_rows[1:2, :] = gain_two[...]

    def gains(step):
        there = ring.peer(step)
        cols = pl.ds(pl.multiple_of(there * slice_width, slice_width), slice_width)
        return remote(
            gain_rows.at[:, cols],
            gain_in.at[ring.me],
            send.at[1, step],
            recv.at[1, step],
            {"seq": there},
        )

    mine = pl.ds(pl.multiple_of(ring.me * slice_width, slice_width), slice_width)
    kept = pltpu.make_async_copy(gain_rows.at[:, mine], gain_in.at[ring.me], keep.at[1])
    for step in range(1, n):
        gains(step).start()
    kept.start()
    d_value = inverse * gain[...] * grad - value * (inverse * inverse * inverse) * inner
    d_inputs[...] = d_middle[...] + d_value
    for step in range(1, f):
        side(step).wait_recv()

    def add(block, carry):
        value = qkv_part[ring.mine, block].astype(F32)
        for step in range(1, f):
            value = value + beside_rows[step - 1, block].astype(F32)
        summed[block] = value.astype(BF16)
        return carry

    lax.fori_loop(0, n, add, 0)
    for step in range(1, n):
        push(step).start()
    local.start()
    for step in range(1, n):
        gains(step).wait()
    kept.wait()
    total = gain_head[...]
    for device in range(n):
        total = total + gain_in[device]
    gain_side[0] = total

    def sums(step):
        return remote(
            gain_side.at[0],
            gain_side.at[step],
            side_send.at[1, step],
            side_recv.at[1, step],
            {"fsdp": ring.beside(step)},
        )

    for step in range(1, f):
        sums(step).start()
    fold.close()
    for i in (chips - 2, chips - 1):
        for which in range(3):
            store(i, which).wait()
    for step in range(1, f):
        side(step).wait_send()
    for step in range(1, n):
        push(step).wait()
    local.wait()
    for step in range(1, f):
        sums(step).wait()
        total = total + gain_side[step]
    gains_out[...] = total
    for step in range(1, f):
        far(step).wait()


def last_stage(
    n, f, d_mixed, w_head, qkv_part, tokens, gain, d_middle, gain_two, gain_head,
    middle, third, moe_part, rows_in, d_in, d_gate, d_up, inner_in
):
    tok, width = tokens.shape
    rows, across = qkv_part.shape[2:]
    units = third.shape[2]
    kind = pltpu.SemaphoreType.DMA
    shape = jax.ShapeDtypeStruct
    return pl.pallas_call(
        partial(last_kernel, n, f),
        out_shape=[
            shape((tok, width), F32),
            shape((n, rows, across), BF16),
            shape((8, width // n), F32),
            shape(third.shape, BF16),
            shape((3, width, units), F32),
            shape((tok, width), BF16),
        ],
        in_specs=[VMEM] * 9 + [ANY] * 7,
        out_specs=[VMEM] * 3 + [ANY] * 2 + [VMEM],
        scratch_shapes=[
            pltpu.VMEM((max(f - 1, 1), n, rows, across), BF16),
            pltpu.VMEM((n, rows, across), BF16),
            pltpu.VMEM((8, width), F32),
            pltpu.VMEM((n, 8, width // n), F32),
            pltpu.VMEM((f, 8, width // n), F32),
            pltpu.VMEM((2, 3, 2 * width // n, units), F32),
            pltpu.VMEM(rows_in.shape, BF16),
            pltpu.VMEM(rows_in.shape, BF16),
            pltpu.VMEM((rows_in.shape[0], units), BF16),
            pltpu.VMEM((rows_in.shape[0], units), BF16),
            pltpu.VMEM((rows_in.shape[0], units), BF16),
        ]
        + Fold.buffers(n, tok, width)
        + Fold.semaphores(n)
        + Stored.buffers(n, tok, width)
        + Stored.semaphores(n)
        + [kind((3, f)), kind((3, f)), kind((2, n)), kind((2, n)), kind((2,)), kind((2, 3))]
        + [kind((5,))],
        compiler_params=pltpu.CompilerParams(
            collective_id=4, has_side_effects=True, vmem_limit_bytes=67_000_000
        ),
        name="last_stage",
    )(
        d_mixed, w_head, qkv_part, tokens, gain, d_middle, gain_two, gain_head,
        middle, third, moe_part, rows_in, d_in, d_gate, d_up, inner_in
    )


def angles_of(n, tok, head_size):
    half = head_size // 2
    freqs = 10000.0 ** (-jnp.arange(half, dtype=F32) / half)
    inside = jnp.arange(tok, dtype=jnp.int32)
    starts = jnp.arange(n, dtype=jnp.int32) * tok
    angles = jnp.concatenate([inside, starts]).astype(F32)[:, None] * freqs[None, :]
    both = jnp.stack([jnp.cos(angles), jnp.sin(angles)])
    both = jnp.concatenate([both, both], -1)
    return both[:, :tok], both[:, tok:, None, :]


def shift_fsdp(values, step, f):
    if step == 0:
        return values
    return lax.ppermute(values, "fsdp", [(i, (i + step) % f) for i in range(f)])


def shards(n, f, inputs, routes, w_qkv, w_out, w_router, norm_gains, w_gate, w_up, w_down, cotangent):
    tokens_low = inputs[0]
    upstream_low = cotangent[0]
    local_routes = routes[0].T
    me = lax.axis_index("seq")
    mine = lax.axis_index("fsdp")
    tok, width = tokens_low.shape
    length = tok * n
    head_size = width // HEADS
    across = 3 * head_size
    rows = w_qkv.shape[0]
    experts = n * w_gate.shape[0]
    capacity = min(tok, 5 * tok * TOPK // (4 * experts))
    factor = head_size ** (-0.5)

    by_head = w_qkv.reshape(rows, 3, HEADS, head_size).transpose(2, 0, 1, 3)
    by_head = by_head.reshape(HEADS, rows, across)
    small = jnp.concatenate([w_router, norm_gains], 1)
    small = jnp.pad(small, ((0, 0), (0, 128 - small.shape[1])))
    (
        hidden_one,
        mixed,
        w_head,
        router,
        gains,
        routes_all,
        gate_near,
        up_near,
        w_out_all,
    ) = first_gather(n, f, tokens_low, by_head, small, local_routes, w_out, w_gate[0], w_up[0])
    w_out_all = w_out_all.reshape(width, width)
    gates = [w_gate[0]] + [gate_near[j] for j in range(f - 1)]
    ups = [w_up[0]] + [up_near[j] for j in range(f - 1)]
    w_low, _ = lax.optimization_barrier((w_down[0], mixed))
    downs = [shift_fsdp(w_low, j, f) for j in range(f)]
    hidden_one = hidden_one.reshape(length, width)
    w_head = w_head.reshape(width, across)
    own = lax.dynamic_slice_in_dim(gains, me * head_size, head_size, 1)
    tables, starts = angles_of(n, tok, head_size)
    queries, keys, values, attended, exact, sums, squares, cosine, sine, upstream_all = attention(
        n, f, mixed, tables, starts, own, upstream_low, factor
    )

    (
        d_middle,
        middle,
        d_attn,
        d_attended,
        d_logits_all,
        gain_two,
        own_hidden,
        expert_rows,
        d_produced,
        inner,
        d_gate,
        d_up,
        moe_part,
    ) = core_stage(
        n,
        f,
        attended.reshape(n, tok, head_size),
        w_out_all,
        tokens_low,
        upstream_low,
        gains[3:4],
        router,
        local_routes,
        routes_all,
        upstream_all,
        gates + ups + downs,
    )
    flat = n * capacity
    units = w_gate.shape[2]
    expert_rows = expert_rows.reshape(flat, width)
    d_produced = d_produced.reshape(flat, width)
    inner, d_gate, d_up = (v.reshape(flat, f * units) for v in (inner, d_gate, d_up))
    pairs = ((expert_rows, d_gate), (expert_rows, d_up), (d_produced, inner))

    def others(which):
        left, right = pairs[which]
        return [
            dot(left, right[:, j * units : (j + 1) * units], BY_FIRST).astype(BF16)
            for j in range(1, f)
        ]

    first, second = others(0), others(1)
    d_attended, first, second = lax.optimization_barrier((d_attended, first, second))
    first = [shift_fsdp(v, f - 1 - j, f) for j, v in enumerate(first)]
    second = [shift_fsdp(v, f - 1 - j, f) for j, v in enumerate(second)]
    d_mixed, gain_head, d_attn_all, third, qkv_part = attention_back(
        n,
        f,
        queries,
        keys,
        values,
        d_attended.reshape(length, head_size),
        sums,
        exact,
        mixed,
        cosine,
        sine,
        own,
        squares,
        d_attn,
        d_produced,
        inner,
        hidden_one,
        rows,
        factor,
    )
    d_attn_all = d_attn_all.reshape(length, width)
    proj_part = dot(attended, d_attn_all, BY_FIRST)
    router_part = jnp.einsum(
        "ntc,nkt->ck", own_hidden, d_logits_all, preferred_element_type=F32
    )
    both = jnp.concatenate([proj_part, router_part], 1).reshape(f, rows, width + experts)
    d_mixed, both = lax.optimization_barrier((d_mixed, both))
    proj = lax.dynamic_index_in_dim(both, mine, 0, keepdims=False)
    for j in range(1, f):
        part = lax.dynamic_index_in_dim(both, (mine + j) % f, 0, keepdims=False)
        proj = proj + shift_fsdp(part.astype(BF16), j, f).astype(F32)
    grad_inputs, qkv_rows, gains_own, third, grads_own, result = last_stage(
        n,
        f,
        d_mixed.reshape(n, tok, across),
        w_head,
        qkv_part,
        tokens_low,
        gains[0:1],
        d_middle,
        gain_two,
        gain_head,
        middle,
        third,
        moe_part,
        expert_rows,
        d_produced,
        d_gate,
        d_up,
        inner,
    )
    grads = []
    for which, arrived in enumerate((first, second, [third[j] for j in range(f - 1)])):
        total = grads_own[which]
        for part in arrived:
            total = total + part.astype(F32)
        grads.append(total[None])
    grad_qkv = (
        qkv_rows.reshape(HEADS, rows, 3, head_size)
        .transpose(1, 2, 0, 3)
        .reshape(rows, 3 * width)
        .astype(F32)
    )
    gains_out = jnp.stack([gains_own[0], gains_own[2], gains_own[3], gains_own[1]], 1)
    grad_gains = lax.dynamic_slice_in_dim(gains_out, mine * rows, rows, 0)
    return (
        result[None],
        grad_inputs[None],
        grad_qkv,
        proj[:, :width],
        proj[:, width:],
        grad_gains,
        *grads,
    )


def solution(mesh):
    tokens = P("fsdp", "seq", None)
    split = P(("seq", "fsdp"), None)
    expert = P("seq", None, "fsdp")
    return jax.shard_map(
        partial(shards, mesh.shape["seq"], mesh.shape["fsdp"]),
        mesh=mesh,
        in_specs=(tokens, tokens, split, split, split, split, expert, expert, expert, tokens),
        out_specs=(tokens, tokens, split, split, split, split, expert, expert, expert),
        check_vma=False,
    )
```

```python
from functools import partial

import jax
import jax.numpy as jnp
from jax import lax
from jax.experimental import pallas as pl
from jax.experimental.pallas import tpu as pltpu
from jax.sharding import PartitionSpec as P


HEADS = 16
TOPK = 8
EPS = 1e-05
NEG = -1e30
F32 = jnp.float32
BF16 = jnp.bfloat16
MESH = pl.DeviceIdType.MESH
PIECES = 2
EARLY = 3
ANY = pl.BlockSpec(memory_space=pl.ANY)
VMEM = pl.BlockSpec(memory_space=pltpu.VMEM)
MATMUL = (((1,), (0,)), ((), ()))
BY_LAST = (((1,), (1,)), ((), ()))
BY_FIRST = (((0,), (0,)), ((), ()))


def dot(a, b, dims):
    return lax.dot_general(a, b, dims, preferred_element_type=F32)


class Ring:
    def __init__(self, n, f):
        self.n, self.f = n, f
        self.chips = n // 2
        self.half = self.chips // 2
        self.pairs_minor = f == 2
        self.me = lax.axis_index("seq")
        self.mine = lax.axis_index("fsdp")
        chip = self.me // 2
        self.core = self.me % 2
        if self.pairs_minor:
            along, side = chip // 2, chip % 2
        else:
            along, side = chip % self.half, chip // self.half
        self.pos = along + side * (self.chips - 1 - 2 * along)
        self.right = self.at(self.pos + 1)
        self.left = self.at(self.pos + self.chips - 1)
        self.mate = self.me + 1 - 2 * self.core
        self.sign = 1 - 2 * self.core
        self.onward = self.at(self.pos + self.sign + self.chips)

    def at(self, place, other=False):
        place = lax.rem(place + self.chips, self.chips)
        side = place // self.half
        along = place + side * (self.chips - 1 - 2 * place)
        chip = along * 2 + side if self.pairs_minor else side * self.half + along
        core = 1 - self.core if other else self.core
        return chip * 2 + core

    def peer(self, step):
        return lax.rem(self.me + step, self.n)

    def beside(self, step):
        return lax.rem(self.mine + step, self.f)


def greet(ring, everyone, beside):
    barrier = pltpu.get_barrier_semaphore()
    count = 0
    if everyone:
        for step in range(1, ring.n):
            pl.semaphore_signal(
                barrier, inc=1, device_id={"seq": ring.peer(step)}, device_id_type=MESH
            )
        count += ring.n - 1
    else:
        for other in (ring.right, ring.left, ring.mate):
            pl.semaphore_signal(barrier, inc=1, device_id={"seq": other}, device_id_type=MESH)
        count += 3
    if beside:
        for step in range(1, ring.f):
            pl.semaphore_signal(
                barrier, inc=1, device_id={"fsdp": ring.beside(step)}, device_id_type=MESH
            )
        count += ring.f - 1
    pl.semaphore_wait(barrier, count)


def remote(src, dst, send, recv, where):
    return pltpu.make_async_remote_copy(
        src_ref=src,
        dst_ref=dst,
        send_sem=send,
        recv_sem=recv,
        device_id=where,
        device_id_type=MESH,
    )


class Gather:
    def __init__(self, ring, own, out, sems):
        self.ring, self.own, self.out = ring, own, out
        self.send, self.recv, self.mate_send, self.mate_recv, self.keep = sems
        self.piece = own.shape[0] // (2 * PIECES)
        self.last = ring.chips - 1

    @staticmethod
    def semaphores(n):
        hops = n // 2 - 1
        kind = pltpu.SemaphoreType.DMA
        return [
            kind((2, hops, PIECES)),
            kind((2, hops, PIECES)),
            kind((2, hops + 1, PIECES)),
            kind((2, hops + 1, PIECES)),
            kind((1,)),
        ]

    def rows(self, way, s):
        return pl.ds((way * PIECES + s) * self.piece, self.piece)

    def hop(self, way, step, s, first):
        ring = self.ring
        chunk = ring.at(ring.pos - step if way == 0 else ring.pos + step)
        rows = self.rows(way, s)
        there = self.out.at[chunk, rows]
        return remote(
            self.own.at[rows] if first else there,
            there,
            self.send.at[way, step, s],
            self.recv.at[way, step, s],
            {"seq": ring.right if way == 0 else ring.left},
        )

    def share(self, way, step, s, first):
        ring = self.ring
        chunk = ring.at(ring.pos - step if way == 0 else ring.pos + step)
        rows = self.rows(way, s)
        there = self.out.at[chunk, rows]
        return remote(
            self.own.at[rows] if first else there,
            there,
            self.mate_send.at[way, step, s],
            self.mate_recv.at[way, step, s],
            {"seq": ring.mate},
        )

    def local(self):
        return pltpu.make_async_copy(self.own, self.out.at[self.ring.me], self.keep.at[0])

    def begin(self):
        for s in range(PIECES):
            for way in (0, 1):
                self.hop(way, 0, s, True).start()
        for s in range(PIECES):
            for way in (0, 1):
                self.share(way, 0, s, True).start()
        self.local().start()

    def pass_on(self, i):
        for s in range(PIECES):
            for way in (0, 1):
                self.hop(way, i, s, False).wait_recv()

                @pl.when(i + 1 < self.ring.chips - 1)
                def _():
                    self.hop(way, i + 1, s, False).start()

                self.share(way, i + 1, s, False).start()

    def run(self):
        def body(step, carry):
            self.pass_on(step)
            return carry

        lax.fori_loop(0, self.ring.chips - 1, body, 0)

    def finish(self):
        hops = self.ring.chips - 1

        def body(step, carry):
            for s in range(PIECES):
                for way in (0, 1):
                    self.hop(way, step, s, False).wait_send()
                    self.share(way, step, s, False).wait()
            return carry

        lax.fori_loop(0, hops, body, 0)
        for s in range(PIECES):
            for way in (0, 1):
                self.share(way, hops, s, False).wait()
        self.local().wait()


class Scatter:
    def __init__(self, ring, part, tok, width, buffers, sems):
        self.ring, self.part, self.tok, self.width = ring, part, tok, width
        self.mate_out, self.mate_in, self.own, self.going, self.coming = buffers
        self.send, self.recv, self.mate_send, self.mate_recv = sems
        self.piece = tok // (2 * PIECES)

    @staticmethod
    def buffers(n, tok, width):
        chips = n // 2
        return [
            pltpu.VMEM((chips, tok, width), BF16),
            pltpu.VMEM((chips, tok, width), BF16),
            pltpu.VMEM((2, tok, width), F32),
            pltpu.VMEM((chips - 1, tok, width), BF16),
            pltpu.VMEM((chips - 1, tok, width), BF16),
        ]

    @staticmethod
    def semaphores(n):
        chips = n // 2
        kind = pltpu.SemaphoreType.DMA
        return [
            kind((2, chips - 1, PIECES)),
            kind((2, chips - 1, PIECES)),
            kind((chips,)),
            kind((chips,)),
        ]

    def rows(self, way, s):
        return pl.ds((way * PIECES + s) * self.piece, self.piece)

    def exchange(self, i):
        return remote(
            self.mate_out.at[i],
            self.mate_in.at[i],
            self.mate_send.at[i],
            self.mate_recv.at[i],
            {"seq": self.ring.mate},
        )

    def hop(self, way, i, s):
        ring = self.ring
        rows = self.rows(way, s)
        return remote(
            self.going.at[i, rows],
            self.coming.at[i, rows],
            self.send.at[way, i, s],
            self.recv.at[way, i, s],
            {"seq": ring.right if way == 0 else ring.left},
        )

    def produce(self, i):
        ring = self.ring
        half = self.tok // 2
        places = (ring.pos - 1 - i, ring.pos + 1 + i)
        for way in (0, 1):
            chunk = ring.at(places[way] + ring.chips, True)
            self.part(chunk, way, self.mate_out, i)
        self.exchange(i).start()
        slot = lax.rem(i, 2)
        for way in (0, 1):
            chunk = ring.at(places[way] + ring.chips)
            self.part(chunk, way, self.own, slot)

    def step(self, i, first):
        self.exchange(i).wait_recv()
        slot = lax.rem(i, 2)
        for s in range(PIECES):
            for way in (0, 1):
                rows = self.rows(way, s)
                value = self.own[slot, rows] + self.mate_in[i, rows].astype(F32)
                if not first:
                    self.hop(way, i - 1, s).wait_recv()
                    value = value + self.coming[i - 1, rows].astype(F32)
                self.going[i, rows] = value.astype(BF16)
                self.hop(way, i, s).start()

    def run(self, finish, between=None):
        last = self.ring.chips - 1
        self.produce(0)
        self.produce(1)
        self.step(0, True)

        def body(i, carry):
            self.produce(i + 1)
            self.step(i, False)
            return carry

        if between is None:
            lax.fori_loop(1, last, body, 0)
        else:
            lax.fori_loop(1, last // 2 + 1, body, 0)
            between()
            lax.fori_loop(last // 2 + 1, last, body, 0)
        self.exchange(last).wait_recv()
        slot = last % 2
        for s in range(PIECES):
            for way in (0, 1):
                rows = self.rows(way, s)
                self.hop(way, last - 1, s).wait_recv()
                value = self.own[slot, rows] + self.mate_in[last, rows].astype(F32)
                value = value + self.coming[last - 1, rows].astype(F32)
                finish(rows, value)

    def close(self):
        last = self.ring.chips - 1

        def body(i, carry):
            self.exchange(i).wait_send()
            for s in range(PIECES):
                for way in (0, 1):
                    self.hop(way, i, s).wait_send()
            return carry

        lax.fori_loop(0, last, body, 0)
        self.exchange(last).wait_send()


class Walk:
    def __init__(self, ring, own, out, sems):
        self.ring, self.own, self.out = ring, own, out
        self.send, self.recv, self.share_send, self.share_recv, self.keep = sems
        self.piece = own.shape[0] // PIECES
        self.last = ring.chips - 1

    @staticmethod
    def semaphores(n):
        kind = pltpu.SemaphoreType.DMA
        return [kind((n // 2, PIECES)) for _ in range(4)] + [kind((1,))]

    def block(self, i):
        ring = self.ring
        return ring.at(ring.pos - ring.sign * i + 2 * ring.chips)

    def hop(self, i, s, first=False):
        rows = pl.ds(s * self.piece, self.piece)
        there = self.out.at[self.block(i), rows]
        return remote(
            self.own.at[rows] if first else there,
            there,
            self.send.at[i, s],
            self.recv.at[i, s],
            {"seq": self.ring.onward},
        )

    def share(self, i, s, first=False):
        rows = pl.ds(s * self.piece, self.piece)
        there = self.out.at[self.block(i), rows]
        return remote(
            self.own.at[rows] if first else there,
            there,
            self.share_send.at[i, s],
            self.share_recv.at[i, s],
            {"seq": self.ring.mate},
        )

    def local(self):
        return pltpu.make_async_copy(self.own, self.out.at[self.ring.me], self.keep.at[0])

    def begin(self):
        for s in range(PIECES):
            self.hop(0, s, True).start()
        for s in range(PIECES):
            self.share(0, s, True).start()
        self.local().start()

    def pass_on(self, i):
        for s in range(PIECES):
            self.hop(i, s).wait_recv()

            @pl.when(i + 1 < self.last)
            def _():
                self.hop(i + 1, s).start()

            self.share(i + 1, s).start()

    def finish(self):
        def body(i, carry):
            for s in range(PIECES):
                self.hop(i, s).wait_send()
                self.share(i, s).wait()
            return carry

        lax.fori_loop(0, self.last, body, 0)
        for s in range(PIECES):
            self.share(self.last, s).wait()
        self.local().wait()


class Fold:
    def __init__(self, ring, part, buffers, sems):
        self.ring, self.part = ring, part
        self.mate_out, self.mate_in, self.own, self.going, self.coming = buffers
        self.swap_send, self.swap_recv, self.send, self.recv = sems
        self.piece = self.own.shape[0] // PIECES
        self.last = ring.chips - 1

    @staticmethod
    def buffers(n, tok, width):
        chips = n // 2
        return [
            pltpu.VMEM((2, tok, width), BF16),
            pltpu.VMEM((chips, tok, width), BF16),
            pltpu.VMEM((tok, width), F32),
            pltpu.VMEM((2, tok, width), BF16),
            pltpu.VMEM((chips - 1, tok, width), BF16),
        ]

    @staticmethod
    def semaphores(n):
        chips = n // 2
        kind = pltpu.SemaphoreType.DMA
        return [kind((chips,)), kind((chips,)), kind((chips, PIECES)), kind((chips, PIECES))]

    def swap(self, i):
        return remote(
            self.mate_out.at[lax.rem(i, 2)],
            self.mate_in.at[i],
            self.swap_send.at[i],
            self.swap_recv.at[i],
            {"seq": self.ring.mate},
        )

    def hop(self, i, s):
        rows = pl.ds(s * self.piece, self.piece)
        return remote(
            self.going.at[lax.rem(i, 2), rows],
            self.coming.at[i, rows],
            self.send.at[i, s],
            self.recv.at[i, s],
            {"seq": self.ring.onward},
        )

    def produce(self, i):
        ring = self.ring

        @pl.when(i >= 2)
        def _():
            self.swap(i - 2).wait_send()

        slot = lax.rem(i, 2)
        there = ring.at(ring.pos + ring.sign * (1 + i) + 2 * ring.chips, True)
        self.part(there, self.mate_out.at[slot])
        self.swap(i).start()
        here = ring.at(ring.pos - ring.sign * (1 + i) + 2 * ring.chips)
        self.part(here, self.own)

    def step(self, i):
        self.swap(i).wait_recv()

        @pl.when(i >= 2)
        def _():
            for s in range(PIECES):
                self.hop(i - 2, s).wait_send()

        for s in range(PIECES):
            rows = pl.ds(s * self.piece, self.piece)

            @pl.when(i > 0)
            def _():
                self.hop(i - 1, s).wait_recv()
                self.own[rows, :] = self.own[rows, :] + self.coming[i - 1, rows].astype(F32)

            value = self.own[rows, :] + self.mate_in[i, rows].astype(F32)
            self.going[lax.rem(i, 2), rows] = value.astype(BF16)
            self.hop(i, s).start()

    def run(self, finish, filler, after):
        last = self.last

        def body(i, carry):
            self.produce(i)
            self.step(i)
            after(i)
            filler(i)
            return carry

        lax.fori_loop(1, last, body, 0)
        self.produce(last)
        filler(last)
        self.swap(last).wait_recv()
        for s in range(PIECES):
            rows = pl.ds(s * self.piece, self.piece)
            self.hop(last - 1, s).wait_recv()
            value = self.own[rows, :] + self.mate_in[last, rows].astype(F32)
            finish(rows, value + self.coming[last - 1, rows].astype(F32))

    def close(self):
        last = self.last
        for s in range(PIECES):
            self.hop(last - 2, s).wait_send()
            self.hop(last - 1, s).wait_send()
        self.swap(last - 1).wait_send()
        self.swap(last).wait_send()


class Stored:
    def __init__(self, ring, parts, buffers, sems):
        self.ring, self.parts = ring, parts
        self.near, self.mate_in, self.going, self.coming = buffers
        self.swap_send, self.swap_recv, self.send, self.recv, self.load_sem = sems
        self.piece = self.near.shape[1] // PIECES
        self.last = ring.chips - 1

    @staticmethod
    def buffers(n, tok, width):
        chips = n // 2
        return [
            pltpu.VMEM((2, tok, width), BF16),
            pltpu.VMEM((chips, tok, width), BF16),
            pltpu.VMEM((2, tok, width), BF16),
            pltpu.VMEM((chips - 1, tok, width), BF16),
        ]

    @staticmethod
    def semaphores(n):
        chips = n // 2
        kind = pltpu.SemaphoreType.DMA
        return [
            kind((chips,)),
            kind((chips,)),
            kind((chips, PIECES)),
            kind((chips, PIECES)),
            kind((2,)),
        ]

    def swap(self, i):
        ring = self.ring
        there = ring.at(ring.pos + ring.sign * (1 + i) + 2 * ring.chips, True)
        return remote(
            self.parts.at[there],
            self.mate_in.at[i],
            self.swap_send.at[i],
            self.swap_recv.at[i],
            {"seq": ring.mate},
        )

    def load(self, i):
        ring = self.ring
        here = ring.at(ring.pos - ring.sign * (1 + i) + 2 * ring.chips)
        slot = lax.rem(i, 2)
        return pltpu.make_async_copy(
            self.parts.at[here], self.near.at[slot], self.load_sem.at[slot]
        )

    def hop(self, i, s):
        rows = pl.ds(s * self.piece, self.piece)
        return remote(
            self.going.at[lax.rem(i, 2), rows],
            self.coming.at[i, rows],
            self.send.at[i, s],
            self.recv.at[i, s],
            {"seq": self.ring.onward},
        )

    def begin(self):
        self.load(0).start()

        def body(i, carry):
            self.swap(i).start()
            return carry

        lax.fori_loop(0, self.last + 1, body, 0)

    def step(self, i):
        self.load(i).wait()
        self.load(i + 1).start()
        self.swap(i).wait_recv()
        slot = lax.rem(i, 2)

        @pl.when(i >= 2)
        def _():
            for s in range(PIECES):
                self.hop(i - 2, s).wait_send()

        for s in range(PIECES):
            rows = pl.ds(s * self.piece, self.piece)
            value = self.near[slot, rows].astype(F32) + self.mate_in[i, rows].astype(F32)
            self.going[slot, rows] = value.astype(BF16)

            @pl.when(i > 0)
            def _():
                self.hop(i - 1, s).wait_recv()
                total = self.near[slot, rows].astype(F32) + self.mate_in[i, rows].astype(F32)
                total = total + self.coming[i - 1, rows].astype(F32)
                self.going[slot, rows] = total.astype(BF16)

            self.hop(i, s).start()

    def close(self, finish):
        last = self.last
        self.load(last).wait()
        self.swap(last).wait_recv()
        for s in range(PIECES):
            rows = pl.ds(s * self.piece, self.piece)
            self.hop(last - 1, s).wait_recv()
            value = self.near[last % 2, rows].astype(F32) + self.mate_in[last, rows].astype(F32)
            finish(rows, value + self.coming[last - 1, rows].astype(F32))
            self.hop(last - 2, s).wait_send()
            self.hop(last - 1, s).wait_send()

        def body(i, carry):
            self.swap(i).wait_send()
            return carry

        lax.fori_loop(0, last + 1, body, 0)


def first_kernel(n, f, *refs):
    own, w_qkv, small, routes, w_out, w_gate, w_up = refs[:7]
    hidden_all, mixed, w_head, router, gains, routes_all, gate_near, up_near, out_all = refs[7:16]
    near, small_all, out_rows, by_head = refs[16:20]
    sems, out_sems = refs[20:25], refs[25:30]
    send, recv, beside_send, beside_recv, keep = refs[30:35]
    wide_send, wide_recv, row_send, row_recv, out_sem = refs[35:]
    ring = Ring(n, f)
    experts = router.shape[0]
    tok, width = own.shape
    rows = small.shape[0]
    hops = ring.chips - 1
    piece = width // ring.chips
    head = width // n
    for h in range(n):
        for k in range(3):
            start = k * width + h * head
            by_head[h, :, k * head : (k + 1) * head] = w_qkv[:, start : start + head]
    greet(ring, True, True)
    gather = Gather(ring, own, near, sems)
    gather_out = Gather(ring, out_rows, out_all, out_sems)
    out_mine = pl.ds(pl.multiple_of(ring.mine * rows, rows), rows)

    def push(kind, step):
        there = ring.peer(step)
        source, target = [
            (by_head.at[there], w_head.at[ring.me, ring.mine]),
            (small, small_all.at[ring.me, ring.mine]),
            (routes, routes_all.at[ring.me]),
        ][kind]
        return remote(
            source, target, send.at[kind, step], recv.at[kind, step], {"seq": there}
        )

    def aside(kind, step, over, first):
        origin = lax.rem(ring.me + n - step, n)
        block = [w_head, small_all][kind].at[origin, ring.mine]
        source = [by_head.at[ring.me], small][kind] if first else block
        return remote(
            source,
            block,
            beside_send.at[kind, step, over],
            beside_recv.at[kind, step, over],
            {"fsdp": ring.beside(over)},
        )

    def row(over):
        return remote(
            w_out,
            out_rows.at[out_mine],
            row_send.at[over],
            row_recv.at[over],
            {"fsdp": ring.beside(over)},
        )

    def wide(part, over):
        kind, part = divmod(part, ring.chips)
        these = pl.ds(part * piece, piece)
        return remote(
            [w_gate, w_up][kind].at[these],
            [gate_near, up_near][kind].at[over - 1, these],
            wide_send.at[kind, part, over],
            wide_recv.at[kind, part, over],
            {"fsdp": ring.beside(over)},
        )

    half_parts = ring.chips + ring.chips // 2

    gather.begin()
    for over in range(1, f):
        row(over).start()
    copies = [
        pltpu.make_async_copy(by_head.at[ring.me], w_head.at[ring.me, ring.mine], keep.at[0]),
        pltpu.make_async_copy(small, small_all.at[ring.me, ring.mine], keep.at[1]),
        pltpu.make_async_copy(routes, routes_all.at[ring.me], keep.at[2]),
        pltpu.make_async_copy(w_out, out_rows.at[out_mine], keep.at[3]),
    ]
    for copy in copies:
        copy.start()
    for step in range(1, n):
        for kind in (1, 0, 2):
            push(kind, step).start()
    for over in range(1, f):
        aside(1, 0, over, True).start()
        aside(0, 0, over, True).start()
        wide(0, over).start()
    each = -(-(n - 1) // 3)
    parts = 1

    def widen(parts):
        if parts < half_parts:
            for over in range(1, f):
                wide(parts, over).start()
        return parts + 1

    for i in range(hops):
        gather.pass_on(i)
        if 2 <= i < 5:
            for step in range((i - 2) * each + 1, min((i - 1) * each, n - 1) + 1):
                for kind in (1, 0):
                    push(kind, step).wait_recv()
                    for over in range(1, f):
                        aside(kind, step, over, False).start()
        else:
            parts = widen(parts)
        if i == hops - 2:
            copies[3].wait()
            for over in range(1, f):
                row(over).wait_recv()
            gather_out.begin()
    gather.finish()
    for copy in copies[:3]:
        copy.wait()
    for step in range(1, n):
        push(2, step).wait_recv()
        for kind in (0, 1, 2):
            push(kind, step).wait_send()
    for step in range(n):
        for kind in (0, 1):
            for over in range(1, f):
                aside(kind, step, over, False).wait()

    lanes = lax.broadcasted_iota(jnp.int32, (32, small.shape[1]), 1)
    places = lax.broadcasted_iota(jnp.int32, (32, small.shape[1]), 0)
    chosen = jnp.where(lanes == places, 1.0, 0.0).astype(BF16)
    for c in range(n):
        for x in range(f):
            start = (c * f + x) * rows
            flipped = dot(chosen, small_all[c, x], BY_LAST)
            router[:, start : start + rows] = flipped[0:experts, :].astype(BF16)
            gains[:, start : start + rows] = flipped[experts : experts + 8, :]

    def out(c):
        return pltpu.make_async_copy(near.at[c], hidden_all.at[c], out_sem.at[c])

    def project(c, carry):
        value = near[c].astype(F32)
        inverse = lax.rsqrt(jnp.mean(value * value, -1, keepdims=True) + EPS)
        near[c] = (value * inverse * gains[0:1, :]).astype(BF16)
        out(c).start()
        here = pl.ds(pl.multiple_of(c * tok, tok), tok)
        total = jnp.zeros((tok, w_head.shape[3]), F32)
        for k in range(n):
            for x in range(f):
                start = (k * f + x) * rows
                if (k * f + x) % (256 // rows):
                    continue
                wide_rows = 256 // rows
                if wide_rows <= f:
                    right = w_head[k, x : x + wide_rows]
                else:
                    right = w_head[k : k + wide_rows // f]
                right = right.reshape(256, w_head.shape[3])
                total = total + dot(near[c, :, start : start + 256], right, MATMUL)
        mixed[here, :] = total
        return carry

    done = 0
    for i in range(hops):
        parts = widen(parts)
        upto = min(n, -(-n * (i + 1) // hops))
        lax.fori_loop(done, upto, project, 0)
        done = upto
        gather_out.pass_on(i)
    while parts < half_parts:
        parts = widen(parts)
    for c in range(n):
        out(c).wait()
    gather_out.finish()
    for over in range(1, f):
        row(over).wait_send()
        for part in range(half_parts):
            wide(part, over).wait()


def first_gather(n, f, own, w_qkv, small, routes, w_out, w_gate, w_up):
    tok, width = own.shape
    experts = n
    by_head = jax.ShapeDtypeStruct((n, w_qkv.shape[0], 3 * width // n), BF16)
    kind = pltpu.SemaphoreType.DMA
    shape = jax.ShapeDtypeStruct
    return pl.pallas_call(
        partial(first_kernel, n, f),
        out_shape=[
            shape((n, tok, width), BF16),
            shape((n * tok, by_head.shape[2]), F32),
            shape((n, f) + by_head.shape[1:], BF16),
            shape((experts, width), BF16),
            shape((8, width), F32),
            shape((n,) + routes.shape, jnp.int32),
            shape((max(f - 1, 1),) + w_gate.shape, BF16),
            shape((max(f - 1, 1), w_up.shape[0] // 2, w_up.shape[1]), BF16),
            shape((n, f * w_out.shape[0], w_out.shape[1]), BF16),
        ],
        in_specs=[VMEM] * 5 + [ANY] * 2,
        out_specs=[ANY] + [VMEM] * 4 + [ANY] * 4,
        scratch_shapes=[
            pltpu.VMEM((n, tok, width), BF16),
            pltpu.VMEM((n, f) + small.shape, BF16),
            pltpu.VMEM((f * w_out.shape[0], w_out.shape[1]), BF16),
            pltpu.VMEM(by_head.shape, BF16),
        ]
        + Gather.semaphores(n)
        + Gather.semaphores(n)
        + [kind((3, n)), kind((3, n)), kind((2, n, f)), kind((2, n, f)), kind((4,))]
        + [kind((2, n // 2, f)), kind((2, n // 2, f)), kind((f,)), kind((f,)), kind((n,))],
        compiler_params=pltpu.CompilerParams(
            collective_id=0, has_side_effects=True, vmem_limit_bytes=67_000_000
        ),
        name="first_gather",
    )(own, w_qkv, small, routes, w_out, w_gate, w_up)


def blocks_of(length):
    block = min(512, length)
    return block, length // block


def across_lanes(value):
    ones = jnp.ones((8, value.shape[1]), F32)
    total = lax.dot_general(
        ones, value, BY_LAST, precision=lax.Precision.HIGHEST, preferred_element_type=F32
    )
    return total[0:1, :]


def to_column(table, index, lanes):
    rows = lax.broadcasted_iota(jnp.int32, (table.shape[0], lanes), 0)
    chosen = jnp.where(rows == index, 1.0, 0.0)
    return lax.dot_general(
        table, chosen, BY_FIRST, precision=lax.Precision.HIGHEST, preferred_element_type=F32
    )


def half_turn(value, first_sign):
    half = value.shape[1] // 2
    lanes = lax.broadcasted_iota(jnp.int32, value.shape, 1)
    sign = jnp.where(lanes < half, first_sign, -first_sign)
    return pltpu.roll(value, half, 1) * sign


def set_angles(n, tables, starts, cosine, sine):
    tok = tables.shape[1]

    def angles(c, carry):
        here = pl.ds(pl.multiple_of(c * tok, tok), tok)
        cosine[here, :] = starts[0, c] * tables[0] - starts[1, c] * tables[1]
        sine[here, :] = starts[1, c] * tables[0] + starts[0, c] * tables[1]
        return carry

    lax.fori_loop(0, n, angles, 0)


class Spread:
    def __init__(self, ring, block, out, sems):
        self.ring, self.block, self.out = ring, block, out
        self.send, self.recv, self.keep = sems

    @staticmethod
    def semaphores(n):
        kind = pltpu.SemaphoreType.DMA
        return [kind((n,)), kind((n,)), kind((1,))]

    def push(self, step):
        return remote(
            self.block,
            self.out.at[self.ring.me],
            self.send.at[step],
            self.recv.at[step],
            {"seq": self.ring.peer(step)},
        )

    def local(self):
        return pltpu.make_async_copy(self.block, self.out.at[self.ring.me], self.keep.at[0])

    def begin(self):
        for step in range(1, self.ring.n):
            self.push(step).start()
        self.local().start()

    def finish(self):
        for step in range(1, self.ring.n):
            self.push(step).wait()
        self.local().wait()

    def total(self):
        total = self.out[0]
        for device in range(1, self.ring.n):
            total = total + self.out[device]
        return total


def attention_kernel(n, f, factor, *refs):
    mixed, tables, starts, gains, upstream = refs[:5]
    q_ref, k_ref, v_ref, out_ref, exact_ref, sums_ref, squares = refs[5:12]
    upstream_all, by_token = refs[12:14]
    partial_sums, arrived, cosine, sine = refs[14:18]
    sems, walk_sems = refs[18:21], refs[21:26]
    deal_send, deal_recv, deal_keep = refs[26:]
    ring = Ring(n, f)
    length, head = q_ref.shape
    width = head * n
    block, count = blocks_of(length)
    greet(ring, True, False)
    walk = Gather(ring, upstream, upstream_all, walk_sems)
    last = walk.last
    mine = pl.ds(pl.multiple_of(ring.me * head, head), head)

    def deal(there):
        these = pl.ds(pl.multiple_of(there * tok, tok), tok)
        return remote(
            out_ref.at[these],
            by_token.at[:, mine],
            deal_send.at[there],
            deal_recv.at[ring.me],
            {"seq": there},
        )

    def dealt(origin):
        return remote(
            out_ref.at[pl.ds(0, tok)],
            by_token.at[:, pl.ds(pl.multiple_of(origin * head, head), head)],
            deal_send.at[origin],
            deal_recv.at[origin],
            {"seq": origin},
        )

    tok = tables.shape[1]

    def measure(b, carry):
        here = pl.ds(pl.multiple_of(b * block, block), block)
        for kind in (0, 1):
            raw = mixed[here, kind * head : (kind + 1) * head]
            partial_sums[pl.ds(kind * count + b, 1), :] = across_lanes(raw * raw)
        v_ref[here, :] = mixed[here, 2 * head :].astype(BF16)
        return carry

    lax.fori_loop(0, count, measure, 0)
    spread = Spread(ring, partial_sums, arrived, sems)
    spread.begin()
    walk.begin()

    set_angles(n, tables, starts, cosine, sine)
    spread.finish()
    squares[...] = spread.total()
    walk.pass_on(0)

    def prepare(b, carry):
        here = pl.ds(pl.multiple_of(b * block, block), block)
        for kind, target in ((0, q_ref), (1, k_ref)):
            inverse = lax.rsqrt(to_column(squares[...], kind * count + b, head) / width + EPS)
            raw = mixed[here, kind * head : (kind + 1) * head]
            normed = raw * inverse * gains[kind + 1 : kind + 2, mine]
            turned = half_turn(normed, -1.0)
            target[here, :] = (normed * cosine[here, :] + turned * sine[here, :]).astype(BF16)
        return carry

    lax.fori_loop(0, count, prepare, 0)
    rows = lax.broadcasted_iota(jnp.int32, (block, block), 0)
    cols = lax.broadcasted_iota(jnp.int32, (block, block), 1)

    def outer(i, carry):
        here = pl.ds(pl.multiple_of(i * block, block), block)
        part = q_ref[here, :]

        def inner(j, state, masked):
            top, total, acc = state
            there = pl.ds(pl.multiple_of(j * block, block), block)
            scores = dot(part, k_ref[there, :], BY_LAST) * factor
            if masked:
                scores = jnp.where(cols <= rows, scores, NEG)
            new = jnp.maximum(top, jnp.max(scores, -1, keepdims=True))
            scale = jnp.exp(top - new)
            expd = jnp.exp(scores - new)
            total = total * scale + jnp.sum(expd, -1, keepdims=True)
            acc = acc * scale + dot(expd.astype(BF16), v_ref[there, :], MATMUL)
            return new, total, acc

        state = (
            jnp.full((block, 1), NEG, F32),
            jnp.zeros((block, 1), F32),
            jnp.zeros((block, head), F32),
        )
        state = lax.fori_loop(0, i, lambda j, s: inner(j, s, False), state)
        top, total, acc = inner(i, state, True)
        exact = acc / total
        exact_ref[here, :] = exact
        out_ref[here, :] = exact.astype(BF16)
        column = jnp.broadcast_to(top + jnp.log(total), (block, 128))
        sums_ref[:, here] = jnp.transpose(column)[0:8, :]

        for r in range(block // tok):
            there = i * (block // tok) + r

            @pl.when(there != ring.me)
            def _():
                deal(there).start()

        @pl.when((i > 0) & (i < last))
        def _():
            walk.pass_on(i)

        return carry

    lax.fori_loop(0, count, outer, 0)
    these = pl.ds(pl.multiple_of(ring.me * tok, tok), tok)
    local = pltpu.make_async_copy(out_ref.at[these], by_token.at[:, mine], deal_keep.at[0])
    local.start()
    for i in range(count, last):
        walk.pass_on(i)
    walk.finish()
    for step in range(1, n):
        deal(ring.peer(step)).wait_send()
        dealt(ring.peer(step)).wait_recv()
    local.wait()


def attention(n, f, mixed, tables, starts, gains, upstream, factor):
    length, head = mixed.shape[0], mixed.shape[1] // 3
    block, count = blocks_of(length)
    shape = jax.ShapeDtypeStruct
    return pl.pallas_call(
        partial(attention_kernel, n, f, factor),
        out_shape=[
            shape((length, head), BF16),
            shape((length, head), BF16),
            shape((length, head), BF16),
            shape((length, head), BF16),
            shape((length, head), F32),
            shape((8, length), F32),
            shape((2 * count, block), F32),
            shape((n,) + upstream.shape, BF16),
            shape((length // n, head * n), BF16),
        ],
        in_specs=[VMEM] * 5,
        out_specs=[VMEM] * 7 + [ANY, VMEM],
        scratch_shapes=[
            pltpu.VMEM((2 * count, block), F32),
            pltpu.VMEM((n, 2 * count, block), F32),
            pltpu.VMEM((length, head), F32),
            pltpu.VMEM((length, head), F32),
        ]
        + Spread.semaphores(n)
        + Gather.semaphores(n)
        + [pltpu.SemaphoreType.DMA((n,)), pltpu.SemaphoreType.DMA((n,))]
        + [pltpu.SemaphoreType.DMA((1,))],
        compiler_params=pltpu.CompilerParams(
            collective_id=5, has_side_effects=True, vmem_limit_bytes=67_000_000
        ),
        cost_estimate=pl.CostEstimate(
            flops=2 * length * length * head,
            transcendentals=length * length // 2,
            bytes_accessed=8 * length * head,
        ),
        name="attention",
    )(mixed, tables, starts, gains, upstream)


def attention_back_kernel(n, f, factor, *refs):
    q_ref, k_ref, v_ref, by_token, sums_ref, exact, mixed, tables, starts, gains, squares = refs[:11]
    d_attn, attended, own_hidden, d_logits = refs[11:15]
    far = refs[15:19]
    d_mixed, gain_head, qkv_part, proj, router, first_in, second_in = refs[19:26]
    dq_ref, dk_ref, dv_ref, delta, partial_sums, arrived, d_attn_all, first, d_ref = refs[26:35]
    cosine, sine = refs[35:37]
    near = refs[37:41]
    rows_in, d_gate, d_up, hidden = near
    walk_sems, spread_sems = refs[41:46], refs[46:49]
    load_sem, first_send, first_recv, deal_send, deal_recv, deal_keep = refs[49:]
    ring = Ring(n, f)
    length, head = q_ref.shape
    width = head * n
    units = first_in.shape[2]
    block, count = blocks_of(length)
    loads = [
        pltpu.make_async_copy(
            source.at[:, units:] if k in (1, 2) else source, target, load_sem.at[k]
        )
        for k, (source, target) in enumerate(zip(far, near))
    ]
    for load in loads:
        load.start()
    greet(ring, True, True)
    tok = d_attn.shape[0]
    here_rows = pl.ds(pl.multiple_of(ring.me * tok, tok), tok)
    mine = pl.ds(pl.multiple_of(ring.me * head, head), head)

    def deal(step):
        there = ring.peer(step)
        return remote(
            by_token.at[:, pl.ds(pl.multiple_of(there * head, head), head)],
            d_ref.at[here_rows],
            deal_send.at[step],
            deal_recv.at[step],
            {"seq": there},
        )

    local = pltpu.make_async_copy(
        by_token.at[:, pl.ds(pl.multiple_of(ring.me * head, head), head)],
        d_ref.at[here_rows],
        deal_keep.at[0],
    )
    for step in range(1, n):
        deal(step).start()
    local.start()
    walk = Gather(ring, d_attn, d_attn_all, walk_sems)
    walk.begin()
    last = walk.last
    tiles = ring.chips
    size = width // tiles

    def send_first(tile, j):
        kind, at = divmod(tile, tiles)
        these = pl.ds(at * size, size)
        return remote(
            first.at[tile, j],
            [first_in, second_in][kind].at[j, these],
            first_send.at[tile, j],
            first_recv.at[tile, j],
            {"fsdp": ring.beside(f - 1 - j)},
        )

    set_angles(n, tables, starts, cosine, sine)
    for load in loads[:3]:
        load.wait()
    for tile in range(tiles + EARLY):
        kind, at = divmod(tile, tiles)
        for j in range(f - 1):
            part = slice(j * units, (j + 1) * units)
            right = [d_gate, d_up][kind]
            value = dot(rows_in[:, at * size : (at + 1) * size], right[:, part], BY_FIRST)
            first[tile, j] = value.astype(BF16)
            send_first(tile, j).start()
    for step in range(1, n):
        deal(step).wait()
    local.wait()
    dq_ref[...] = jnp.zeros_like(dq_ref)

    def measure(b, carry):
        here = pl.ds(pl.multiple_of(b * block, block), block)
        value = across_lanes(d_ref[here, :].astype(F32) * exact[here, :])
        delta[:, here] = jnp.broadcast_to(value, (8, block))
        return carry

    lax.fori_loop(0, count, measure, 0)
    rows = lax.broadcasted_iota(jnp.int32, (block, block), 0)
    cols = lax.broadcasted_iota(jnp.int32, (block, block), 1)

    def outer(j, carry):
        there = pl.ds(pl.multiple_of(j * block, block), block)
        keys = k_ref[there, :]
        values = v_ref[there, :]

        def inner(i, state, masked):
            d_keys, d_values = state
            here = pl.ds(pl.multiple_of(i * block, block), block)
            part = q_ref[here, :]
            d_part = d_ref[here, :]
            scores = dot(keys, part, BY_LAST) * factor
            if masked:
                scores = jnp.where(rows <= cols, scores, NEG)
            probs = jnp.exp(scores - sums_ref[0:1, here])
            d_probs = dot(values, d_part, BY_LAST)
            d_scores = (probs * (d_probs - delta[0:1, here])).astype(BF16)
            d_values = d_values + dot(probs.astype(BF16), d_part, MATMUL)
            d_keys = d_keys + dot(d_scores, part, MATMUL)
            dq_ref[here, :] += dot(d_scores, keys, BY_FIRST)
            return d_keys, d_values

        zero = jnp.zeros((block, head), F32)
        state = inner(j, (zero, zero), True)
        state = lax.fori_loop(j + 1, count, lambda i, s: inner(i, s, False), state)
        dk_ref[there, :] = state[0]
        dv_ref[there, :] = state[1]

        @pl.when((j >= 1) & (j < last + 1))
        def _():
            walk.pass_on(j - 1)

        return carry

    lax.fori_loop(0, count, outer, 0)

    def unturn(b, carry):
        here = pl.ds(pl.multiple_of(b * block, block), block)
        for kind, source in ((0, dq_ref), (1, dk_ref)):
            grad = (source[here, :] * factor).astype(BF16).astype(F32)
            grad = grad * cosine[here, :] + half_turn(grad * sine[here, :], 1.0)
            source[here, :] = grad
            raw = mixed[here, kind * head : (kind + 1) * head]
            partial_sums[pl.ds(kind * count + b, 1), :] = across_lanes(
                raw * gains[kind + 1 : kind + 2, mine] * grad
            )
        return carry

    lax.fori_loop(0, count, unturn, 0)
    spread = Spread(ring, partial_sums, arrived, spread_sems)
    spread.begin()
    walk.pass_on(count - 1)
    loads[3].wait()
    spread.finish()
    total = spread.total()
    gain_head[...] = jnp.zeros_like(gain_head)

    def close(b, carry):
        here = pl.ds(pl.multiple_of(b * block, block), block)
        for kind, source in ((0, dq_ref), (1, dk_ref)):
            index = kind * count + b
            inverse = lax.rsqrt(to_column(squares[...], index, head) / width + EPS)
            inner = to_column(total, index, head) / width
            raw = mixed[here, kind * head : (kind + 1) * head]
            grad = source[here, :]
            value = inverse * gains[kind + 1 : kind + 2, mine] * grad
            value = value - raw * (inverse * inverse * inverse) * inner
            d_mixed[here, kind * head : (kind + 1) * head] = value.astype(BF16)
            gain_head[kind + 2 : kind + 3, :] += jnp.sum(raw * inverse * grad, 0, keepdims=True)
        d_mixed[here, 2 * head :] = dv_ref[here, :].astype(BF16)
        return carry

    lax.fori_loop(0, count, close, 0)
    walk.pass_on(count)
    chunks, beside, rows_each = qkv_part.shape[1], qkv_part.shape[0], qkv_part.shape[2]
    span = width // chunks

    def weigh(c, carry):
        these = pl.ds(pl.multiple_of(c * span, span), span)
        value = dot(hidden[:, these], d_mixed[...], BY_FIRST).astype(BF16)
        for x in range(beside):
            qkv_part[x, c] = value[x * rows_each : (x + 1) * rows_each]
        return carry

    lax.fori_loop(0, chunks, weigh, 0)
    for i in range(count + 1, last):
        walk.pass_on(i)
    router[...] = jnp.zeros_like(router)

    def route(c, carry):
        router[...] += dot(d_logits[c], own_hidden[c], MATMUL)
        return carry

    lax.fori_loop(0, n, route, 0)
    walk.finish()
    group = block // tok
    tile = min(512, width)

    def project(c, carry):
        left = attended[pl.ds(pl.multiple_of(c * block, block), block), :]
        for start in range(0, width, tile):
            cols = slice(start, start + tile)
            right = d_attn_all[pl.ds(c * group, group), :, cols].reshape(block, tile)
            value = dot(left, right, BY_FIRST)

            @pl.when(c == 0)
            def _():
                proj[:, cols] = value

            @pl.when(c > 0)
            def _():
                proj[:, cols] = proj[:, cols] + value

        return carry

    lax.fori_loop(0, count, project, 0)
    for at in range(tiles + EARLY):
        for j in range(f - 1):
            send_first(at, j).wait()


def attention_back(
    n, f, queries, keys, values, by_token, sums, exact, mixed, tables, starts, gains, squares,
    d_attn, attended, own_hidden, d_logits, rows_in, d_gate, d_up, hidden, rows, factor
):
    length, head = queries.shape
    tok, width = d_attn.shape
    block, count = blocks_of(length)
    experts = d_logits.shape[1]
    shape = jax.ShapeDtypeStruct
    kind = pltpu.SemaphoreType.DMA
    flat, every = d_gate.shape
    units = every // f
    tiles = n // 2
    grad = shape((max(f - 1, 1), width, units), BF16)
    return pl.pallas_call(
        partial(attention_back_kernel, n, f, factor),
        out_shape=[
            shape((length, 3 * head), BF16),
            shape((8, head), F32),
            shape((f, n, rows, 3 * head), BF16),
            shape((head, width), F32),
            shape((experts, head), F32),
            grad,
            grad,
        ],
        in_specs=[VMEM] * 15 + [ANY] * 4,
        out_specs=[VMEM] * 5 + [ANY] * 2,
        scratch_shapes=[pltpu.VMEM((length, head), F32)] * 3
        + [
            pltpu.VMEM((8, length), F32),
            pltpu.VMEM((2 * count, block), F32),
            pltpu.VMEM((n, 2 * count, block), F32),
            pltpu.VMEM((n, tok, width), BF16),
            pltpu.VMEM((tiles + EARLY, max(f - 1, 1), width // tiles, units), BF16),
            pltpu.VMEM((length, head), BF16),
            pltpu.VMEM((length, head), F32),
            pltpu.VMEM((length, head), F32),
            pltpu.VMEM(rows_in.shape, BF16),
            pltpu.VMEM((flat, every - units), BF16),
            pltpu.VMEM((flat, every - units), BF16),
            pltpu.VMEM(hidden.shape, BF16),
        ]
        + Gather.semaphores(n)
        + Spread.semaphores(n)
        + [kind((4,))]
        + [kind((tiles + EARLY, max(f - 1, 1))), kind((tiles + EARLY, max(f - 1, 1)))]
        + [kind((n,)), kind((n,)), kind((1,))],
        compiler_params=pltpu.CompilerParams(
            collective_id=6, has_side_effects=True, vmem_limit_bytes=67_000_000
        ),
        name="attention_back",
    )(
        queries, keys, values, by_token, sums, exact, mixed, tables, starts, gains, squares,
        d_attn, attended, own_hidden, d_logits, rows_in, d_gate, d_up, hidden
    )


def core_kernel(n, f, *refs):
    by_token, w_out, tokens, upstream, gain, router, routes, routes_all, upstream_all = refs[:9]
    shards_in = refs[9 : 8 + 4 * f]
    refs = refs[8 + 4 * f :]
    d_middle, middle, d_attn, d_by_token, d_logits_all, gain_two = refs[:6]
    own_hidden, rows_out, d_out, inner_out, d_gate_out, d_up_out, moe_out = refs[6:13]
    refs = refs[13:]
    w_near, w_gate, w_up, w_down, d_logits, arrived, outgoing, weights_in = refs[:8]
    refs = refs[8:]
    ring_in, mate_near, d_mate_in, coming, going, d_mate_out, own, lift = refs[:8]
    refs = refs[8:]
    rows_now, lifted, d_now, inner_now, d_gate_now, d_up_now, moe_now, d_weight, places = refs[:9]
    refs = refs[9:]
    hop_send, hop_recv, share_send, share_recv, swap_send, swap_recv = refs[:6]
    sum_send, sum_recv, send, recv, keep, load_sem, lift_sem, stage_sem, own_sem = refs[6:]
    ring = Ring(n, f)
    tok, width = tokens.shape
    head = width // n
    chips = ring.chips
    last = chips - 1
    capacity = rows_now.shape[1] // 2
    hidden_units = w_gate.shape[1]
    piece = tok // PIECES
    sign = 1 - 2 * ring.core
    onward = ring.at(ring.pos + sign + chips)
    local_units = hidden_units // f

    loads = [pltpu.make_async_copy(w_out, w_near, keep.at[0])]
    half_width = width // 2
    sources = []
    for j in range(f):
        cols = slice(j * local_units, (j + 1) * local_units)
        sources.append((w_gate.at[:, cols], 0, j))
        sources.append((w_down.at[:, cols], 2, j))
        if j:
            sources.append((w_up.at[pl.ds(0, half_width), cols], 1, j))
            sources.append((w_up.at[pl.ds(half_width, half_width), cols], 3, j))
        else:
            sources.append((w_up.at[:, cols], 1, j))
    for source, (target, kind, j) in zip(shards_in, sources):
        loads.append(pltpu.make_async_copy(source, target, load_sem.at[kind, j]))
    for load in loads:
        load.start()

    def chunk_of(i, other):
        return ring.at(
            ring.pos + (sign * (1 + i) if other else -sign * (1 + i)) + 2 * chips, other
        )

    def lift_copy(i, other):
        slot = lax.rem(i, 2)
        return pltpu.make_async_copy(
            upstream_all.at[chunk_of(i, other)],
            lift.at[slot, other],
            lift_sem.at[slot, other],
        )

    lift_copy(0, 0).start()
    lift_copy(0, 1).start()
    greet(ring, True, False)

    mine = pl.ds(pl.multiple_of(ring.me * head, head), head)

    before = lax.broadcasted_iota(jnp.int32, (tok, tok), 0)
    after = lax.broadcasted_iota(jnp.int32, (tok, tok), 1)
    earlier = jnp.where(before < after, 1.0, 0.0).astype(BF16)
    for c in range(n):
        here = jnp.where(routes_all[c] == ring.me, 1.0, 0.0)
        here = jnp.sum(here, 0, keepdims=True)
        count = dot(jnp.broadcast_to(here, (8, tok)).astype(BF16), earlier, MATMUL)
        places[c] = jnp.where(jnp.broadcast_to(here, (8, tok)) > 0.5, count, -1.0)

    loads[0].wait()
    tile = min(512, width)
    squares = jnp.zeros((tok, 1), F32)
    for start in range(0, width, tile):
        cols = slice(start, start + tile)
        value = tokens[:, cols].astype(F32) + dot(by_token[...], w_near[:, cols], MATMUL)
        middle[:, cols] = value
        squares = squares + jnp.sum(value * value, -1, keepdims=True)
    inverse = lax.rsqrt(squares / width + EPS)
    ring_in[last] = (middle[...] * inverse * gain[...]).astype(BF16)

    def hop(i, s):
        rows = pl.ds(s * piece, piece)
        source = lax.rem(i + last, chips)
        return remote(
            ring_in.at[source, rows],
            ring_in.at[i, rows],
            hop_send.at[i, s],
            hop_recv.at[i, s],
            {"seq": onward},
        )

    def share(i, s):
        rows = pl.ds(s * piece, piece)
        return remote(
            ring_in.at[i, rows],
            mate_near.at[i, rows],
            share_send.at[i, s],
            share_recv.at[i, s],
            {"seq": ring.mate},
        )

    for s in range(PIECES):
        hop(0, s).start()
    for s in range(PIECES):
        share(last, s).start()

    logits = dot(router[...], ring_in[last], BY_LAST)
    expd = jnp.exp(logits - jnp.max(logits, 0, keepdims=True))
    gate = expd / jnp.sum(expd, 0, keepdims=True)
    experts = lax.broadcasted_iota(jnp.int32, gate.shape, 0)
    named = jnp.zeros(gate.shape, F32)
    for k in range(routes.shape[0]):
        named = named + jnp.where(routes[k : k + 1, :] == experts, 1.0, 0.0)
    weights = gate * named
    for e in range(n):
        outgoing[e] = jnp.broadcast_to(weights[e : e + 1, :], (8, tok))

    def push(there):
        return remote(
            outgoing.at[there],
            weights_in.at[ring.me],
            send.at[1, there],
            recv.at[1, ring.me],
            {"seq": there},
        )

    def pushed(origin):
        return remote(
            outgoing.at[origin],
            weights_in.at[origin],
            send.at[1, origin],
            recv.at[1, origin],
            {"seq": origin},
        )

    for step in range(1, n):
        push(ring.peer(step)).start()
    weights_in[ring.me] = outgoing[ring.me]
    for load in loads[1:]:
        load.wait()

    def swap(i):
        return remote(
            d_mate_out.at[lax.rem(i, 2)],
            d_mate_in.at[i],
            swap_send.at[i],
            swap_recv.at[i],
            {"seq": ring.mate},
        )

    def sum_hop(i, s):
        rows = pl.ds(s * piece, piece)
        return remote(
            going.at[lax.rem(i, 2), rows],
            coming.at[i, rows],
            sum_send.at[i, s],
            sum_recv.at[i, s],
            {"seq": onward},
        )

    def sum_step(i):
        swap(i).wait_recv()

        @pl.when(i >= 2)
        def _():
            for s in range(PIECES):
                sum_hop(i - 2, s).wait_send()

        for s in range(PIECES):
            rows = pl.ds(s * piece, piece)

            @pl.when(i > 0)
            def _():
                sum_hop(i - 1, s).wait_recv()
                own[rows, :] = own[rows, :] + coming[i - 1, rows].astype(F32)

            value = own[rows, :] + d_mate_in[i, rows].astype(F32)
            going[lax.rem(i, 2), rows] = value.astype(BF16)
            sum_hop(i, s).start()

    def give(kind, target, other, slot):
        chunk = target
        source, sink = [
            (rows_now, rows_out),
            (d_now, d_out),
            (inner_now, inner_out),
            (d_gate_now, d_gate_out),
            (d_up_now, d_up_out),
            (moe_now, moe_out),
        ][kind]
        size = tok if kind == 5 else capacity
        return pltpu.make_async_copy(
            source.at[slot, pl.ds(other * size, size)],
            sink.at[chunk],
            stage_sem.at[slot, kind, other],
        )

    def keep_hidden(i, other):
        return pltpu.make_async_copy(
            (mate_near if other else ring_in).at[i, :, mine],
            own_hidden.at[chunk_of(i, other)],
            own_sem.at[other, i],
        )

    def report(there, slot, other):
        return remote(
            d_weight.at[slot, other],
            arrived.at[ring.me],
            send.at[2, there],
            recv.at[2, ring.me],
            {"seq": there},
        )

    def reported(origin):
        return remote(
            d_weight.at[0, 0],
            arrived.at[origin],
            send.at[2, origin],
            recv.at[2, origin],
            {"seq": origin},
        )

    def pass_on(i):
        for s in range(PIECES):
            hop(i, s).wait_recv()

            @pl.when(i < last - 1)
            def _():
                hop(i + 1, s).start()

            share(i, s).start()

    def work(i):
        slot = lax.rem(i, 2)
        chunks = (chunk_of(i, 0), chunk_of(i, 1))
        for s in range(PIECES):
            share(i, s).wait_recv()
        keep_hidden(i, 0).start()
        keep_hidden(i, 1).start()
        for other in (0, 1):
            lift_copy(i, other).wait()

        @pl.when(i < last)
        def _():
            lift_copy(i + 1, 0).start()
            lift_copy(i + 1, 1).start()
            pushed(chunks[0]).wait_recv()

        pushed(chunks[1]).wait_recv()

        @pl.when(i >= 2)
        def _():
            for kind in range(6):
                for other in (0, 1):
                    give(kind, chunks[other], other, slot).wait()
            swap(i - 2).wait_send()
            for other in (0, 1):
                report(chunk_of(i - 2, other), slot, other).wait_send()

        slots = lax.broadcasted_iota(jnp.int32, (capacity, tok), 0).astype(F32)
        picks, rates = [], []
        for other in (0, 1):
            rows = slice(other * capacity, (other + 1) * capacity)
            where = slots == jnp.broadcast_to(places[chunks[other], 0:1, :], (capacity, tok))
            pick = jnp.where(where, 1.0, 0.0)
            low = pick.astype(BF16)
            source = mate_near.at[i] if other else ring_in.at[i]
            share_of = weights_in[chunks[other], 0:1, :]
            rate = jnp.sum(jnp.where(where, share_of, 0.0), -1, keepdims=True)
            for start in range(0, width, tile):
                cols = slice(start, start + tile)
                rows_now[slot, rows, cols] = dot(low, source[:, cols], MATMUL).astype(BF16)
                picked = dot(low, lift[slot, other, :, cols], MATMUL)
                lifted[rows, cols] = picked.astype(BF16)
                d_now[slot, rows, cols] = (rate * picked).astype(BF16)
            picks.append((low, where))
            rates.append(rate)
        rate = jnp.concatenate(rates, 0)
        unit = min(256, hidden_units)
        for start in range(0, hidden_units, unit):
            cols = slice(start, start + unit)
            gate_act = dot(rows_now[slot], w_gate[:, cols], MATMUL)
            up_act = dot(rows_now[slot], w_up[:, cols], MATMUL)
            d_inner = dot(d_now[slot], w_down[:, cols], MATMUL)
            sigma = 1.0 / (1.0 + jnp.exp(-gate_act))
            silu = gate_act * sigma
            inner_now[slot, :, cols] = (silu * up_act).astype(BF16)
            d_gate_now[slot, :, cols] = (
                d_inner * up_act * sigma * (1.0 + gate_act * (1.0 - sigma))
            ).astype(BF16)
            d_up_now[slot, :, cols] = (d_inner * silu).astype(BF16)
        inner_product = jnp.zeros((2 * capacity, 1), F32)
        for start in range(0, width, tile):
            cols = slice(start, start + tile)
            produced = dot(inner_now[slot], w_down[cols, :], BY_LAST)
            produced = produced.astype(BF16).astype(F32)
            inner_product = inner_product + jnp.sum(
                produced * lifted[:, cols].astype(F32), -1, keepdims=True
            )
            scaled = (rate * produced).astype(BF16)
            d_rows = dot(d_gate_now[slot], w_gate[cols, :], BY_LAST)
            d_rows = (d_rows + dot(d_up_now[slot], w_up[cols, :], BY_LAST)).astype(BF16)
            for other in (0, 1):
                rows = slice(other * capacity, (other + 1) * capacity)
                low = picks[other][0]
                moe_now[slot, other * tok : (other + 1) * tok, cols] = dot(
                    low, scaled[rows], BY_FIRST
                ).astype(BF16)
                spread_rows = dot(low, d_rows[rows], BY_FIRST)
                if other:
                    d_mate_out[slot, :, cols] = spread_rows.astype(BF16)
                else:
                    own[:, cols] = spread_rows
        swap(i).start()
        for kind in range(6):
            for other in (0, 1):
                give(kind, chunks[other], other, slot).start()
        for other in (0, 1):
            rows = slice(other * capacity, (other + 1) * capacity)
            value = jnp.sum(
                jnp.where(picks[other][1], inner_product[rows], 0.0), 0, keepdims=True
            )
            d_weight[slot, other] = jnp.broadcast_to(value, (8, tok))
        report(chunks[1], slot, 1).start()

        @pl.when(i < last)
        def _():
            report(chunks[0], slot, 0).start()

    pass_on(0)
    work(0)

    def body(i, carry):
        @pl.when(i < last)
        def _():
            pass_on(i)

        sum_step(i - 1)
        work(i)
        return carry

    lax.fori_loop(1, chips, body, 0)
    arrived[ring.me] = d_weight[last % 2, 0]
    for step in range(1, n):
        reported(ring.peer(step)).wait_recv()
    gate_back = jnp.concatenate([arrived[e, 0:1, :] for e in range(n)], 0)
    gate_back = gate * (gate_back - jnp.sum(gate * gate_back, 0, keepdims=True))
    d_logits[...] = gate_back.astype(BF16)

    def publish(step):
        return remote(
            d_logits,
            d_logits_all.at[ring.me],
            send.at[4, step],
            recv.at[4, step],
            {"seq": ring.peer(step)},
        )

    kept = pltpu.make_async_copy(d_logits, d_logits_all.at[ring.me], keep.at[1])
    swap(last).wait_recv()
    for s in range(PIECES):
        rows = pl.ds(s * piece, piece)
        sum_hop(last - 1, s).wait_recv()
        value = own[rows, :] + d_mate_in[last, rows].astype(F32)
        own[rows, :] = value + coming[last - 1, rows].astype(F32)
    d_hidden = own[...] + dot(gate_back.astype(BF16), router[...], BY_FIRST)
    value = middle[...]
    inner = jnp.mean(value * gain[...] * d_hidden, -1, keepdims=True)
    gain_two[...] = jnp.sum(value * inverse * d_hidden, 0, keepdims=True)
    d_value = inverse * gain[...] * d_hidden - value * (inverse * inverse * inverse) * inner
    d_value = upstream[...].astype(F32) + d_value
    d_middle[...] = d_value
    d_attn[...] = d_value.astype(BF16)
    for start in range(0, width, tile):
        cols = slice(start, start + tile)
        d_by_token[:, cols] = dot(d_attn[...], w_near[cols, :], BY_LAST).astype(BF16)
    for step in range(1, n):
        publish(step).start()
    kept.start()

    for s in range(PIECES):
        share(last, s).wait_send()

    def settle(i, carry):
        for s in range(PIECES):
            hop(i, s).wait_send()
            share(i, s).wait_send()
        for other in (0, 1):
            keep_hidden(i, other).wait()
        return carry

    lax.fori_loop(0, last, settle, 0)
    for other in (0, 1):
        keep_hidden(last, other).wait()
    for s in range(PIECES):
        sum_hop(last - 2, s).wait_send()
        sum_hop(last - 1, s).wait_send()
    for i in (last - 1, last):
        swap(i).wait_send()
        for other in (0, 1):
            for kind in range(6):
                give(kind, chunk_of(i, other), other, i % 2).wait()
            if other or i < last:
                report(chunk_of(i, other), i % 2, other).wait_send()
    for step in range(1, n):
        push(ring.peer(step)).wait_send()
    for step in range(1, n):
        publish(step).wait()
    kept.wait()


def core_stage(
    n, f, by_token, w_out, tokens, upstream, gain, router, routes, routes_all, upstream_all, halves
):
    tok, width = tokens.shape
    experts = router.shape[0]
    units = f * halves[0].shape[1]
    capacity = min(tok, 5 * tok * TOPK // (4 * experts))
    chips = n // 2
    kind = pltpu.SemaphoreType.DMA
    shape = jax.ShapeDtypeStruct
    rows = 2 * capacity
    return pl.pallas_call(
        partial(core_kernel, n, f),
        out_shape=[
            shape((tok, width), F32),
            shape((tok, width), F32),
            shape((tok, width), BF16),
            shape((tok, width), BF16),
            shape((n, experts, tok), BF16),
            shape((1, width), F32),
            shape((n, tok, width // n), BF16),
            shape((n, capacity, width), BF16),
            shape((n, capacity, width), BF16),
            shape((n, capacity, units), BF16),
            shape((n, capacity, units), BF16),
            shape((n, capacity, units), BF16),
            shape((n, tok, width), BF16),
        ],
        in_specs=[VMEM, ANY] + [VMEM] * 6 + [ANY] * (4 * f),
        out_specs=[VMEM] * 4 + [ANY, VMEM] + [ANY] * 7,
        scratch_shapes=[
            pltpu.VMEM((width, width), BF16),
            pltpu.VMEM((width, units), BF16),
            pltpu.VMEM((width, units), BF16),
            pltpu.VMEM((width, units), BF16),
            pltpu.VMEM((experts, tok), BF16),
            pltpu.VMEM((n, 8, tok), F32),
            pltpu.VMEM((n, 8, tok), F32),
            pltpu.VMEM((n, 8, tok), F32),
            pltpu.VMEM((chips, tok, width), BF16),
            pltpu.VMEM((chips, tok, width), BF16),
            pltpu.VMEM((chips, tok, width), BF16),
            pltpu.VMEM((chips - 1, tok, width), BF16),
            pltpu.VMEM((2, tok, width), BF16),
            pltpu.VMEM((2, tok, width), BF16),
            pltpu.VMEM((tok, width), F32),
            pltpu.VMEM((2, 2, tok, width), BF16),
            pltpu.VMEM((2, rows, width), BF16),
            pltpu.VMEM((rows, width), BF16),
            pltpu.VMEM((2, rows, width), BF16),
            pltpu.VMEM((2, rows, units), BF16),
            pltpu.VMEM((2, rows, units), BF16),
            pltpu.VMEM((2, rows, units), BF16),
            pltpu.VMEM((2, 2 * tok, width), BF16),
            pltpu.VMEM((2, 2, 8, tok), F32),
            pltpu.VMEM((n, 8, tok), F32),
            kind((chips, PIECES)),
            kind((chips, PIECES)),
            kind((chips, PIECES)),
            kind((chips, PIECES)),
            kind((chips,)),
            kind((chips,)),
            kind((chips, PIECES)),
            kind((chips, PIECES)),
            kind((5, n)),
            kind((5, n)),
            kind((2,)),
            kind((4, f)),
            kind((2, 2)),
            kind((2, 6, 2)),
            kind((2, chips)),
        ],
        compiler_params=pltpu.CompilerParams(
            collective_id=1, has_side_effects=True, vmem_limit_bytes=67_000_000
        ),
        name="core_stage",
    )(by_token, w_out, tokens, upstream, gain, router, routes, routes_all, upstream_all, *halves)


def last_kernel(n, f, *refs):
    d_mixed, w_head, qkv_part, tokens, gain, d_middle, gain_two, gain_head = refs[:8]
    middle, proj, router, moe_part = refs[8:12]
    far_refs = refs[12:17]
    d_inputs, qkv_out, gains_out, second_in, third_in, grads_out, result = refs[17:24]
    proj_out, router_out = refs[24:26]
    beside_rows, summed, qkv_rows, gain_rows, gain_in, gain_side, stage, far_stage = refs[26:34]
    proj_low, proj_in, router_low = refs[34:37]
    near_refs = refs[37:42]
    rows_in, d_in, d_gate, d_up, inner_in = near_refs
    buffers, fold_sems = refs[42:47], refs[47:51]
    stored_buffers, stored_sems = refs[51:55], refs[55:60]
    side_send, side_recv, send, recv, keep, stage_sem, load_sem, far_send, far_recv = refs[60:]
    ring = Ring(n, f)
    _, width = tokens.shape
    slice_width = width // n
    units = grads_out.shape[2]
    chips = ring.chips
    size = width // chips
    loads = [
        pltpu.make_async_copy(source.at[:, :units] if k == 2 else source, target, load_sem.at[k])
        for k, (source, target) in enumerate(zip(far_refs, near_refs))
    ]
    greet(ring, True, True)

    def side(step):
        there = ring.beside(step)
        return remote(
            qkv_part.at[there],
            beside_rows.at[step - 1],
            side_send.at[0, step],
            side_recv.at[0, step],
            {"fsdp": there},
        )

    for step in range(1, f):
        side(step).start()

    def proj_side(step):
        there = ring.beside(step)
        return remote(
            proj_low.at[there],
            proj_in.at[step - 1],
            side_send.at[3, step],
            side_recv.at[3, step],
            {"fsdp": there},
        )

    def router_side(step):
        return remote(
            router_low.at[0],
            router_low.at[step],
            side_send.at[4, step],
            side_recv.at[4, step],
            {"fsdp": ring.beside(step)},
        )

    for x in range(f):
        proj_low[x] = proj[x].astype(BF16)
    router_low[0] = router[...].astype(BF16)
    for step in range(1, f):
        proj_side(step).start()
        router_side(step).start()

    def part(chunk, target):
        tile = min(512, width)
        for start in range(0, width, tile):
            cols = slice(start, start + tile)
            target[:, cols] = dot(d_mixed[chunk], w_head[cols, :], BY_LAST).astype(target.dtype)

    fold = Fold(ring, part, buffers, fold_sems)

    def finish(rows, value):
        d_inputs[rows, :] = value

    def store(i, which):
        these = pl.ds(pl.multiple_of(i * size, size), size)
        slot = lax.rem(i, 2)
        return pltpu.make_async_copy(
            stage.at[slot, which], grads_out.at[which, these], stage_sem.at[slot, which]
        )

    def filler(i):
        these = pl.ds(pl.multiple_of(i * size, size), size)
        slot = lax.rem(i, 2)
        pairs = ((rows_in, d_gate), (rows_in, d_up), (d_in, inner_in))
        for which, (left, right) in enumerate(pairs):

            @pl.when(i >= 2)
            def _():
                store(i - 2, which).wait()

            stage[slot, which] = dot(left[:, these], right[:, :units], BY_FIRST).astype(BF16)
            store(i, which).start()
        afar(i)

    def far(kind, i, j):
        these = pl.ds(pl.multiple_of(i * size, size), size)
        return remote(
            far_stage.at[lax.rem(i, 2), kind, j],
            [second_in, third_in][kind].at[j, these],
            far_send.at[kind, i, j],
            far_recv.at[kind, i, j],
            {"fsdp": ring.beside(f - 1 - j)},
        )

    def afar(i):
        these = pl.ds(pl.multiple_of(i * size, size), size)
        slot = lax.rem(i, 2)

        def make(kind, first_tile, left, right):
            @pl.when(i >= first_tile + 2)
            def _():
                for j in range(f - 1):
                    far(kind, i - 2, j).wait_send()

            @pl.when(i >= first_tile)
            def _():
                for j in range(f - 1):
                    part = slice((j + 1) * units, (j + 2) * units)
                    value = dot(left[:, these], right[:, part], BY_FIRST)
                    far_stage[slot, kind, j] = value.astype(BF16)
                    far(kind, i, j).start()

        make(0, EARLY, rows_in, d_up)
        make(1, 0, d_in, inner_in)

    def push(step):
        there = ring.peer(step)
        return remote(
            summed.at[there],
            qkv_rows.at[ring.me],
            send.at[0, step],
            recv.at[0, step],
            {"seq": there},
        )

    local = pltpu.make_async_copy(summed.at[ring.me], qkv_rows.at[ring.me], keep.at[0])

    stored = Stored(ring, moe_part, stored_buffers, stored_sems)
    fold.produce(0)
    stored.begin()
    for load in loads:
        load.start()
    fold.step(0)
    stored.step(0)
    for load in loads:
        load.wait()
    filler(0)
    fold.run(finish, filler, stored.step)

    def settle(rows, value):
        result[rows, :] = (middle[rows, :] + value).astype(BF16)

    stored.close(settle)
    value = tokens[...].astype(F32)
    grad = d_inputs[...]
    inverse = lax.rsqrt(jnp.mean(value * value, -1, keepdims=True) + EPS)
    inner = jnp.mean(value * gain[...] * grad, -1, keepdims=True)
    gain_rows[...] = jnp.zeros_like(gain_rows)
    gain_rows[0:1, :] = jnp.sum(value * inverse * grad, 0, keepdims=True)
    gain_rows[1:2, :] = gain_two[...]

    def gains(step):
        there = ring.peer(step)
        cols = pl.ds(pl.multiple_of(there * slice_width, slice_width), slice_width)
        return remote(
            gain_rows.at[:, cols],
            gain_in.at[ring.me],
            send.at[1, step],
            recv.at[1, step],
            {"seq": there},
        )

    mine = pl.ds(pl.multiple_of(ring.me * slice_width, slice_width), slice_width)
    kept = pltpu.make_async_copy(gain_rows.at[:, mine], gain_in.at[ring.me], keep.at[1])
    for step in range(1, n):
        gains(step).start()
    kept.start()
    d_value = inverse * gain[...] * grad - value * (inverse * inverse * inverse) * inner
    d_inputs[...] = d_middle[...] + d_value
    for step in range(1, f):
        side(step).wait_recv()

    def add(block, carry):
        value = qkv_part[ring.mine, block].astype(F32)
        for step in range(1, f):
            value = value + beside_rows[step - 1, block].astype(F32)
        summed[block] = value.astype(BF16)
        return carry

    lax.fori_loop(0, n, add, 0)
    for step in range(1, n):
        push(step).start()
    local.start()
    for step in range(1, n):
        gains(step).wait()
    kept.wait()
    total = gain_head[...]
    for device in range(n):
        total = total + gain_in[device]
    gain_side[0] = total

    def sums(step):
        return remote(
            gain_side.at[0],
            gain_side.at[step],
            side_send.at[1, step],
            side_recv.at[1, step],
            {"fsdp": ring.beside(step)},
        )

    for step in range(1, f):
        sums(step).start()
    proj_total = proj[ring.mine]
    router_total = router[...]
    for step in range(1, f):
        proj_side(step).wait()
        router_side(step).wait()
        proj_total = proj_total + proj_in[step - 1].astype(F32)
        router_total = router_total + router_low[step].astype(F32)
    proj_out[...] = proj_total
    router_out[...] = router_total
    fold.close()
    for i in (chips - 2, chips - 1):
        for which in range(3):
            store(i, which).wait()
    for step in range(1, f):
        side(step).wait_send()
    for step in range(1, n):
        push(step).wait()
    local.wait()
    piece = qkv_rows.shape[2] // 3
    for h in range(n):
        for k in range(3):
            start = k * width + h * piece
            qkv_out[:, start : start + piece] = qkv_rows[
                h, :, k * piece : (k + 1) * piece
            ].astype(F32)
    for step in range(1, f):
        sums(step).wait()
        total = total + gain_side[step]
    gains_out[...] = total
    for j in range(f - 1):
        for kind, first_tile in ((0, EARLY), (1, 0)):
            for i in range(first_tile, chips):
                far(kind, i, j).wait_recv()
                if i >= chips - 2:
                    far(kind, i, j).wait_send()


def last_stage(
    n, f, d_mixed, w_head, qkv_part, tokens, gain, d_middle, gain_two, gain_head,
    middle, proj, router, moe_part, rows_in, d_in, d_gate, d_up, inner_in, second
):
    tok, width = tokens.shape
    rows, across = qkv_part.shape[2:]
    units = second.shape[2]
    kind = pltpu.SemaphoreType.DMA
    shape = jax.ShapeDtypeStruct
    return pl.pallas_call(
        partial(last_kernel, n, f),
        out_shape=[
            shape((tok, width), F32),
            shape((rows, n * across), F32),
            shape((8, width // n), F32),
            shape(second.shape, BF16),
            shape(second.shape, BF16),
            shape((3, width, units), BF16),
            shape((tok, width), BF16),
            shape((rows, width), F32),
            shape(router.shape, F32),
        ],
        in_specs=[VMEM] * 11 + [ANY] * 6,
        out_specs=[VMEM] * 3 + [ANY] * 3 + [VMEM] * 3,
        scratch_shapes=[
            pltpu.VMEM((max(f - 1, 1), n, rows, across), BF16),
            pltpu.VMEM((n, rows, across), BF16),
            pltpu.VMEM((n, rows, across), BF16),
            pltpu.VMEM((8, width), F32),
            pltpu.VMEM((n, 8, width // n), F32),
            pltpu.VMEM((f, 8, width // n), F32),
            pltpu.VMEM((2, 3, 2 * width // n, units), BF16),
            pltpu.VMEM((2, 2, max(f - 1, 1), 2 * width // n, units), BF16),
            pltpu.VMEM(proj.shape, BF16),
            pltpu.VMEM((max(f - 1, 1),) + proj.shape[1:], BF16),
            pltpu.VMEM((f,) + router.shape, BF16),
            pltpu.VMEM(rows_in.shape, BF16),
            pltpu.VMEM(rows_in.shape, BF16),
            pltpu.VMEM((rows_in.shape[0], units), BF16),
            pltpu.VMEM(d_up.shape, BF16),
            pltpu.VMEM(inner_in.shape, BF16),
        ]
        + Fold.buffers(n, tok, width)
        + Fold.semaphores(n)
        + Stored.buffers(n, tok, width)
        + Stored.semaphores(n)
        + [kind((5, f)), kind((5, f)), kind((2, n)), kind((2, n)), kind((2,)), kind((2, 3))]
        + [kind((5,))]
        + [kind((2, n // 2, max(f - 1, 1))), kind((2, n // 2, max(f - 1, 1)))],
        compiler_params=pltpu.CompilerParams(
            collective_id=4, has_side_effects=True, vmem_limit_bytes=67_000_000
        ),
        name="last_stage",
    )(
        d_mixed, w_head, qkv_part, tokens, gain, d_middle, gain_two, gain_head,
        middle, proj, router, moe_part, rows_in, d_in, d_gate, d_up, inner_in
    )


def angles_of(n, tok, head_size):
    half = head_size // 2
    freqs = 10000.0 ** (-jnp.arange(half, dtype=F32) / half)
    inside = jnp.arange(tok, dtype=jnp.int32)
    starts = jnp.arange(n, dtype=jnp.int32) * tok
    angles = jnp.concatenate([inside, starts]).astype(F32)[:, None] * freqs[None, :]
    both = jnp.stack([jnp.cos(angles), jnp.sin(angles)])
    both = jnp.concatenate([both, both], -1)
    return both[:, :tok], both[:, tok:, None, :]


def shift_fsdp(values, step, f):
    if step == 0:
        return values
    return lax.ppermute(values, "fsdp", [(i, (i + step) % f) for i in range(f)])


def shards(n, f, inputs, routes, w_qkv, w_out, w_router, norm_gains, w_gate, w_up, w_down, cotangent):
    tokens_low = inputs[0]
    upstream_low = cotangent[0]
    local_routes = routes[0].T
    mine = lax.axis_index("fsdp")
    tok, width = tokens_low.shape
    length = tok * n
    head_size = width // HEADS
    across = 3 * head_size
    rows = w_qkv.shape[0]
    experts = n * w_gate.shape[0]
    capacity = min(tok, 5 * tok * TOPK // (4 * experts))
    factor = head_size ** (-0.5)

    small = jnp.concatenate([w_router, norm_gains], 1)
    small = jnp.pad(small, ((0, 0), (0, 128 - small.shape[1])))
    (
        hidden_one,
        mixed,
        w_head,
        router,
        gains,
        routes_all,
        gate_near,
        up_near,
        w_out_all,
    ) = first_gather(n, f, tokens_low, w_qkv, small, local_routes, w_out, w_gate[0], w_up[0])
    w_out_all = w_out_all.reshape(width, width)
    up_low, down_low, _ = lax.optimization_barrier((w_up[0, width // 2 :], w_down[0], mixed))
    halves = [w_gate[0], w_down[0], w_up[0]]
    for j in range(1, f):
        up_rest = shift_fsdp(up_low, j, f)
        down = shift_fsdp(down_low, j, f)
        halves += [gate_near[j - 1], down, up_near[j - 1], up_rest]
    hidden_one = hidden_one.reshape(length, width)
    w_head = w_head.reshape(width, across)
    tables, starts = angles_of(n, tok, head_size)
    (
        queries,
        keys,
        values,
        attended,
        exact,
        sums,
        squares,
        upstream_all,
        by_token,
    ) = attention(n, f, mixed, tables, starts, gains, upstream_low, factor)

    (
        d_middle,
        middle,
        d_attn,
        d_attended,
        d_logits_all,
        gain_two,
        own_hidden,
        expert_rows,
        d_produced,
        inner,
        d_gate,
        d_up,
        moe_part,
    ) = core_stage(
        n,
        f,
        by_token,
        w_out_all,
        tokens_low,
        upstream_low,
        gains[3:4],
        router,
        local_routes,
        routes_all,
        upstream_all,
        halves,
    )
    flat = n * capacity
    units = w_gate.shape[2]
    expert_rows = expert_rows.reshape(flat, width)
    d_produced = d_produced.reshape(flat, width)
    inner, d_gate, d_up = (v.reshape(flat, f * units) for v in (inner, d_gate, d_up))
    d_mixed, gain_head, qkv_part, proj, router_part, first, second = attention_back(
        n,
        f,
        queries,
        keys,
        values,
        d_attended,
        sums,
        exact,
        mixed,
        tables,
        starts,
        gains,
        squares,
        d_attn,
        attended,
        own_hidden,
        d_logits_all,
        expert_rows,
        d_gate,
        d_up,
        hidden_one,
        rows,
        factor,
    )
    (
        grad_inputs,
        grad_qkv,
        gains_own,
        second_rest,
        third,
        grads_own,
        result,
        grad_proj,
        grad_router,
    ) = last_stage(
        n,
        f,
        d_mixed.reshape(n, tok, across),
        w_head,
        qkv_part,
        tokens_low,
        gains[0:1],
        d_middle,
        gain_two,
        gain_head,
        middle,
        proj.reshape(f, rows, width),
        router_part,
        moe_part,
        expert_rows,
        d_produced,
        d_gate,
        d_up,
        inner,
        second,
    )
    grad_router = lax.dynamic_slice_in_dim(grad_router, mine * rows, rows, 1).T
    split = EARLY * (width // (n // 2))
    grads = []
    for which in range(3):
        total = grads_own[which].astype(F32)
        for j in range(f - 1):
            if which == 1:
                late = jnp.arange(width)[:, None] >= split
                part = jnp.where(late, second_rest[j], second[j])
            else:
                part = (first if which == 0 else third)[j]
            total = total + part.astype(F32)
        grads.append(total[None])
    gains_out = jnp.stack([gains_own[0], gains_own[2], gains_own[3], gains_own[1]], 1)
    grad_gains = lax.dynamic_slice_in_dim(gains_out, mine * rows, rows, 0)
    return (
        result[None],
        grad_inputs[None],
        grad_qkv,
        grad_proj,
        grad_router,
        grad_gains,
        *grads,
    )


def solution(mesh):
    tokens = P("fsdp", "seq", None)
    split = P(("seq", "fsdp"), None)
    expert = P("seq", None, "fsdp")
    return jax.shard_map(
        partial(shards, mesh.shape["seq"], mesh.shape["fsdp"]),
        mesh=mesh,
        in_specs=(tokens, tokens, split, split, split, split, expert, expert, expert, tokens),
        out_specs=(tokens, tokens, split, split, split, split, expert, expert, expert),
        check_vma=False,
    )
```

```python
from functools import partial

import jax
import jax.numpy as jnp
from jax import lax
from jax.experimental import pallas as pl
from jax.experimental.pallas import tpu as pltpu
from jax.sharding import PartitionSpec as P

HEADS = 16
TOPK = 8
EPS = 1e-05
NEG = -1e30
F32 = jnp.float32
BF16 = jnp.bfloat16
MESH = pl.DeviceIdType.MESH
PIECES = 2
EARLY = 3
UPPER = 4
DOWN = 7
ANY = pl.BlockSpec(memory_space=pl.ANY)
VMEM = pl.BlockSpec(memory_space=pltpu.VMEM)
MATMUL = (((1,), (0,)), ((), ()))
BY_LAST = (((1,), (1,)), ((), ()))
BY_FIRST = (((0,), (0,)), ((), ()))


def dot(a, b, dims):
    return lax.dot_general(a, b, dims, preferred_element_type=F32)


class Ring:
    def __init__(self, n, f):
        self.n, self.f = n, f
        self.chips = n // 2
        self.half = self.chips // 2
        self.pairs_minor = f == 2
        self.me = lax.axis_index("seq")
        self.mine = lax.axis_index("fsdp")
        chip = self.me // 2
        self.core = self.me % 2
        if self.pairs_minor:
            along, side = chip // 2, chip % 2
        else:
            along, side = chip % self.half, chip // self.half
        self.pos = along + side * (self.chips - 1 - 2 * along)
        self.right = self.at(self.pos + 1)
        self.left = self.at(self.pos + self.chips - 1)
        self.mate = self.me + 1 - 2 * self.core
        self.sign = 1 - 2 * self.core
        self.onward = self.at(self.pos + self.sign + self.chips)

    def at(self, place, other=False):
        place = lax.rem(place + self.chips, self.chips)
        side = place // self.half
        along = place + side * (self.chips - 1 - 2 * place)
        chip = along * 2 + side if self.pairs_minor else side * self.half + along
        core = 1 - self.core if other else self.core
        return chip * 2 + core

    def peer(self, step):
        return lax.rem(self.me + step, self.n)

    def beside(self, step):
        return lax.rem(self.mine + step, self.f)


def greet(ring, everyone, beside):
    barrier = pltpu.get_barrier_semaphore()
    count = 0
    if everyone:

        def each_0(step, carry):
            pl.semaphore_signal(
                barrier, inc=1, device_id={"seq": ring.peer(step)}, device_id_type=MESH
            )
            return carry

        lax.fori_loop(1, ring.n, each_0, 0)
        count += ring.n - 1
    else:
        for other in (ring.right, ring.left, ring.mate):
            pl.semaphore_signal(barrier, inc=1, device_id={"seq": other}, device_id_type=MESH)
        count += 3
    if beside:
        for step in range(1, ring.f):
            pl.semaphore_signal(
                barrier, inc=1, device_id={"fsdp": ring.beside(step)}, device_id_type=MESH
            )
        count += ring.f - 1
    pl.semaphore_wait(barrier, count)


def remote(src, dst, send, recv, where):
    return pltpu.make_async_remote_copy(
        src_ref=src,
        dst_ref=dst,
        send_sem=send,
        recv_sem=recv,
        device_id=where,
        device_id_type=MESH,
    )


class Gather:
    def __init__(self, ring, own, out, sems):
        self.ring, self.own, self.out = ring, own, out
        self.send, self.recv, self.mate_send, self.mate_recv, self.keep = sems
        self.piece = own.shape[0] // (2 * PIECES)
        self.last = ring.chips - 1

    @staticmethod
    def semaphores(n):
        hops = n // 2 - 1
        kind = pltpu.SemaphoreType.DMA
        return [
            kind((2, hops, PIECES)),
            kind((2, hops, PIECES)),
            kind((2, hops + 1, PIECES)),
            kind((2, hops + 1, PIECES)),
            kind((1,)),
        ]

    def rows(self, way, s):
        return pl.ds((way * PIECES + s) * self.piece, self.piece)

    def hop(self, way, step, s, first):
        ring = self.ring
        chunk = ring.at(ring.pos - step if way == 0 else ring.pos + step)
        rows = self.rows(way, s)
        there = self.out.at[chunk, rows]
        return remote(
            self.own.at[rows] if first else there,
            there,
            self.send.at[way, step, s],
            self.recv.at[way, step, s],
            {"seq": ring.right if way == 0 else ring.left},
        )

    def share(self, way, step, s, first):
        ring = self.ring
        chunk = ring.at(ring.pos - step if way == 0 else ring.pos + step)
        rows = self.rows(way, s)
        there = self.out.at[chunk, rows]
        return remote(
            self.own.at[rows] if first else there,
            there,
            self.mate_send.at[way, step, s],
            self.mate_recv.at[way, step, s],
            {"seq": ring.mate},
        )

    def local(self):
        return pltpu.make_async_copy(self.own, self.out.at[self.ring.me], self.keep.at[0])

    def begin(self):
        for s in range(PIECES):
            for way in (0, 1):
                self.hop(way, 0, s, True).start()
        for s in range(PIECES):
            for way in (0, 1):
                self.share(way, 0, s, True).start()
        self.local().start()

    def pass_on(self, i):
        for s in range(PIECES):
            for way in (0, 1):
                self.hop(way, i, s, False).wait_recv()

                @pl.when(i + 1 < self.ring.chips - 1)
                def _():
                    self.hop(way, i + 1, s, False).start()

                self.share(way, i + 1, s, False).start()

    def run(self):
        def body(step, carry):
            self.pass_on(step)
            return carry

        lax.fori_loop(0, self.ring.chips - 1, body, 0)

    def finish(self):
        hops = self.ring.chips - 1

        def body(step, carry):
            for s in range(PIECES):
                for way in (0, 1):
                    self.hop(way, step, s, False).wait_send()
                    self.share(way, step, s, False).wait()
            return carry

        lax.fori_loop(0, hops, body, 0)
        for s in range(PIECES):
            for way in (0, 1):
                self.share(way, hops, s, False).wait()
        self.local().wait()


class Scatter:
    def __init__(self, ring, part, tok, width, buffers, sems):
        self.ring, self.part, self.tok, self.width = ring, part, tok, width
        self.mate_out, self.mate_in, self.own, self.going, self.coming = buffers
        self.send, self.recv, self.mate_send, self.mate_recv = sems
        self.piece = tok // (2 * PIECES)

    @staticmethod
    def buffers(n, tok, width):
        chips = n // 2
        return [
            pltpu.VMEM((chips, tok, width), BF16),
            pltpu.VMEM((chips, tok, width), BF16),
            pltpu.VMEM((2, tok, width), F32),
            pltpu.VMEM((chips - 1, tok, width), BF16),
            pltpu.VMEM((chips - 1, tok, width), BF16),
        ]

    @staticmethod
    def semaphores(n):
        chips = n // 2
        kind = pltpu.SemaphoreType.DMA
        return [
            kind((2, chips - 1, PIECES)),
            kind((2, chips - 1, PIECES)),
            kind((chips,)),
            kind((chips,)),
        ]

    def rows(self, way, s):
        return pl.ds((way * PIECES + s) * self.piece, self.piece)

    def exchange(self, i):
        return remote(
            self.mate_out.at[i],
            self.mate_in.at[i],
            self.mate_send.at[i],
            self.mate_recv.at[i],
            {"seq": self.ring.mate},
        )

    def hop(self, way, i, s):
        ring = self.ring
        rows = self.rows(way, s)
        return remote(
            self.going.at[i, rows],
            self.coming.at[i, rows],
            self.send.at[way, i, s],
            self.recv.at[way, i, s],
            {"seq": ring.right if way == 0 else ring.left},
        )

    def produce(self, i):
        ring = self.ring
        half = self.tok // 2
        places = (ring.pos - 1 - i, ring.pos + 1 + i)
        for way in (0, 1):
            chunk = ring.at(places[way] + ring.chips, True)
            self.part(chunk, way, self.mate_out, i)
        self.exchange(i).start()
        slot = lax.rem(i, 2)
        for way in (0, 1):
            chunk = ring.at(places[way] + ring.chips)
            self.part(chunk, way, self.own, slot)

    def step(self, i, first):
        self.exchange(i).wait_recv()
        slot = lax.rem(i, 2)
        for s in range(PIECES):
            for way in (0, 1):
                rows = self.rows(way, s)
                value = self.own[slot, rows] + self.mate_in[i, rows].astype(F32)
                if not first:
                    self.hop(way, i - 1, s).wait_recv()
                    value = value + self.coming[i - 1, rows].astype(F32)
                self.going[i, rows] = value.astype(BF16)
                self.hop(way, i, s).start()

    def run(self, finish, between=None):
        last = self.ring.chips - 1
        self.produce(0)
        self.produce(1)
        self.step(0, True)

        def body(i, carry):
            self.produce(i + 1)
            self.step(i, False)
            return carry

        if between is None:
            lax.fori_loop(1, last, body, 0)
        else:
            lax.fori_loop(1, last // 2 + 1, body, 0)
            between()
            lax.fori_loop(last // 2 + 1, last, body, 0)
        self.exchange(last).wait_recv()
        slot = last % 2
        for s in range(PIECES):
            for way in (0, 1):
                rows = self.rows(way, s)
                self.hop(way, last - 1, s).wait_recv()
                value = self.own[slot, rows] + self.mate_in[last, rows].astype(F32)
                value = value + self.coming[last - 1, rows].astype(F32)
                finish(rows, value)

    def close(self):
        last = self.ring.chips - 1

        def body(i, carry):
            self.exchange(i).wait_send()
            for s in range(PIECES):
                for way in (0, 1):
                    self.hop(way, i, s).wait_send()
            return carry

        lax.fori_loop(0, last, body, 0)
        self.exchange(last).wait_send()


class Walk:
    def __init__(self, ring, own, out, sems):
        self.ring, self.own, self.out = ring, own, out
        self.send, self.recv, self.share_send, self.share_recv, self.keep = sems
        self.piece = own.shape[0] // PIECES
        self.last = ring.chips - 1

    @staticmethod
    def semaphores(n):
        kind = pltpu.SemaphoreType.DMA
        return [kind((n // 2, PIECES)) for _ in range(4)] + [kind((1,))]

    def block(self, i):
        ring = self.ring
        return ring.at(ring.pos - ring.sign * i + 2 * ring.chips)

    def hop(self, i, s, first=False):
        rows = pl.ds(s * self.piece, self.piece)
        there = self.out.at[self.block(i), rows]
        return remote(
            self.own.at[rows] if first else there,
            there,
            self.send.at[i, s],
            self.recv.at[i, s],
            {"seq": self.ring.onward},
        )

    def share(self, i, s, first=False):
        rows = pl.ds(s * self.piece, self.piece)
        there = self.out.at[self.block(i), rows]
        return remote(
            self.own.at[rows] if first else there,
            there,
            self.share_send.at[i, s],
            self.share_recv.at[i, s],
            {"seq": self.ring.mate},
        )

    def local(self):
        return pltpu.make_async_copy(self.own, self.out.at[self.ring.me], self.keep.at[0])

    def begin(self):
        for s in range(PIECES):
            self.hop(0, s, True).start()
        for s in range(PIECES):
            self.share(0, s, True).start()
        self.local().start()

    def pass_on(self, i):
        for s in range(PIECES):
            self.hop(i, s).wait_recv()

            @pl.when(i + 1 < self.last)
            def _():
                self.hop(i + 1, s).start()

            self.share(i + 1, s).start()

    def finish(self):
        def body(i, carry):
            for s in range(PIECES):
                self.hop(i, s).wait_send()
                self.share(i, s).wait()
            return carry

        lax.fori_loop(0, self.last, body, 0)
        for s in range(PIECES):
            self.share(self.last, s).wait()
        self.local().wait()


class Fold:
    def __init__(self, ring, part, buffers, sems):
        self.ring, self.part = ring, part
        self.mate_out, self.mate_in, self.own, self.going, self.coming = buffers
        self.swap_send, self.swap_recv, self.send, self.recv = sems
        self.piece = self.own.shape[0] // PIECES
        self.last = ring.chips - 1

    @staticmethod
    def buffers(n, tok, width):
        chips = n // 2
        return [
            pltpu.VMEM((2, tok, width), BF16),
            pltpu.VMEM((chips, tok, width), BF16),
            pltpu.VMEM((tok, width), F32),
            pltpu.VMEM((2, tok, width), BF16),
            pltpu.VMEM((chips - 1, tok, width), BF16),
        ]

    @staticmethod
    def semaphores(n):
        chips = n // 2
        kind = pltpu.SemaphoreType.DMA
        return [kind((chips,)), kind((chips,)), kind((chips, PIECES)), kind((chips, PIECES))]

    def swap(self, i):
        return remote(
            self.mate_out.at[lax.rem(i, 2)],
            self.mate_in.at[i],
            self.swap_send.at[i],
            self.swap_recv.at[i],
            {"seq": self.ring.mate},
        )

    def hop(self, i, s):
        rows = pl.ds(s * self.piece, self.piece)
        return remote(
            self.going.at[lax.rem(i, 2), rows],
            self.coming.at[i, rows],
            self.send.at[i, s],
            self.recv.at[i, s],
            {"seq": self.ring.onward},
        )

    def produce(self, i):
        ring = self.ring

        @pl.when(i >= 2)
        def _():
            self.swap(i - 2).wait_send()

        slot = lax.rem(i, 2)
        there = ring.at(ring.pos + ring.sign * (1 + i) + 2 * ring.chips, True)
        self.part(there, self.mate_out.at[slot])
        self.swap(i).start()
        here = ring.at(ring.pos - ring.sign * (1 + i) + 2 * ring.chips)
        self.part(here, self.own)

    def step(self, i):
        self.swap(i).wait_recv()

        @pl.when(i >= 2)
        def _():
            for s in range(PIECES):
                self.hop(i - 2, s).wait_send()

        for s in range(PIECES):
            rows = pl.ds(s * self.piece, self.piece)

            @pl.when(i > 0)
            def _():
                self.hop(i - 1, s).wait_recv()
                self.own[rows, :] = self.own[rows, :] + self.coming[i - 1, rows].astype(F32)

            value = self.own[rows, :] + self.mate_in[i, rows].astype(F32)
            self.going[lax.rem(i, 2), rows] = value.astype(BF16)
            self.hop(i, s).start()

    def run(self, finish, filler, before, after):
        last = self.last

        def body(i, carry):
            self.produce(i)
            before(i)
            self.step(i)
            after(i)
            filler(i)
            return carry

        lax.fori_loop(0, last, body, 0)
        self.produce(last)
        filler(last)
        self.swap(last).wait_recv()
        for s in range(PIECES):
            rows = pl.ds(s * self.piece, self.piece)
            self.hop(last - 1, s).wait_recv()
            value = self.own[rows, :] + self.mate_in[last, rows].astype(F32)
            finish(rows, value + self.coming[last - 1, rows].astype(F32))

    def close(self):
        last = self.last
        for s in range(PIECES):
            self.hop(last - 2, s).wait_send()
            self.hop(last - 1, s).wait_send()
        self.swap(last - 1).wait_send()
        self.swap(last).wait_send()


class Stored:
    def __init__(self, ring, parts, buffers, sems):
        self.ring, self.parts = ring, parts
        self.near, self.mate_in, self.going, self.coming = buffers
        self.swap_send, self.swap_recv, self.send, self.recv, self.load_sem = sems
        self.piece = self.near.shape[1] // PIECES
        self.last = ring.chips - 1

    @staticmethod
    def buffers(n, tok, width):
        chips = n // 2
        return [
            pltpu.VMEM((2, tok, width), BF16),
            pltpu.VMEM((chips, tok, width), BF16),
            pltpu.VMEM((2, tok, width), BF16),
            pltpu.VMEM((chips - 1, tok, width), BF16),
        ]

    @staticmethod
    def semaphores(n):
        chips = n // 2
        kind = pltpu.SemaphoreType.DMA
        return [
            kind((chips,)),
            kind((chips,)),
            kind((chips, PIECES)),
            kind((chips, PIECES)),
            kind((2,)),
        ]

    def swap(self, i):
        ring = self.ring
        there = ring.at(ring.pos + ring.sign * (1 + i) + 2 * ring.chips, True)
        return remote(
            self.parts.at[there],
            self.mate_in.at[i],
            self.swap_send.at[i],
            self.swap_recv.at[i],
            {"seq": ring.mate},
        )

    def load(self, i):
        ring = self.ring
        here = ring.at(ring.pos - ring.sign * (1 + i) + 2 * ring.chips)
        slot = lax.rem(i, 2)
        return pltpu.make_async_copy(
            self.parts.at[here], self.near.at[slot], self.load_sem.at[slot]
        )

    def hop(self, i, s):
        rows = pl.ds(s * self.piece, self.piece)
        return remote(
            self.going.at[lax.rem(i, 2), rows],
            self.coming.at[i, rows],
            self.send.at[i, s],
            self.recv.at[i, s],
            {"seq": self.ring.onward},
        )

    def begin(self):
        self.load(0).start()
        self.swap(0).start()
        self.swap(1).start()

    def step(self, i):
        self.load(i).wait()
        self.load(i + 1).start()
        self.swap(i).wait_recv()

        @pl.when(i + 2 <= self.last)
        def _():
            self.swap(i + 2).start()

        slot = lax.rem(i, 2)

        @pl.when(i >= 2)
        def _():
            for s in range(PIECES):
                self.hop(i - 2, s).wait_send()

        for s in range(PIECES):
            rows = pl.ds(s * self.piece, self.piece)
            value = self.near[slot, rows].astype(F32) + self.mate_in[i, rows].astype(F32)
            self.going[slot, rows] = value.astype(BF16)

            @pl.when(i > 0)
            def _():
                self.hop(i - 1, s).wait_recv()
                total = self.near[slot, rows].astype(F32) + self.mate_in[i, rows].astype(F32)
                total = total + self.coming[i - 1, rows].astype(F32)
                self.going[slot, rows] = total.astype(BF16)

            self.hop(i, s).start()

    def close(self, finish):
        last = self.last
        self.load(last).wait()
        self.swap(last).wait_recv()
        for s in range(PIECES):
            rows = pl.ds(s * self.piece, self.piece)
            self.hop(last - 1, s).wait_recv()
            value = self.near[last % 2, rows].astype(F32) + self.mate_in[last, rows].astype(F32)
            finish(rows, value + self.coming[last - 1, rows].astype(F32))
            self.hop(last - 2, s).wait_send()
            self.hop(last - 1, s).wait_send()

        def body(i, carry):
            self.swap(i).wait_send()
            return carry

        lax.fori_loop(0, last + 1, body, 0)


def first_kernel(n, f, *refs):
    own, w_qkv, small, routes, w_out, w_gate, w_up = refs[:7]
    hidden_all, mixed, w_head, router, gains, routes_all, gate_near, up_near, out_all = refs[7:16]
    near, small_all, out_rows, by_head = refs[16:20]
    sems, out_sems = refs[20:25], refs[25:30]
    send, recv, beside_send, beside_recv, keep = refs[30:35]
    wide_send, wide_recv, row_send, row_recv, out_sem = refs[35:]
    ring = Ring(n, f)
    experts = router.shape[0]
    tok, width = own.shape
    rows = small.shape[0]
    hops = ring.chips - 1
    piece = width // ring.chips
    head = width // n
    for h in range(n):
        for k in range(3):
            start = k * width + h * head
            by_head[h, :, k * head : (k + 1) * head] = w_qkv[:, start : start + head]
    greet(ring, True, True)
    gather = Gather(ring, own, near, sems)
    gather_out = Gather(ring, out_rows, out_all, out_sems)
    out_mine = pl.ds(pl.multiple_of(ring.mine * rows, rows), rows)

    def push(kind, step):
        there = ring.peer(step)
        source, target = [
            (by_head.at[there], w_head.at[ring.me, ring.mine]),
            (small, small_all.at[ring.me, ring.mine]),
            (routes, routes_all.at[ring.me]),
        ][kind]
        return remote(
            source, target, send.at[kind, step], recv.at[kind, step], {"seq": there}
        )

    def aside(kind, step, over, first):
        origin = lax.rem(ring.me + n - step, n)
        block = [w_head, small_all][kind].at[origin, ring.mine]
        source = [by_head.at[ring.me], small][kind] if first else block
        return remote(
            source,
            block,
            beside_send.at[kind, step, over],
            beside_recv.at[kind, step, over],
            {"fsdp": ring.beside(over)},
        )

    def row(over):
        return remote(
            w_out,
            out_rows.at[out_mine],
            row_send.at[over],
            row_recv.at[over],
            {"fsdp": ring.beside(over)},
        )

    def wide(part, over):
        kind, part = divmod(part, ring.chips)
        these = pl.ds(part * piece, piece)
        return remote(
            [w_gate, w_up][kind].at[these],
            [gate_near, up_near][kind].at[over - 1, these],
            wide_send.at[kind, part, over],
            wide_recv.at[kind, part, over],
            {"fsdp": ring.beside(over)},
        )

    half_parts = ring.chips + ring.chips * UPPER // 8

    gather.begin()
    for over in range(1, f):
        row(over).start()
    copies = [
        pltpu.make_async_copy(by_head.at[ring.me], w_head.at[ring.me, ring.mine], keep.at[0]),
        pltpu.make_async_copy(small, small_all.at[ring.me, ring.mine], keep.at[1]),
        pltpu.make_async_copy(routes, routes_all.at[ring.me], keep.at[2]),
        pltpu.make_async_copy(w_out, out_rows.at[out_mine], keep.at[3]),
    ]
    for copy in copies:
        copy.start()

    def each_1(step, carry):
        for kind in (1, 0, 2):
            push(kind, step).start()
        return carry

    lax.fori_loop(1, n, each_1, 0)
    for over in range(1, f):
        aside(1, 0, over, True).start()
        aside(0, 0, over, True).start()
        wide(0, over).start()
    each = -(-(n - 1) // 3)
    parts = 1

    def widen(parts):
        if parts < half_parts:
            for over in range(1, f):
                wide(parts, over).start()
        return parts + 1

    for i in range(hops):
        gather.pass_on(i)
        if 2 <= i < 5:
            for step in range((i - 2) * each + 1, min((i - 1) * each, n - 1) + 1):
                for kind in (1, 0):
                    push(kind, step).wait_recv()
                    for over in range(1, f):
                        aside(kind, step, over, False).start()
        parts = widen(parts)
        while i >= 4 and parts < half_parts:
            parts = widen(parts)
        if i == hops - 2:
            copies[3].wait()
            for over in range(1, f):
                row(over).wait_recv()
            gather_out.begin()
    gather.finish()
    for copy in copies[:3]:
        copy.wait()

    def each_2(step, carry):
        push(2, step).wait_recv()
        for kind in (0, 1, 2):
            push(kind, step).wait_send()
        return carry

    lax.fori_loop(1, n, each_2, 0)

    def each_3(step, carry):
        for kind in (0, 1):
            for over in range(1, f):
                aside(kind, step, over, False).wait()
        return carry

    lax.fori_loop(0, n, each_3, 0)

    lanes = lax.broadcasted_iota(jnp.int32, (32, small.shape[1]), 1)
    places = lax.broadcasted_iota(jnp.int32, (32, small.shape[1]), 0)
    chosen = jnp.where(lanes == places, 1.0, 0.0).astype(BF16)
    for c in range(n):
        for x in range(f):
            start = (c * f + x) * rows
            flipped = dot(chosen, small_all[c, x], BY_LAST)
            router[:, start : start + rows] = flipped[0:experts, :].astype(BF16)
            gains[:, start : start + rows] = flipped[experts : experts + 8, :]

    def out(c):
        return pltpu.make_async_copy(near.at[c], hidden_all.at[c], out_sem.at[c])

    def project(c, carry):
        value = near[c].astype(F32)
        inverse = lax.rsqrt(jnp.mean(value * value, -1, keepdims=True) + EPS)
        near[c] = (value * inverse * gains[0:1, :]).astype(BF16)
        out(c).start()
        here = pl.ds(pl.multiple_of(c * tok, tok), tok)
        total = jnp.zeros((tok, w_head.shape[3]), F32)
        for k in range(n):
            for x in range(f):
                start = (k * f + x) * rows
                if (k * f + x) % (256 // rows):
                    continue
                wide_rows = 256 // rows
                if wide_rows <= f:
                    right = w_head[k, x : x + wide_rows]
                else:
                    right = w_head[k : k + wide_rows // f]
                right = right.reshape(256, w_head.shape[3])
                total = total + dot(near[c, :, start : start + 256], right, MATMUL)
        mixed[here, :] = total
        return carry

    while parts < half_parts:
        parts = widen(parts)

    def second_phase(i, carry):
        lax.fori_loop(n * i // hops, n * (i + 1) // hops, project, 0)
        gather_out.pass_on(i)
        return carry

    lax.fori_loop(0, hops, second_phase, 0)
    for c in range(n):
        out(c).wait()
    gather_out.finish()
    for over in range(1, f):
        row(over).wait_send()
        for part in range(half_parts):
            wide(part, over).wait()


def first_gather(n, f, own, w_qkv, small, routes, w_out, w_gate, w_up):
    tok, width = own.shape
    experts = n
    by_head = jax.ShapeDtypeStruct((n, w_qkv.shape[0], 3 * width // n), BF16)
    kind = pltpu.SemaphoreType.DMA
    shape = jax.ShapeDtypeStruct
    return pl.pallas_call(
        partial(first_kernel, n, f),
        out_shape=[
            shape((n, tok, width), BF16),
            shape((n * tok, by_head.shape[2]), F32),
            shape((n, f) + by_head.shape[1:], BF16),
            shape((experts, width), BF16),
            shape((8, width), F32),
            shape((n,) + routes.shape, jnp.int32),
            shape((max(f - 1, 1),) + w_gate.shape, BF16),
            shape((max(f - 1, 1), w_up.shape[0] * UPPER // 8, w_up.shape[1]), BF16),
            shape((n, f * w_out.shape[0], w_out.shape[1]), BF16),
        ],
        in_specs=[VMEM] * 5 + [ANY] * 2,
        out_specs=[ANY] + [VMEM] * 4 + [ANY] * 4,
        scratch_shapes=[
            pltpu.VMEM((n, tok, width), BF16),
            pltpu.VMEM((n, f) + small.shape, BF16),
            pltpu.VMEM((f * w_out.shape[0], w_out.shape[1]), BF16),
            pltpu.VMEM(by_head.shape, BF16),
        ]
        + Gather.semaphores(n)
        + Gather.semaphores(n)
        + [kind((3, n)), kind((3, n)), kind((2, n, f)), kind((2, n, f)), kind((4,))]
        + [kind((2, n // 2, f)), kind((2, n // 2, f)), kind((f,)), kind((f,)), kind((n,))],
        compiler_params=pltpu.CompilerParams(
            collective_id=0, has_side_effects=True, vmem_limit_bytes=67_000_000
        ),
        name="first_gather",
    )(own, w_qkv, small, routes, w_out, w_gate, w_up)


def blocks_of(length):
    block = min(512, length)
    return block, length // block


def across_lanes(value):
    ones = jnp.ones((8, value.shape[1]), F32)
    total = lax.dot_general(
        ones, value, BY_LAST, precision=lax.Precision.HIGHEST, preferred_element_type=F32
    )
    return total[0:1, :]


def to_column(table, index, lanes):
    rows = lax.broadcasted_iota(jnp.int32, (table.shape[0], lanes), 0)
    chosen = jnp.where(rows == index, 1.0, 0.0)
    return lax.dot_general(
        table, chosen, BY_FIRST, precision=lax.Precision.HIGHEST, preferred_element_type=F32
    )


def half_turn(value, first_sign):
    half = value.shape[1] // 2
    lanes = lax.broadcasted_iota(jnp.int32, value.shape, 1)
    sign = jnp.where(lanes < half, first_sign, -first_sign)
    return pltpu.roll(value, half, 1) * sign


def set_angles(n, tables, starts, cosine, sine):
    tok = tables.shape[1]

    def angles(c, carry):
        here = pl.ds(pl.multiple_of(c * tok, tok), tok)
        cosine[here, :] = starts[0, c] * tables[0] - starts[1, c] * tables[1]
        sine[here, :] = starts[1, c] * tables[0] + starts[0, c] * tables[1]
        return carry

    lax.fori_loop(0, n, angles, 0)


class Spread:
    def __init__(self, ring, block, out, sems):
        self.ring, self.block, self.out = ring, block, out
        self.send, self.recv, self.keep = sems

    @staticmethod
    def semaphores(n):
        kind = pltpu.SemaphoreType.DMA
        return [kind((n,)), kind((n,)), kind((1,))]

    def push(self, step):
        return remote(
            self.block,
            self.out.at[self.ring.me],
            self.send.at[step],
            self.recv.at[step],
            {"seq": self.ring.peer(step)},
        )

    def local(self):
        return pltpu.make_async_copy(self.block, self.out.at[self.ring.me], self.keep.at[0])

    def begin(self):

        def each_4(step, carry):
            self.push(step).start()
            return carry

        lax.fori_loop(1, self.ring.n, each_4, 0)
        self.local().start()

    def finish(self):

        def each_5(step, carry):
            self.push(step).wait()
            return carry

        lax.fori_loop(1, self.ring.n, each_5, 0)
        self.local().wait()

    def total(self):
        total = self.out[0]
        for device in range(1, self.ring.n):
            total = total + self.out[device]
        return total


def attention_kernel(n, f, factor, *refs):
    mixed, tables, starts, gains, upstream, w_up, w_down = refs[:7]
    q_ref, k_ref, v_ref, out_ref, exact_ref, sums_ref, squares = refs[7:14]
    upstream_all, by_token, up_rest, down_near = refs[14:18]
    partial_sums, arrived, cosine, sine = refs[18:22]
    sems, walk_sems = refs[22:25], refs[25:30]
    deal_send, deal_recv, deal_keep, wide_send, wide_recv = refs[30:]
    ring = Ring(n, f)
    length, head = q_ref.shape
    width = head * n
    block, count = blocks_of(length)
    greet(ring, True, True)
    rest = up_rest.shape[1]
    later = pl.ds(w_up.shape[0] - rest, rest)

    def wide(kind, over):
        return remote(
            [w_up.at[later], w_down.at[pl.ds(0, down_near.shape[1])]][kind],
            [up_rest, down_near][kind].at[over - 1],
            wide_send.at[kind, over],
            wide_recv.at[kind, over],
            {"fsdp": ring.beside(over)},
        )

    for over in range(1, f):
        wide(0, over).start()
        wide(1, over).start()
    walk = Gather(ring, upstream, upstream_all, walk_sems)
    last = walk.last
    mine = pl.ds(pl.multiple_of(ring.me * head, head), head)

    def deal(there):
        these = pl.ds(pl.multiple_of(there * tok, tok), tok)
        return remote(
            out_ref.at[these],
            by_token.at[:, mine],
            deal_send.at[there],
            deal_recv.at[ring.me],
            {"seq": there},
        )

    def dealt(origin):
        return remote(
            out_ref.at[pl.ds(0, tok)],
            by_token.at[:, pl.ds(pl.multiple_of(origin * head, head), head)],
            deal_send.at[origin],
            deal_recv.at[origin],
            {"seq": origin},
        )

    tok = tables.shape[1]

    def measure(b, carry):
        here = pl.ds(pl.multiple_of(b * block, block), block)
        for kind in (0, 1):
            raw = mixed[here, kind * head : (kind + 1) * head]
            partial_sums[pl.ds(kind * count + b, 1), :] = across_lanes(raw * raw)
        v_ref[here, :] = mixed[here, 2 * head :].astype(BF16)
        return carry

    lax.fori_loop(0, count, measure, 0)
    spread = Spread(ring, partial_sums, arrived, sems)
    spread.begin()
    walk.begin()

    set_angles(n, tables, starts, cosine, sine)
    spread.finish()
    squares[...] = spread.total()
    walk.pass_on(0)

    def prepare(b, carry):
        here = pl.ds(pl.multiple_of(b * block, block), block)
        for kind, target in ((0, q_ref), (1, k_ref)):
            inverse = lax.rsqrt(to_column(squares[...], kind * count + b, head) / width + EPS)
            raw = mixed[here, kind * head : (kind + 1) * head]
            normed = raw * inverse * gains[kind + 1 : kind + 2, mine]
            turned = half_turn(normed, -1.0)
            target[here, :] = (normed * cosine[here, :] + turned * sine[here, :]).astype(BF16)
        return carry

    lax.fori_loop(0, count, prepare, 0)
    rows = lax.broadcasted_iota(jnp.int32, (block, block), 0)
    cols = lax.broadcasted_iota(jnp.int32, (block, block), 1)

    def outer(i, carry):
        here = pl.ds(pl.multiple_of(i * block, block), block)
        part = q_ref[here, :]

        def inner(j, state, masked):
            top, total, acc = state
            there = pl.ds(pl.multiple_of(j * block, block), block)
            scores = dot(part, k_ref[there, :], BY_LAST) * factor
            if masked:
                scores = jnp.where(cols <= rows, scores, NEG)
            new = jnp.maximum(top, jnp.max(scores, -1, keepdims=True))
            scale = jnp.exp(top - new)
            expd = jnp.exp(scores - new)
            total = total * scale + jnp.sum(expd, -1, keepdims=True)
            acc = acc * scale + dot(expd.astype(BF16), v_ref[there, :], MATMUL)
            return new, total, acc

        state = (
            jnp.full((block, 1), NEG, F32),
            jnp.zeros((block, 1), F32),
            jnp.zeros((block, head), F32),
        )
        state = lax.fori_loop(0, i, lambda j, s: inner(j, s, False), state)
        top, total, acc = inner(i, state, True)
        exact = acc / total
        exact_ref[here, :] = exact
        out_ref[here, :] = exact.astype(BF16)
        column = jnp.broadcast_to(top + jnp.log(total), (block, 128))
        sums_ref[:, here] = jnp.transpose(column)[0:8, :]

        for r in range(block // tok):
            there = i * (block // tok) + r

            @pl.when(there != ring.me)
            def _():
                deal(there).start()

        @pl.when((i > 0) & (i < last))
        def _():
            walk.pass_on(i)

        return carry

    lax.fori_loop(0, count, outer, 0)
    these = pl.ds(pl.multiple_of(ring.me * tok, tok), tok)
    local = pltpu.make_async_copy(out_ref.at[these], by_token.at[:, mine], deal_keep.at[0])
    local.start()
    for i in range(count, last):
        walk.pass_on(i)
    walk.finish()

    def each_6(step, carry):
        deal(ring.peer(step)).wait_send()
        dealt(ring.peer(step)).wait_recv()
        return carry

    lax.fori_loop(1, n, each_6, 0)
    local.wait()
    for over in range(1, f):
        wide(0, over).wait()
        wide(1, over).wait()


def attention(n, f, mixed, tables, starts, gains, upstream, w_up, w_down, factor):
    length, head = mixed.shape[0], mixed.shape[1] // 3
    block, count = blocks_of(length)
    shape = jax.ShapeDtypeStruct
    return pl.pallas_call(
        partial(attention_kernel, n, f, factor),
        out_shape=[
            shape((length, head), BF16),
            shape((length, head), BF16),
            shape((length, head), BF16),
            shape((length, head), BF16),
            shape((length, head), F32),
            shape((8, length), F32),
            shape((2 * count, block), F32),
            shape((n,) + upstream.shape, BF16),
            shape((length // n, head * n), BF16),
            shape((max(f - 1, 1), w_up.shape[0] - w_up.shape[0] * UPPER // 8, w_up.shape[1]), BF16),
            shape((max(f - 1, 1), w_down.shape[0] * DOWN // 8, w_down.shape[1]), BF16),
        ],
        in_specs=[VMEM] * 5 + [ANY] * 2,
        out_specs=[VMEM] * 7 + [ANY, VMEM, ANY, ANY],
        scratch_shapes=[
            pltpu.VMEM((2 * count, block), F32),
            pltpu.VMEM((n, 2 * count, block), F32),
            pltpu.VMEM((length, head), F32),
            pltpu.VMEM((length, head), F32),
        ]
        + Spread.semaphores(n)
        + Gather.semaphores(n)
        + [pltpu.SemaphoreType.DMA((n,)), pltpu.SemaphoreType.DMA((n,))]
        + [pltpu.SemaphoreType.DMA((1,))]
        + [pltpu.SemaphoreType.DMA((2, f)), pltpu.SemaphoreType.DMA((2, f))],
        compiler_params=pltpu.CompilerParams(
            collective_id=5, has_side_effects=True, vmem_limit_bytes=67_000_000
        ),
        cost_estimate=pl.CostEstimate(
            flops=2 * length * length * head,
            transcendentals=length * length // 2,
            bytes_accessed=8 * length * head,
        ),
        name="attention",
    )(mixed, tables, starts, gains, upstream, w_up, w_down)


def attention_back_kernel(n, f, factor, *refs):
    q_ref, k_ref, v_ref, by_token, sums_ref, exact, mixed, tables, starts, gains, squares = refs[:11]
    d_attn, attended, own_hidden, d_logits = refs[11:15]
    far = refs[15:19]
    d_mixed, gain_head, qkv_part, proj, router, first_in, second_in = refs[19:26]
    dq_ref, dk_ref, dv_ref, delta, partial_sums, arrived, d_attn_all, first, d_ref = refs[26:35]
    cosine, sine = refs[35:37]
    near = refs[37:41]
    rows_in, d_gate, d_up, hidden = near
    walk_sems, spread_sems = refs[41:46], refs[46:49]
    load_sem, first_send, first_recv, deal_send, deal_recv, deal_keep = refs[49:]
    ring = Ring(n, f)
    length, head = q_ref.shape
    width = head * n
    units = first_in.shape[2]
    block, count = blocks_of(length)
    loads = [
        pltpu.make_async_copy(
            source.at[:, units:] if k in (1, 2) else source, target, load_sem.at[k]
        )
        for k, (source, target) in enumerate(zip(far, near))
    ]
    for load in loads:
        load.start()
    greet(ring, True, True)
    tok = d_attn.shape[0]
    here_rows = pl.ds(pl.multiple_of(ring.me * tok, tok), tok)
    mine = pl.ds(pl.multiple_of(ring.me * head, head), head)

    def deal(step):
        there = ring.peer(step)
        return remote(
            by_token.at[:, pl.ds(pl.multiple_of(there * head, head), head)],
            d_ref.at[here_rows],
            deal_send.at[step],
            deal_recv.at[step],
            {"seq": there},
        )

    local = pltpu.make_async_copy(
        by_token.at[:, pl.ds(pl.multiple_of(ring.me * head, head), head)],
        d_ref.at[here_rows],
        deal_keep.at[0],
    )

    def each_7(step, carry):
        deal(step).start()
        return carry

    lax.fori_loop(1, n, each_7, 0)
    local.start()
    walk = Gather(ring, d_attn, d_attn_all, walk_sems)
    walk.begin()
    last = walk.last
    tiles = ring.chips
    size = width // tiles

    def send_first(kind, at, j):
        these = pl.ds(pl.multiple_of(at * size, size), size)
        tile = kind * tiles + at
        return remote(
            first.at[tile, j],
            [first_in, second_in][kind].at[j, these],
            first_send.at[tile, j],
            first_recv.at[tile, j],
            {"fsdp": ring.beside(f - 1 - j)},
        )

    set_angles(n, tables, starts, cosine, sine)
    for load in loads[:3]:
        load.wait()

    def early(kind, right):
        def body(at, carry):
            these = pl.ds(pl.multiple_of(at * size, size), size)
            for j in range(f - 1):
                part = slice(j * units, (j + 1) * units)
                value = dot(rows_in[:, these], right[:, part], BY_FIRST)
                first[kind * tiles + at, j] = value.astype(BF16)
                send_first(kind, at, j).start()
            return carry

        lax.fori_loop(0, EARLY if kind else tiles, body, 0)

    early(0, d_gate)
    early(1, d_up)

    def each_8(step, carry):
        deal(step).wait()
        return carry

    lax.fori_loop(1, n, each_8, 0)
    local.wait()
    dq_ref[...] = jnp.zeros_like(dq_ref)

    def measure(b, carry):
        here = pl.ds(pl.multiple_of(b * block, block), block)
        value = across_lanes(d_ref[here, :].astype(F32) * exact[here, :])
        delta[:, here] = jnp.broadcast_to(value, (8, block))
        return carry

    lax.fori_loop(0, count, measure, 0)
    rows = lax.broadcasted_iota(jnp.int32, (block, block), 0)
    cols = lax.broadcasted_iota(jnp.int32, (block, block), 1)

    def outer(j, carry):
        there = pl.ds(pl.multiple_of(j * block, block), block)
        keys = k_ref[there, :]
        values = v_ref[there, :]

        def inner(i, state, masked):
            d_keys, d_values = state
            here = pl.ds(pl.multiple_of(i * block, block), block)
            part = q_ref[here, :]
            d_part = d_ref[here, :]
            scores = dot(keys, part, BY_LAST) * factor
            if masked:
                scores = jnp.where(rows <= cols, scores, NEG)
            probs = jnp.exp(scores - sums_ref[0:1, here])
            d_probs = dot(values, d_part, BY_LAST)
            d_scores = (probs * (d_probs - delta[0:1, here])).astype(BF16)
            d_values = d_values + dot(probs.astype(BF16), d_part, MATMUL)
            d_keys = d_keys + dot(d_scores, part, MATMUL)
            dq_ref[here, :] += dot(d_scores, keys, BY_FIRST)
            return d_keys, d_values

        zero = jnp.zeros((block, head), F32)
        state = inner(j, (zero, zero), True)
        state = lax.fori_loop(j + 1, count, lambda i, s: inner(i, s, False), state)
        dk_ref[there, :] = state[0]
        dv_ref[there, :] = state[1]

        @pl.when((j >= 1) & (j < last + 1))
        def _():
            walk.pass_on(j - 1)

        return carry

    lax.fori_loop(0, count, outer, 0)

    def unturn(b, carry):
        here = pl.ds(pl.multiple_of(b * block, block), block)
        for kind, source in ((0, dq_ref), (1, dk_ref)):
            grad = (source[here, :] * factor).astype(BF16).astype(F32)
            grad = grad * cosine[here, :] + half_turn(grad * sine[here, :], 1.0)
            source[here, :] = grad
            raw = mixed[here, kind * head : (kind + 1) * head]
            partial_sums[pl.ds(kind * count + b, 1), :] = across_lanes(
                raw * gains[kind + 1 : kind + 2, mine] * grad
            )
        return carry

    lax.fori_loop(0, count, unturn, 0)
    spread = Spread(ring, partial_sums, arrived, spread_sems)
    spread.begin()
    walk.pass_on(count - 1)
    loads[3].wait()
    spread.finish()
    total = spread.total()
    gain_head[...] = jnp.zeros_like(gain_head)

    def close(b, carry):
        here = pl.ds(pl.multiple_of(b * block, block), block)
        for kind, source in ((0, dq_ref), (1, dk_ref)):
            index = kind * count + b
            inverse = lax.rsqrt(to_column(squares[...], index, head) / width + EPS)
            inner = to_column(total, index, head) / width
            raw = mixed[here, kind * head : (kind + 1) * head]
            grad = source[here, :]
            value = inverse * gains[kind + 1 : kind + 2, mine] * grad
            value = value - raw * (inverse * inverse * inverse) * inner
            d_mixed[here, kind * head : (kind + 1) * head] = value.astype(BF16)
            gain_head[kind + 2 : kind + 3, :] += jnp.sum(raw * inverse * grad, 0, keepdims=True)
        d_mixed[here, 2 * head :] = dv_ref[here, :].astype(BF16)
        return carry

    lax.fori_loop(0, count, close, 0)
    walk.pass_on(count)
    chunks, beside, rows_each = qkv_part.shape[1], qkv_part.shape[0], qkv_part.shape[2]
    span = width // chunks

    def weigh(c, carry):
        these = pl.ds(pl.multiple_of(c * span, span), span)
        value = dot(hidden[:, these], d_mixed[...], BY_FIRST).astype(BF16)
        for x in range(beside):
            qkv_part[x, c] = value[x * rows_each : (x + 1) * rows_each]
        return carry

    lax.fori_loop(0, chunks, weigh, 0)
    for i in range(count + 1, last):
        walk.pass_on(i)
    router[...] = jnp.zeros_like(router)

    def route(c, carry):
        router[...] += dot(d_logits[c], own_hidden[c], MATMUL)
        return carry

    lax.fori_loop(0, n, route, 0)
    walk.finish()
    group = block // tok
    tile = min(512, width)

    def project(c, carry):
        left = attended[pl.ds(pl.multiple_of(c * block, block), block), :]
        for start in range(0, width, tile):
            cols = slice(start, start + tile)
            right = d_attn_all[pl.ds(c * group, group), :, cols].reshape(block, tile)
            value = dot(left, right, BY_FIRST)

            @pl.when(c == 0)
            def _():
                proj[:, cols] = value

            @pl.when(c > 0)
            def _():
                proj[:, cols] = proj[:, cols] + value

        return carry

    lax.fori_loop(0, count, project, 0)
    for at in range(tiles + EARLY):
        for j in range(f - 1):
            send_first(at // tiles, at % tiles, j).wait()


def attention_back(
    n, f, queries, keys, values, by_token, sums, exact, mixed, tables, starts, gains, squares,
    d_attn, attended, own_hidden, d_logits, rows_in, d_gate, d_up, hidden, rows, factor
):
    length, head = queries.shape
    tok, width = d_attn.shape
    block, count = blocks_of(length)
    experts = d_logits.shape[1]
    shape = jax.ShapeDtypeStruct
    kind = pltpu.SemaphoreType.DMA
    flat, every = d_gate.shape
    units = every // f
    tiles = n // 2
    grad = shape((max(f - 1, 1), width, units), BF16)
    return pl.pallas_call(
        partial(attention_back_kernel, n, f, factor),
        out_shape=[
            shape((length, 3 * head), BF16),
            shape((8, head), F32),
            shape((f, n, rows, 3 * head), BF16),
            shape((head, width), F32),
            shape((experts, head), F32),
            grad,
            grad,
        ],
        in_specs=[VMEM] * 15 + [ANY] * 4,
        out_specs=[VMEM] * 5 + [ANY] * 2,
        scratch_shapes=[pltpu.VMEM((length, head), F32)] * 3
        + [
            pltpu.VMEM((8, length), F32),
            pltpu.VMEM((2 * count, block), F32),
            pltpu.VMEM((n, 2 * count, block), F32),
            pltpu.VMEM((n, tok, width), BF16),
            pltpu.VMEM((tiles + EARLY, max(f - 1, 1), width // tiles, units), BF16),
            pltpu.VMEM((length, head), BF16),
            pltpu.VMEM((length, head), F32),
            pltpu.VMEM((length, head), F32),
            pltpu.VMEM(rows_in.shape, BF16),
            pltpu.VMEM((flat, every - units), BF16),
            pltpu.VMEM((flat, every - units), BF16),
            pltpu.VMEM(hidden.shape, BF16),
        ]
        + Gather.semaphores(n)
        + Spread.semaphores(n)
        + [kind((4,))]
        + [kind((tiles + EARLY, max(f - 1, 1))), kind((tiles + EARLY, max(f - 1, 1)))]
        + [kind((n,)), kind((n,)), kind((1,))],
        compiler_params=pltpu.CompilerParams(
            collective_id=6, has_side_effects=True, vmem_limit_bytes=67_000_000
        ),
        name="attention_back",
    )(
        queries, keys, values, by_token, sums, exact, mixed, tables, starts, gains, squares,
        d_attn, attended, own_hidden, d_logits, rows_in, d_gate, d_up, hidden
    )


def core_kernel(n, f, *refs):
    by_token, w_out, tokens, upstream, gain, router, routes, routes_all, upstream_all = refs[:9]
    shards_in = refs[9 : 8 + 4 * f]
    refs = refs[8 + 4 * f :]
    d_middle, middle, d_attn, d_by_token, d_logits_all, gain_two = refs[:6]
    own_hidden, rows_out, d_out, inner_out, d_gate_out, d_up_out, moe_out = refs[6:13]
    refs = refs[13:]
    w_near, w_gate, w_up, w_down, d_logits, arrived, outgoing, weights_in = refs[:8]
    refs = refs[8:]
    ring_in, mate_near, d_mate_in, coming, going, d_mate_out, own, lift = refs[:8]
    refs = refs[8:]
    rows_now, lifted, d_now, inner_now, d_gate_now, d_up_now, moe_now, d_weight, places = refs[:9]
    refs = refs[9:]
    hop_send, hop_recv, share_send, share_recv, swap_send, swap_recv = refs[:6]
    sum_send, sum_recv, send, recv, keep, load_sem, lift_sem, stage_sem, own_sem = refs[6:15]
    down_send, down_recv = refs[15:]
    ring = Ring(n, f)
    tok, width = tokens.shape
    head = width // n
    chips = ring.chips
    last = chips - 1
    capacity = rows_now.shape[1] // 2
    hidden_units = w_gate.shape[1]
    piece = tok // PIECES
    sign = 1 - 2 * ring.core
    onward = ring.at(ring.pos + sign + chips)
    local_units = hidden_units // f

    loads = [pltpu.make_async_copy(w_out, w_near, keep.at[0])]
    half_width = width * UPPER // 8
    soon = width * DOWN // 8
    sources = []
    for j in range(f):
        cols = slice(j * local_units, (j + 1) * local_units)
        sources.append((w_gate.at[:, cols], 0, j))
        sources.append((w_down.at[pl.ds(0, soon), cols] if j else w_down.at[:, cols], 2, j))
        if j:
            sources.append((w_up.at[pl.ds(0, half_width), cols], 1, j))
            sources.append((w_up.at[pl.ds(half_width, width - half_width), cols], 3, j))
        else:
            sources.append((w_up.at[:, cols], 1, j))
    for source, (target, kind, j) in zip(shards_in, sources):
        loads.append(pltpu.make_async_copy(source, target, load_sem.at[kind, j]))
    for load in loads:
        load.start()

    def chunk_of(i, other):
        return ring.at(
            ring.pos + (sign * (1 + i) if other else -sign * (1 + i)) + 2 * chips, other
        )

    def lift_copy(i, other):
        slot = lax.rem(i, 2)
        return pltpu.make_async_copy(
            upstream_all.at[chunk_of(i, other)],
            lift.at[slot, other],
            lift_sem.at[slot, other],
        )

    lift_copy(0, 0).start()
    lift_copy(0, 1).start()
    greet(ring, True, True)

    def down_rest(over):
        rows = pl.ds(soon, width - soon)
        return remote(
            shards_in[1].at[rows],
            w_down.at[rows, over * local_units : (over + 1) * local_units],
            down_send.at[over],
            down_recv.at[over],
            {"fsdp": ring.beside(over)},
        )

    for over in range(1, f):
        down_rest(over).start()

    mine = pl.ds(pl.multiple_of(ring.me * head, head), head)

    before = lax.broadcasted_iota(jnp.int32, (tok, tok), 0)
    after = lax.broadcasted_iota(jnp.int32, (tok, tok), 1)
    earlier = jnp.where(before < after, 1.0, 0.0).astype(BF16)

    def stand(c, carry):
        here = jnp.where(routes_all[c] == ring.me, 1.0, 0.0)
        here = jnp.sum(here, 0, keepdims=True)
        count = dot(jnp.broadcast_to(here, (8, tok)).astype(BF16), earlier, MATMUL)
        places[c] = jnp.where(jnp.broadcast_to(here, (8, tok)) > 0.5, count, -1.0)
        return carry

    lax.fori_loop(0, n, stand, 0)
    loads[0].wait()
    tile = min(512, width)
    squares = jnp.zeros((tok, 1), F32)
    for start in range(0, width, tile):
        cols = slice(start, start + tile)
        value = tokens[:, cols].astype(F32) + dot(by_token[...], w_near[:, cols], MATMUL)
        middle[:, cols] = value
        squares = squares + jnp.sum(value * value, -1, keepdims=True)
    inverse = lax.rsqrt(squares / width + EPS)
    ring_in[last] = (middle[...] * inverse * gain[...]).astype(BF16)

    def hop(i, s):
        rows = pl.ds(s * piece, piece)
        source = lax.rem(i + last, chips)
        return remote(
            ring_in.at[source, rows],
            ring_in.at[i, rows],
            hop_send.at[i, s],
            hop_recv.at[i, s],
            {"seq": onward},
        )

    def share(i, s):
        rows = pl.ds(s * piece, piece)
        return remote(
            ring_in.at[i, rows],
            mate_near.at[i, rows],
            share_send.at[i, s],
            share_recv.at[i, s],
            {"seq": ring.mate},
        )

    for s in range(PIECES):
        hop(0, s).start()
    for s in range(PIECES):
        share(last, s).start()

    logits = dot(router[...], ring_in[last], BY_LAST)
    expd = jnp.exp(logits - jnp.max(logits, 0, keepdims=True))
    gate = expd / jnp.sum(expd, 0, keepdims=True)
    experts = lax.broadcasted_iota(jnp.int32, gate.shape, 0)
    named = jnp.zeros(gate.shape, F32)
    for k in range(routes.shape[0]):
        named = named + jnp.where(routes[k : k + 1, :] == experts, 1.0, 0.0)
    weights = gate * named
    for e in range(n):
        outgoing[e] = jnp.broadcast_to(weights[e : e + 1, :], (8, tok))

    def push(there):
        return remote(
            outgoing.at[there],
            weights_in.at[ring.me],
            send.at[1, there],
            recv.at[1, ring.me],
            {"seq": there},
        )

    def pushed(origin):
        return remote(
            outgoing.at[origin],
            weights_in.at[origin],
            send.at[1, origin],
            recv.at[1, origin],
            {"seq": origin},
        )

    def each_9(step, carry):
        push(ring.peer(step)).start()
        return carry

    lax.fori_loop(1, n, each_9, 0)
    weights_in[ring.me] = outgoing[ring.me]
    for load in loads[1:]:
        load.wait()
    for over in range(1, f):
        down_rest(over).wait_recv()

    def swap(i):
        return remote(
            d_mate_out.at[lax.rem(i, 2)],
            d_mate_in.at[i],
            swap_send.at[i],
            swap_recv.at[i],
            {"seq": ring.mate},
        )

    def sum_hop(i, s):
        rows = pl.ds(s * piece, piece)
        return remote(
            going.at[lax.rem(i, 2), rows],
            coming.at[i, rows],
            sum_send.at[i, s],
            sum_recv.at[i, s],
            {"seq": onward},
        )

    def sum_step(i):
        swap(i).wait_recv()

        @pl.when(i >= 2)
        def _():
            for s in range(PIECES):
                sum_hop(i - 2, s).wait_send()

        for s in range(PIECES):
            rows = pl.ds(s * piece, piece)

            @pl.when(i > 0)
            def _():
                sum_hop(i - 1, s).wait_recv()
                own[rows, :] = own[rows, :] + coming[i - 1, rows].astype(F32)

            value = own[rows, :] + d_mate_in[i, rows].astype(F32)
            going[lax.rem(i, 2), rows] = value.astype(BF16)
            sum_hop(i, s).start()

    def give(kind, target, other, slot):
        chunk = target
        source, sink = [
            (rows_now, rows_out),
            (d_now, d_out),
            (inner_now, inner_out),
            (d_gate_now, d_gate_out),
            (d_up_now, d_up_out),
            (moe_now, moe_out),
        ][kind]
        size = tok if kind == 5 else capacity
        return pltpu.make_async_copy(
            source.at[slot, pl.ds(other * size, size)],
            sink.at[chunk],
            stage_sem.at[slot, kind, other],
        )

    def keep_hidden(i, other):
        return pltpu.make_async_copy(
            (mate_near if other else ring_in).at[i, :, mine],
            own_hidden.at[chunk_of(i, other)],
            own_sem.at[other, i],
        )

    def report(there, slot, other):
        return remote(
            d_weight.at[slot, other],
            arrived.at[ring.me],
            send.at[2, there],
            recv.at[2, ring.me],
            {"seq": there},
        )

    def reported(origin):
        return remote(
            d_weight.at[0, 0],
            arrived.at[origin],
            send.at[2, origin],
            recv.at[2, origin],
            {"seq": origin},
        )

    def pass_on(i):
        for s in range(PIECES):
            hop(i, s).wait_recv()

            @pl.when(i < last - 1)
            def _():
                hop(i + 1, s).start()

            share(i, s).start()

    def work(i):
        slot = lax.rem(i, 2)
        chunks = (chunk_of(i, 0), chunk_of(i, 1))
        for s in range(PIECES):
            share(i, s).wait_recv()
        keep_hidden(i, 0).start()
        keep_hidden(i, 1).start()
        for other in (0, 1):
            lift_copy(i, other).wait()

        @pl.when(i < last)
        def _():
            lift_copy(i + 1, 0).start()
            lift_copy(i + 1, 1).start()
            pushed(chunks[0]).wait_recv()

        pushed(chunks[1]).wait_recv()

        @pl.when(i >= 2)
        def _():
            for kind in range(6):
                for other in (0, 1):
                    give(kind, chunks[other], other, slot).wait()
            swap(i - 2).wait_send()
            for other in (0, 1):
                report(chunk_of(i - 2, other), slot, other).wait_send()

        slots = lax.broadcasted_iota(jnp.int32, (capacity, tok), 0).astype(F32)
        picks, rates = [], []
        for other in (0, 1):
            rows = slice(other * capacity, (other + 1) * capacity)
            where = slots == jnp.broadcast_to(places[chunks[other], 0:1, :], (capacity, tok))
            pick = jnp.where(where, 1.0, 0.0)
            low = pick.astype(BF16)
            source = mate_near.at[i] if other else ring_in.at[i]
            share_of = weights_in[chunks[other], 0:1, :]
            rate = jnp.sum(jnp.where(where, share_of, 0.0), -1, keepdims=True)
            for start in range(0, width, tile):
                cols = slice(start, start + tile)
                rows_now[slot, rows, cols] = dot(low, source[:, cols], MATMUL).astype(BF16)
                picked = dot(low, lift[slot, other, :, cols], MATMUL)
                lifted[rows, cols] = picked.astype(BF16)
                d_now[slot, rows, cols] = (rate * picked).astype(BF16)
            picks.append((low, where))
            rates.append(rate)
        rate = jnp.concatenate(rates, 0)
        unit = min(256, hidden_units)
        for start in range(0, hidden_units, unit):
            cols = slice(start, start + unit)
            gate_act = dot(rows_now[slot], w_gate[:, cols], MATMUL)
            up_act = dot(rows_now[slot], w_up[:, cols], MATMUL)
            d_inner = dot(d_now[slot], w_down[:, cols], MATMUL)
            sigma = 1.0 / (1.0 + jnp.exp(-gate_act))
            silu = gate_act * sigma
            inner_now[slot, :, cols] = (silu * up_act).astype(BF16)
            d_gate_now[slot, :, cols] = (
                d_inner * up_act * sigma * (1.0 + gate_act * (1.0 - sigma))
            ).astype(BF16)
            d_up_now[slot, :, cols] = (d_inner * silu).astype(BF16)
        inner_product = jnp.zeros((2 * capacity, 1), F32)
        for start in range(0, width, tile):
            cols = slice(start, start + tile)
            produced = dot(inner_now[slot], w_down[cols, :], BY_LAST)
            produced = produced.astype(BF16).astype(F32)
            inner_product = inner_product + jnp.sum(
                produced * lifted[:, cols].astype(F32), -1, keepdims=True
            )
            scaled = (rate * produced).astype(BF16)
            d_rows = dot(d_gate_now[slot], w_gate[cols, :], BY_LAST)
            d_rows = (d_rows + dot(d_up_now[slot], w_up[cols, :], BY_LAST)).astype(BF16)
            for other in (0, 1):
                rows = slice(other * capacity, (other + 1) * capacity)
                low = picks[other][0]
                moe_now[slot, other * tok : (other + 1) * tok, cols] = dot(
                    low, scaled[rows], BY_FIRST
                ).astype(BF16)
                spread_rows = dot(low, d_rows[rows], BY_FIRST)
                if other:
                    d_mate_out[slot, :, cols] = spread_rows.astype(BF16)
                else:
                    own[:, cols] = spread_rows
        swap(i).start()
        for kind in range(6):
            for other in (0, 1):
                give(kind, chunks[other], other, slot).start()
        for other in (0, 1):
            rows = slice(other * capacity, (other + 1) * capacity)
            value = jnp.sum(
                jnp.where(picks[other][1], inner_product[rows], 0.0), 0, keepdims=True
            )
            d_weight[slot, other] = jnp.broadcast_to(value, (8, tok))
        report(chunks[1], slot, 1).start()

        @pl.when(i < last)
        def _():
            report(chunks[0], slot, 0).start()

    def body(i, carry):
        @pl.when(i < last)
        def _():
            pass_on(i)

        @pl.when(i > 0)
        def _():
            sum_step(i - 1)

        work(i)
        return carry

    lax.fori_loop(0, chips, body, 0)
    arrived[ring.me] = d_weight[last % 2, 0]

    def each_10(step, carry):
        reported(ring.peer(step)).wait_recv()
        return carry

    lax.fori_loop(1, n, each_10, 0)
    gate_back = jnp.concatenate([arrived[e, 0:1, :] for e in range(n)], 0)
    gate_back = gate * (gate_back - jnp.sum(gate * gate_back, 0, keepdims=True))
    d_logits[...] = gate_back.astype(BF16)

    def publish(step):
        return remote(
            d_logits,
            d_logits_all.at[ring.me],
            send.at[4, step],
            recv.at[4, step],
            {"seq": ring.peer(step)},
        )

    kept = pltpu.make_async_copy(d_logits, d_logits_all.at[ring.me], keep.at[1])
    swap(last).wait_recv()
    for s in range(PIECES):
        rows = pl.ds(s * piece, piece)
        sum_hop(last - 1, s).wait_recv()
        value = own[rows, :] + d_mate_in[last, rows].astype(F32)
        own[rows, :] = value + coming[last - 1, rows].astype(F32)
    d_hidden = own[...] + dot(gate_back.astype(BF16), router[...], BY_FIRST)
    value = middle[...]
    inner = jnp.mean(value * gain[...] * d_hidden, -1, keepdims=True)
    gain_two[...] = jnp.sum(value * inverse * d_hidden, 0, keepdims=True)
    d_value = inverse * gain[...] * d_hidden - value * (inverse * inverse * inverse) * inner
    d_value = upstream[...].astype(F32) + d_value
    d_middle[...] = d_value
    d_attn[...] = d_value.astype(BF16)
    for start in range(0, width, tile):
        cols = slice(start, start + tile)
        d_by_token[:, cols] = dot(d_attn[...], w_near[cols, :], BY_LAST).astype(BF16)

    def each_11(step, carry):
        publish(step).start()
        return carry

    lax.fori_loop(1, n, each_11, 0)
    kept.start()

    for over in range(1, f):
        down_rest(over).wait_send()
    for s in range(PIECES):
        share(last, s).wait_send()

    def settle(i, carry):
        for s in range(PIECES):
            hop(i, s).wait_send()
            share(i, s).wait_send()
        for other in (0, 1):
            keep_hidden(i, other).wait()
        return carry

    lax.fori_loop(0, last, settle, 0)
    for other in (0, 1):
        keep_hidden(last, other).wait()
    for s in range(PIECES):
        sum_hop(last - 2, s).wait_send()
        sum_hop(last - 1, s).wait_send()
    for i in (last - 1, last):
        swap(i).wait_send()
        for other in (0, 1):
            for kind in range(6):
                give(kind, chunk_of(i, other), other, i % 2).wait()
            if other or i < last:
                report(chunk_of(i, other), i % 2, other).wait_send()

    def each_12(step, carry):
        push(ring.peer(step)).wait_send()
        return carry

    lax.fori_loop(1, n, each_12, 0)

    def each_13(step, carry):
        publish(step).wait()
        return carry

    lax.fori_loop(1, n, each_13, 0)
    kept.wait()


def core_stage(
    n, f, by_token, w_out, tokens, upstream, gain, router, routes, routes_all, upstream_all, halves
):
    tok, width = tokens.shape
    experts = router.shape[0]
    units = f * halves[0].shape[1]
    capacity = min(tok, 5 * tok * TOPK // (4 * experts))
    chips = n // 2
    kind = pltpu.SemaphoreType.DMA
    shape = jax.ShapeDtypeStruct
    rows = 2 * capacity
    return pl.pallas_call(
        partial(core_kernel, n, f),
        out_shape=[
            shape((tok, width), F32),
            shape((tok, width), F32),
            shape((tok, width), BF16),
            shape((tok, width), BF16),
            shape((n, experts, tok), BF16),
            shape((1, width), F32),
            shape((n, tok, width // n), BF16),
            shape((n, capacity, width), BF16),
            shape((n, capacity, width), BF16),
            shape((n, capacity, units), BF16),
            shape((n, capacity, units), BF16),
            shape((n, capacity, units), BF16),
            shape((n, tok, width), BF16),
        ],
        in_specs=[VMEM, ANY] + [VMEM] * 6 + [ANY] * (4 * f),
        out_specs=[VMEM] * 4 + [ANY, VMEM] + [ANY] * 7,
        scratch_shapes=[
            pltpu.VMEM((width, width), BF16),
            pltpu.VMEM((width, units), BF16),
            pltpu.VMEM((width, units), BF16),
            pltpu.VMEM((width, units), BF16),
            pltpu.VMEM((experts, tok), BF16),
            pltpu.VMEM((n, 8, tok), F32),
            pltpu.VMEM((n, 8, tok), F32),
            pltpu.VMEM((n, 8, tok), F32),
            pltpu.VMEM((chips, tok, width), BF16),
            pltpu.VMEM((chips, tok, width), BF16),
            pltpu.VMEM((chips, tok, width), BF16),
            pltpu.VMEM((chips - 1, tok, width), BF16),
            pltpu.VMEM((2, tok, width), BF16),
            pltpu.VMEM((2, tok, width), BF16),
            pltpu.VMEM((tok, width), F32),
            pltpu.VMEM((2, 2, tok, width), BF16),
            pltpu.VMEM((2, rows, width), BF16),
            pltpu.VMEM((rows, width), BF16),
            pltpu.VMEM((2, rows, width), BF16),
            pltpu.VMEM((2, rows, units), BF16),
            pltpu.VMEM((2, rows, units), BF16),
            pltpu.VMEM((2, rows, units), BF16),
            pltpu.VMEM((2, 2 * tok, width), BF16),
            pltpu.VMEM((2, 2, 8, tok), F32),
            pltpu.VMEM((n, 8, tok), F32),
            kind((chips, PIECES)),
            kind((chips, PIECES)),
            kind((chips, PIECES)),
            kind((chips, PIECES)),
            kind((chips,)),
            kind((chips,)),
            kind((chips, PIECES)),
            kind((chips, PIECES)),
            kind((5, n)),
            kind((5, n)),
            kind((2,)),
            kind((4, f)),
            kind((2, 2)),
            kind((2, 6, 2)),
            kind((2, chips)),
            kind((f,)),
            kind((f,)),
        ],
        compiler_params=pltpu.CompilerParams(
            collective_id=1, has_side_effects=True, vmem_limit_bytes=67_000_000
        ),
        name="core_stage",
    )(by_token, w_out, tokens, upstream, gain, router, routes, routes_all, upstream_all, *halves)


def last_kernel(n, f, *refs):
    d_mixed, w_head, qkv_part, tokens, gain, d_middle, gain_two, gain_head = refs[:8]
    middle, proj, router, moe_part = refs[8:12]
    far_refs = refs[12:17]
    d_inputs, qkv_out, gains_out, second_in, third_in, grads_out, result = refs[17:24]
    proj_out, router_out = refs[24:26]
    beside_rows, summed, qkv_rows, gain_rows, gain_in, gain_side, stage, far_stage = refs[26:34]
    proj_low, proj_in, router_low = refs[34:37]
    near_refs = refs[37:42]
    rows_in, d_in, d_gate, d_up, inner_in = near_refs
    buffers, fold_sems = refs[42:47], refs[47:51]
    stored_buffers, stored_sems = refs[51:55], refs[55:60]
    side_send, side_recv, send, recv, keep, stage_sem, load_sem, far_send, far_recv = refs[60:]
    ring = Ring(n, f)
    _, width = tokens.shape
    slice_width = width // n
    units = grads_out.shape[2]
    chips = ring.chips
    size = width // chips
    loads = [
        pltpu.make_async_copy(source.at[:, :units] if k == 2 else source, target, load_sem.at[k])
        for k, (source, target) in enumerate(zip(far_refs, near_refs))
    ]
    greet(ring, True, True)

    def side(step):
        there = ring.beside(step)
        return remote(
            qkv_part.at[there],
            beside_rows.at[step - 1],
            side_send.at[0, step],
            side_recv.at[0, step],
            {"fsdp": there},
        )

    for step in range(1, f):
        side(step).start()

    def proj_side(step):
        there = ring.beside(step)
        return remote(
            proj_low.at[there],
            proj_in.at[step - 1],
            side_send.at[3, step],
            side_recv.at[3, step],
            {"fsdp": there},
        )

    def router_side(step):
        return remote(
            router_low.at[0],
            router_low.at[step],
            side_send.at[4, step],
            side_recv.at[4, step],
            {"fsdp": ring.beside(step)},
        )

    for x in range(f):
        proj_low[x] = proj[x].astype(BF16)
    router_low[0] = router[...].astype(BF16)
    for step in range(1, f):
        proj_side(step).start()
        router_side(step).start()

    def part(chunk, target):
        tile = min(512, width)
        for start in range(0, width, tile):
            cols = slice(start, start + tile)
            target[:, cols] = dot(d_mixed[chunk], w_head[cols, :], BY_LAST).astype(target.dtype)

    fold = Fold(ring, part, buffers, fold_sems)

    def finish(rows, value):
        d_inputs[rows, :] = value

    def store(i, which):
        these = pl.ds(pl.multiple_of(i * size, size), size)
        slot = lax.rem(i, 2)
        return pltpu.make_async_copy(
            stage.at[slot, which], grads_out.at[which, these], stage_sem.at[slot, which]
        )

    def filler(i):
        these = pl.ds(pl.multiple_of(i * size, size), size)
        slot = lax.rem(i, 2)
        pairs = ((rows_in, d_gate), (rows_in, d_up), (d_in, inner_in))
        for which, (left, right) in enumerate(pairs):

            @pl.when(i >= 2)
            def _():
                store(i - 2, which).wait()

            stage[slot, which] = dot(left[:, these], right[:, :units], BY_FIRST).astype(BF16)
            store(i, which).start()
        afar(i)

    def far(kind, i, j):
        these = pl.ds(pl.multiple_of(i * size, size), size)
        return remote(
            far_stage.at[lax.rem(i, 2), kind, j],
            [second_in, third_in][kind].at[j, these],
            far_send.at[kind, i, j],
            far_recv.at[kind, i, j],
            {"fsdp": ring.beside(f - 1 - j)},
        )

    def afar(i):
        these = pl.ds(pl.multiple_of(i * size, size), size)
        slot = lax.rem(i, 2)

        def make(kind, first_tile, left, right):
            @pl.when(i >= first_tile + 2)
            def _():
                for j in range(f - 1):
                    far(kind, i - 2, j).wait_send()

            @pl.when(i >= first_tile)
            def _():
                for j in range(f - 1):
                    part = slice((j + 1) * units, (j + 2) * units)
                    value = dot(left[:, these], right[:, part], BY_FIRST)
                    far_stage[slot, kind, j] = value.astype(BF16)
                    far(kind, i, j).start()

        make(0, EARLY, rows_in, d_up)
        make(1, 0, d_in, inner_in)

    def push(step):
        there = ring.peer(step)
        return remote(
            summed.at[there],
            qkv_rows.at[ring.me],
            send.at[0, step],
            recv.at[0, step],
            {"seq": there},
        )

    local = pltpu.make_async_copy(summed.at[ring.me], qkv_rows.at[ring.me], keep.at[0])

    stored = Stored(ring, moe_part, stored_buffers, stored_sems)

    def before(i):
        @pl.when(i == 0)
        def _():
            stored.begin()
            for load in loads:
                load.start()

    def spread_qkv():
        for step in range(1, f):
            side(step).wait_recv()

        def add(block, carry):
            value = qkv_part[ring.mine, block].astype(F32)
            for step in range(1, f):
                value = value + beside_rows[step - 1, block].astype(F32)
            summed[block] = value.astype(BF16)
            return carry

        lax.fori_loop(0, n, add, 0)

        def each_14(step, carry):
            push(step).start()
            return carry

        lax.fori_loop(1, n, each_14, 0)
        local.start()

    def after(i):
        stored.step(i)

        @pl.when(i == 0)
        def _():
            for load in loads:
                load.wait()

    fold.run(finish, filler, before, after)

    def settle(rows, value):
        result[rows, :] = (middle[rows, :] + value).astype(BF16)

    stored.close(settle)
    value = tokens[...].astype(F32)
    grad = d_inputs[...]
    inverse = lax.rsqrt(jnp.mean(value * value, -1, keepdims=True) + EPS)
    inner = jnp.mean(value * gain[...] * grad, -1, keepdims=True)
    gain_rows[...] = jnp.zeros_like(gain_rows)
    gain_rows[0:1, :] = jnp.sum(value * inverse * grad, 0, keepdims=True)
    gain_rows[1:2, :] = gain_two[...]

    def gains(step):
        there = ring.peer(step)
        cols = pl.ds(pl.multiple_of(there * slice_width, slice_width), slice_width)
        return remote(
            gain_rows.at[:, cols],
            gain_in.at[ring.me],
            send.at[1, step],
            recv.at[1, step],
            {"seq": there},
        )

    mine = pl.ds(pl.multiple_of(ring.me * slice_width, slice_width), slice_width)
    kept = pltpu.make_async_copy(gain_rows.at[:, mine], gain_in.at[ring.me], keep.at[1])

    def each_15(step, carry):
        gains(step).start()
        return carry

    lax.fori_loop(1, n, each_15, 0)
    kept.start()
    spread_qkv()
    d_value = inverse * gain[...] * grad - value * (inverse * inverse * inverse) * inner
    d_inputs[...] = d_middle[...] + d_value

    def each_16(step, carry):
        gains(step).wait()
        return carry

    lax.fori_loop(1, n, each_16, 0)
    kept.wait()
    total = gain_head[...]
    for device in range(n):
        total = total + gain_in[device]
    gain_side[0] = total

    def sums(step):
        return remote(
            gain_side.at[0],
            gain_side.at[step],
            side_send.at[1, step],
            side_recv.at[1, step],
            {"fsdp": ring.beside(step)},
        )

    for step in range(1, f):
        sums(step).start()
    proj_total = proj[ring.mine]
    router_total = router[...]
    for step in range(1, f):
        proj_side(step).wait()
        router_side(step).wait()
        proj_total = proj_total + proj_in[step - 1].astype(F32)
        router_total = router_total + router_low[step].astype(F32)
    proj_out[...] = proj_total
    router_out[...] = router_total
    fold.close()
    for i in (chips - 2, chips - 1):
        for which in range(3):
            store(i, which).wait()
    for step in range(1, f):
        side(step).wait_send()

    def each_17(step, carry):
        push(step).wait()
        return carry

    lax.fori_loop(1, n, each_17, 0)
    local.wait()
    piece = qkv_rows.shape[2] // 3
    for h in range(n):
        for k in range(3):
            start = k * width + h * piece
            qkv_out[:, start : start + piece] = qkv_rows[
                h, :, k * piece : (k + 1) * piece
            ].astype(F32)
    for step in range(1, f):
        sums(step).wait()
        total = total + gain_side[step]
    gains_out[...] = total
    for j in range(f - 1):
        for kind, first_tile in ((0, EARLY), (1, 0)):
            for i in range(first_tile, chips):
                far(kind, i, j).wait_recv()
                if i >= chips - 2:
                    far(kind, i, j).wait_send()


def last_stage(
    n, f, d_mixed, w_head, qkv_part, tokens, gain, d_middle, gain_two, gain_head,
    middle, proj, router, moe_part, rows_in, d_in, d_gate, d_up, inner_in, second
):
    tok, width = tokens.shape
    rows, across = qkv_part.shape[2:]
    units = second.shape[2]
    kind = pltpu.SemaphoreType.DMA
    shape = jax.ShapeDtypeStruct
    return pl.pallas_call(
        partial(last_kernel, n, f),
        out_shape=[
            shape((tok, width), F32),
            shape((rows, n * across), F32),
            shape((8, width // n), F32),
            shape(second.shape, BF16),
            shape(second.shape, BF16),
            shape((3, width, units), BF16),
            shape((tok, width), BF16),
            shape((rows, width), F32),
            shape(router.shape, F32),
        ],
        in_specs=[VMEM] * 11 + [ANY] * 6,
        out_specs=[VMEM] * 3 + [ANY] * 3 + [VMEM] * 3,
        scratch_shapes=[
            pltpu.VMEM((max(f - 1, 1), n, rows, across), BF16),
            pltpu.VMEM((n, rows, across), BF16),
            pltpu.VMEM((n, rows, across), BF16),
            pltpu.VMEM((8, width), F32),
            pltpu.VMEM((n, 8, width // n), F32),
            pltpu.VMEM((f, 8, width // n), F32),
            pltpu.VMEM((2, 3, 2 * width // n, units), BF16),
            pltpu.VMEM((2, 2, max(f - 1, 1), 2 * width // n, units), BF16),
            pltpu.VMEM(proj.shape, BF16),
            pltpu.VMEM((max(f - 1, 1),) + proj.shape[1:], BF16),
            pltpu.VMEM((f,) + router.shape, BF16),
            pltpu.VMEM(rows_in.shape, BF16),
            pltpu.VMEM(rows_in.shape, BF16),
            pltpu.VMEM((rows_in.shape[0], units), BF16),
            pltpu.VMEM(d_up.shape, BF16),
            pltpu.VMEM(inner_in.shape, BF16),
        ]
        + Fold.buffers(n, tok, width)
        + Fold.semaphores(n)
        + Stored.buffers(n, tok, width)
        + Stored.semaphores(n)
        + [kind((5, f)), kind((5, f)), kind((2, n)), kind((2, n)), kind((2,)), kind((2, 3))]
        + [kind((5,))]
        + [kind((2, n // 2, max(f - 1, 1))), kind((2, n // 2, max(f - 1, 1)))],
        compiler_params=pltpu.CompilerParams(
            collective_id=4, has_side_effects=True, vmem_limit_bytes=67_000_000
        ),
        name="last_stage",
    )(
        d_mixed, w_head, qkv_part, tokens, gain, d_middle, gain_two, gain_head,
        middle, proj, router, moe_part, rows_in, d_in, d_gate, d_up, inner_in
    )


def angles_of(n, tok, head_size):
    half = head_size // 2
    freqs = 10000.0 ** (-jnp.arange(half, dtype=F32) / half)
    inside = jnp.arange(tok, dtype=jnp.int32)
    starts = jnp.arange(n, dtype=jnp.int32) * tok
    angles = jnp.concatenate([inside, starts]).astype(F32)[:, None] * freqs[None, :]
    both = jnp.stack([jnp.cos(angles), jnp.sin(angles)])
    both = jnp.concatenate([both, both], -1)
    return both[:, :tok], both[:, tok:, None, :]


def shards(n, f, inputs, routes, w_qkv, w_out, w_router, norm_gains, w_gate, w_up, w_down, cotangent):
    tokens_low = inputs[0]
    upstream_low = cotangent[0]
    local_routes = routes[0].T
    mine = lax.axis_index("fsdp")
    tok, width = tokens_low.shape
    length = tok * n
    head_size = width // HEADS
    across = 3 * head_size
    rows = w_qkv.shape[0]
    experts = n * w_gate.shape[0]
    capacity = min(tok, 5 * tok * TOPK // (4 * experts))
    factor = head_size ** (-0.5)

    small = jnp.concatenate([w_router, norm_gains], 1)
    small = jnp.pad(small, ((0, 0), (0, 128 - small.shape[1])))
    (
        hidden_one,
        mixed,
        w_head,
        router,
        gains,
        routes_all,
        gate_near,
        up_near,
        w_out_all,
    ) = first_gather(n, f, tokens_low, w_qkv, small, local_routes, w_out, w_gate[0], w_up[0])
    w_out_all = w_out_all.reshape(width, width)
    hidden_one = hidden_one.reshape(length, width)
    w_head = w_head.reshape(width, across)
    tables, starts = angles_of(n, tok, head_size)
    (
        queries,
        keys,
        values,
        attended,
        exact,
        sums,
        squares,
        upstream_all,
        by_token,
        up_rest,
        down_near,
    ) = attention(n, f, mixed, tables, starts, gains, upstream_low, w_up[0], w_down[0], factor)
    halves = [w_gate[0], w_down[0], w_up[0]]
    for j in range(f - 1):
        halves += [gate_near[j], down_near[j], up_near[j], up_rest[j]]

    (
        d_middle,
        middle,
        d_attn,
        d_attended,
        d_logits_all,
        gain_two,
        own_hidden,
        expert_rows,
        d_produced,
        inner,
        d_gate,
        d_up,
        moe_part,
    ) = core_stage(
        n,
        f,
        by_token,
        w_out_all,
        tokens_low,
        upstream_low,
        gains[3:4],
        router,
        local_routes,
        routes_all,
        upstream_all,
        halves,
    )
    flat = n * capacity
    units = w_gate.shape[2]
    expert_rows = expert_rows.reshape(flat, width)
    d_produced = d_produced.reshape(flat, width)
    inner, d_gate, d_up = (v.reshape(flat, f * units) for v in (inner, d_gate, d_up))
    d_mixed, gain_head, qkv_part, proj, router_part, first, second = attention_back(
        n,
        f,
        queries,
        keys,
        values,
        d_attended,
        sums,
        exact,
        mixed,
        tables,
        starts,
        gains,
        squares,
        d_attn,
        attended,
        own_hidden,
        d_logits_all,
        expert_rows,
        d_gate,
        d_up,
        hidden_one,
        rows,
        factor,
    )
    (
        grad_inputs,
        grad_qkv,
        gains_own,
        second_rest,
        third,
        grads_own,
        result,
        grad_proj,
        grad_router,
    ) = last_stage(
        n,
        f,
        d_mixed.reshape(n, tok, across),
        w_head,
        qkv_part,
        tokens_low,
        gains[0:1],
        d_middle,
        gain_two,
        gain_head,
        middle,
        proj.reshape(f, rows, width),
        router_part,
        moe_part,
        expert_rows,
        d_produced,
        d_gate,
        d_up,
        inner,
        second,
    )
    grad_router = lax.dynamic_slice_in_dim(grad_router, mine * rows, rows, 1).T
    split = EARLY * (width // (n // 2))
    grads = []
    for which in range(3):
        total = grads_own[which].astype(F32)
        for j in range(f - 1):
            if which == 1:
                late = jnp.arange(width)[:, None] >= split
                part = jnp.where(late, second_rest[j], second[j])
            else:
                part = (first if which == 0 else third)[j]
            total = total + part.astype(F32)
        grads.append(total[None])
    gains_out = jnp.stack([gains_own[0], gains_own[2], gains_own[3], gains_own[1]], 1)
    grad_gains = lax.dynamic_slice_in_dim(gains_out, mine * rows, rows, 0)
    return (
        result[None],
        grad_inputs[None],
        grad_qkv,
        grad_proj,
        grad_router,
        grad_gains,
        *grads,
    )


def solution(mesh):
    tokens = P("fsdp", "seq", None)
    split = P(("seq", "fsdp"), None)
    expert = P("seq", None, "fsdp")
    return jax.shard_map(
        partial(shards, mesh.shape["seq"], mesh.shape["fsdp"]),
        mesh=mesh,
        in_specs=(tokens, tokens, split, split, split, split, expert, expert, expert, tokens),
        out_specs=(tokens, tokens, split, split, split, split, expert, expert, expert),
        check_vma=False,
    )
```

```python
from functools import partial

import jax
import jax.numpy as jnp
from jax import lax
from jax.experimental import pallas as pl
from jax.experimental.pallas import tpu as pltpu
from jax.sharding import PartitionSpec as P

HEADS = 16
TOPK = 8
EPS = 1e-05
NEG = -1e30
F32 = jnp.float32
BF16 = jnp.bfloat16
MESH = pl.DeviceIdType.MESH
PIECES = 2
EARLY = 3
UPPER = 4
DOWN = 7
ANY = pl.BlockSpec(memory_space=pl.ANY)
VMEM = pl.BlockSpec(memory_space=pltpu.VMEM)
MATMUL = (((1,), (0,)), ((), ()))
BY_LAST = (((1,), (1,)), ((), ()))
BY_FIRST = (((0,), (0,)), ((), ()))


def dot(a, b, dims):
    return lax.dot_general(a, b, dims, preferred_element_type=F32)


class Ring:
    def __init__(self, n, f):
        self.n, self.f = n, f
        self.chips = n // 2
        self.half = self.chips // 2
        self.pairs_minor = f == 2
        self.me = lax.axis_index("seq")
        self.mine = lax.axis_index("fsdp")
        chip = self.me // 2
        self.core = self.me % 2
        if self.pairs_minor:
            along, side = chip // 2, chip % 2
        else:
            along, side = chip % self.half, chip // self.half
        self.pos = along + side * (self.chips - 1 - 2 * along)
        self.right = self.at(self.pos + 1)
        self.left = self.at(self.pos + self.chips - 1)
        self.mate = self.me + 1 - 2 * self.core
        self.sign = 1 - 2 * self.core
        self.onward = self.at(self.pos + self.sign + self.chips)

    def at(self, place, other=False):
        place = lax.rem(place + self.chips, self.chips)
        side = place // self.half
        along = place + side * (self.chips - 1 - 2 * place)
        chip = along * 2 + side if self.pairs_minor else side * self.half + along
        core = 1 - self.core if other else self.core
        return chip * 2 + core

    def peer(self, step):
        return lax.rem(self.me + step, self.n)

    def beside(self, step):
        return lax.rem(self.mine + step, self.f)


def greet(ring, everyone, beside):
    barrier = pltpu.get_barrier_semaphore()
    count = 0
    if everyone:

        def each_0(step, carry):
            pl.semaphore_signal(
                barrier, inc=1, device_id={"seq": ring.peer(step)}, device_id_type=MESH
            )
            return carry

        lax.fori_loop(1, ring.n, each_0, 0)
        count += ring.n - 1
    else:
        for other in (ring.right, ring.left, ring.mate):
            pl.semaphore_signal(barrier, inc=1, device_id={"seq": other}, device_id_type=MESH)
        count += 3
    if beside:
        for step in range(1, ring.f):
            pl.semaphore_signal(
                barrier, inc=1, device_id={"fsdp": ring.beside(step)}, device_id_type=MESH
            )
        count += ring.f - 1
    pl.semaphore_wait(barrier, count)


def remote(src, dst, send, recv, where):
    return pltpu.make_async_remote_copy(
        src_ref=src,
        dst_ref=dst,
        send_sem=send,
        recv_sem=recv,
        device_id=where,
        device_id_type=MESH,
    )


class Gather:
    def __init__(self, ring, own, out, sems):
        self.ring, self.own, self.out = ring, own, out
        self.send, self.recv, self.mate_send, self.mate_recv, self.keep = sems
        self.piece = own.shape[0] // (2 * PIECES)
        self.last = ring.chips - 1

    @staticmethod
    def semaphores(n):
        hops = n // 2 - 1
        kind = pltpu.SemaphoreType.DMA
        return [
            kind((2, hops, PIECES)),
            kind((2, hops, PIECES)),
            kind((2, hops + 1, PIECES)),
            kind((2, hops + 1, PIECES)),
            kind((1,)),
        ]

    def rows(self, way, s):
        return pl.ds((way * PIECES + s) * self.piece, self.piece)

    def hop(self, way, step, s, first):
        ring = self.ring
        chunk = ring.at(ring.pos - step if way == 0 else ring.pos + step)
        rows = self.rows(way, s)
        there = self.out.at[chunk, rows]
        return remote(
            self.own.at[rows] if first else there,
            there,
            self.send.at[way, step, s],
            self.recv.at[way, step, s],
            {"seq": ring.right if way == 0 else ring.left},
        )

    def share(self, way, step, s, first):
        ring = self.ring
        chunk = ring.at(ring.pos - step if way == 0 else ring.pos + step)
        rows = self.rows(way, s)
        there = self.out.at[chunk, rows]
        return remote(
            self.own.at[rows] if first else there,
            there,
            self.mate_send.at[way, step, s],
            self.mate_recv.at[way, step, s],
            {"seq": ring.mate},
        )

    def local(self):
        return pltpu.make_async_copy(self.own, self.out.at[self.ring.me], self.keep.at[0])

    def begin(self):
        for s in range(PIECES):
            for way in (0, 1):
                self.hop(way, 0, s, True).start()
        for s in range(PIECES):
            for way in (0, 1):
                self.share(way, 0, s, True).start()
        self.local().start()

    def pass_on(self, i):
        for s in range(PIECES):
            for way in (0, 1):
                self.hop(way, i, s, False).wait_recv()

                @pl.when(i + 1 < self.ring.chips - 1)
                def _():
                    self.hop(way, i + 1, s, False).start()

                self.share(way, i + 1, s, False).start()

    def run(self):
        def body(step, carry):
            self.pass_on(step)
            return carry

        lax.fori_loop(0, self.ring.chips - 1, body, 0)

    def finish(self):
        hops = self.ring.chips - 1

        def body(step, carry):
            for s in range(PIECES):
                for way in (0, 1):
                    self.hop(way, step, s, False).wait_send()
                    self.share(way, step, s, False).wait()
            return carry

        lax.fori_loop(0, hops, body, 0)
        for s in range(PIECES):
            for way in (0, 1):
                self.share(way, hops, s, False).wait()
        self.local().wait()


class Scatter:
    def __init__(self, ring, part, tok, width, buffers, sems):
        self.ring, self.part, self.tok, self.width = ring, part, tok, width
        self.mate_out, self.mate_in, self.own, self.going, self.coming = buffers
        self.send, self.recv, self.mate_send, self.mate_recv = sems
        self.piece = tok // (2 * PIECES)

    @staticmethod
    def buffers(n, tok, width):
        chips = n // 2
        return [
            pltpu.VMEM((chips, tok, width), BF16),
            pltpu.VMEM((chips, tok, width), BF16),
            pltpu.VMEM((2, tok, width), F32),
            pltpu.VMEM((chips - 1, tok, width), BF16),
            pltpu.VMEM((chips - 1, tok, width), BF16),
        ]

    @staticmethod
    def semaphores(n):
        chips = n // 2
        kind = pltpu.SemaphoreType.DMA
        return [
            kind((2, chips - 1, PIECES)),
            kind((2, chips - 1, PIECES)),
            kind((chips,)),
            kind((chips,)),
        ]

    def rows(self, way, s):
        return pl.ds((way * PIECES + s) * self.piece, self.piece)

    def exchange(self, i):
        return remote(
            self.mate_out.at[i],
            self.mate_in.at[i],
            self.mate_send.at[i],
            self.mate_recv.at[i],
            {"seq": self.ring.mate},
        )

    def hop(self, way, i, s):
        ring = self.ring
        rows = self.rows(way, s)
        return remote(
            self.going.at[i, rows],
            self.coming.at[i, rows],
            self.send.at[way, i, s],
            self.recv.at[way, i, s],
            {"seq": ring.right if way == 0 else ring.left},
        )

    def produce(self, i):
        ring = self.ring
        half = self.tok // 2
        places = (ring.pos - 1 - i, ring.pos + 1 + i)
        for way in (0, 1):
            chunk = ring.at(places[way] + ring.chips, True)
            self.part(chunk, way, self.mate_out, i)
        self.exchange(i).start()
        slot = lax.rem(i, 2)
        for way in (0, 1):
            chunk = ring.at(places[way] + ring.chips)
            self.part(chunk, way, self.own, slot)

    def step(self, i, first):
        self.exchange(i).wait_recv()
        slot = lax.rem(i, 2)
        for s in range(PIECES):
            for way in (0, 1):
                rows = self.rows(way, s)
                value = self.own[slot, rows] + self.mate_in[i, rows].astype(F32)
                if not first:
                    self.hop(way, i - 1, s).wait_recv()
                    value = value + self.coming[i - 1, rows].astype(F32)
                self.going[i, rows] = value.astype(BF16)
                self.hop(way, i, s).start()

    def run(self, finish, between=None):
        last = self.ring.chips - 1
        self.produce(0)
        self.produce(1)
        self.step(0, True)

        def body(i, carry):
            self.produce(i + 1)
            self.step(i, False)
            return carry

        if between is None:
            lax.fori_loop(1, last, body, 0)
        else:
            lax.fori_loop(1, last // 2 + 1, body, 0)
            between()
            lax.fori_loop(last // 2 + 1, last, body, 0)
        self.exchange(last).wait_recv()
        slot = last % 2
        for s in range(PIECES):
            for way in (0, 1):
                rows = self.rows(way, s)
                self.hop(way, last - 1, s).wait_recv()
                value = self.own[slot, rows] + self.mate_in[last, rows].astype(F32)
                value = value + self.coming[last - 1, rows].astype(F32)
                finish(rows, value)

    def close(self):
        last = self.ring.chips - 1

        def body(i, carry):
            self.exchange(i).wait_send()
            for s in range(PIECES):
                for way in (0, 1):
                    self.hop(way, i, s).wait_send()
            return carry

        lax.fori_loop(0, last, body, 0)
        self.exchange(last).wait_send()


class Walk:
    def __init__(self, ring, own, out, sems):
        self.ring, self.own, self.out = ring, own, out
        self.send, self.recv, self.share_send, self.share_recv, self.keep = sems
        self.piece = own.shape[0] // PIECES
        self.last = ring.chips - 1

    @staticmethod
    def semaphores(n):
        kind = pltpu.SemaphoreType.DMA
        return [kind((n // 2, PIECES)) for _ in range(4)] + [kind((1,))]

    def block(self, i):
        ring = self.ring
        return ring.at(ring.pos - ring.sign * i + 2 * ring.chips)

    def hop(self, i, s, first=False):
        rows = pl.ds(s * self.piece, self.piece)
        there = self.out.at[self.block(i), rows]
        return remote(
            self.own.at[rows] if first else there,
            there,
            self.send.at[i, s],
            self.recv.at[i, s],
            {"seq": self.ring.onward},
        )

    def share(self, i, s, first=False):
        rows = pl.ds(s * self.piece, self.piece)
        there = self.out.at[self.block(i), rows]
        return remote(
            self.own.at[rows] if first else there,
            there,
            self.share_send.at[i, s],
            self.share_recv.at[i, s],
            {"seq": self.ring.mate},
        )

    def local(self):
        return pltpu.make_async_copy(self.own, self.out.at[self.ring.me], self.keep.at[0])

    def begin(self):
        for s in range(PIECES):
            self.hop(0, s, True).start()
        for s in range(PIECES):
            self.share(0, s, True).start()
        self.local().start()

    def pass_on(self, i):
        for s in range(PIECES):
            self.hop(i, s).wait_recv()

            @pl.when(i + 1 < self.last)
            def _():
                self.hop(i + 1, s).start()

            self.share(i + 1, s).start()

    def finish(self):
        def body(i, carry):
            for s in range(PIECES):
                self.hop(i, s).wait_send()
                self.share(i, s).wait()
            return carry

        lax.fori_loop(0, self.last, body, 0)
        for s in range(PIECES):
            self.share(self.last, s).wait()
        self.local().wait()


class Fold:
    def __init__(self, ring, part, buffers, sems):
        self.ring, self.part = ring, part
        self.mate_out, self.mate_in, self.own, self.going, self.coming = buffers
        self.swap_send, self.swap_recv, self.send, self.recv = sems
        self.piece = self.own.shape[0] // PIECES
        self.last = ring.chips - 1

    @staticmethod
    def buffers(n, tok, width):
        chips = n // 2
        return [
            pltpu.VMEM((2, tok, width), BF16),
            pltpu.VMEM((chips, tok, width), BF16),
            pltpu.VMEM((tok, width), F32),
            pltpu.VMEM((2, tok, width), BF16),
            pltpu.VMEM((chips - 1, tok, width), BF16),
        ]

    @staticmethod
    def semaphores(n):
        chips = n // 2
        kind = pltpu.SemaphoreType.DMA
        return [kind((chips,)), kind((chips,)), kind((chips, PIECES)), kind((chips, PIECES))]

    def swap(self, i):
        return remote(
            self.mate_out.at[lax.rem(i, 2)],
            self.mate_in.at[i],
            self.swap_send.at[i],
            self.swap_recv.at[i],
            {"seq": self.ring.mate},
        )

    def hop(self, i, s):
        rows = pl.ds(s * self.piece, self.piece)
        return remote(
            self.going.at[lax.rem(i, 2), rows],
            self.coming.at[i, rows],
            self.send.at[i, s],
            self.recv.at[i, s],
            {"seq": self.ring.onward},
        )

    def produce(self, i):
        ring = self.ring

        @pl.when(i >= 2)
        def _():
            self.swap(i - 2).wait_send()

        slot = lax.rem(i, 2)
        there = ring.at(ring.pos + ring.sign * (1 + i) + 2 * ring.chips, True)
        self.part(there, self.mate_out.at[slot])
        self.swap(i).start()
        here = ring.at(ring.pos - ring.sign * (1 + i) + 2 * ring.chips)
        self.part(here, self.own)

    def step(self, i):
        self.swap(i).wait_recv()

        @pl.when(i >= 2)
        def _():
            for s in range(PIECES):
                self.hop(i - 2, s).wait_send()

        for s in range(PIECES):
            rows = pl.ds(s * self.piece, self.piece)

            @pl.when(i > 0)
            def _():
                self.hop(i - 1, s).wait_recv()
                self.own[rows, :] = self.own[rows, :] + self.coming[i - 1, rows].astype(F32)

            value = self.own[rows, :] + self.mate_in[i, rows].astype(F32)
            self.going[lax.rem(i, 2), rows] = value.astype(BF16)
            self.hop(i, s).start()

    def run(self, finish, filler, before, after):
        last = self.last

        def body(i, carry):
            self.produce(i)
            before(i)
            self.step(i)
            after(i)
            filler(i)
            return carry

        lax.fori_loop(0, last, body, 0)
        self.produce(last)
        filler(last)
        self.swap(last).wait_recv()
        for s in range(PIECES):
            rows = pl.ds(s * self.piece, self.piece)
            self.hop(last - 1, s).wait_recv()
            value = self.own[rows, :] + self.mate_in[last, rows].astype(F32)
            finish(rows, value + self.coming[last - 1, rows].astype(F32))

    def close(self):
        last = self.last
        for s in range(PIECES):
            self.hop(last - 2, s).wait_send()
            self.hop(last - 1, s).wait_send()
        self.swap(last - 1).wait_send()
        self.swap(last).wait_send()


class Stored:
    def __init__(self, ring, parts, buffers, sems):
        self.ring, self.parts = ring, parts
        self.near, self.mate_in, self.going, self.coming = buffers
        self.swap_send, self.swap_recv, self.send, self.recv, self.load_sem = sems
        self.piece = self.near.shape[1] // PIECES
        self.last = ring.chips - 1

    @staticmethod
    def buffers(n, tok, width):
        chips = n // 2
        return [
            pltpu.VMEM((2, tok, width), BF16),
            pltpu.VMEM((chips, tok, width), BF16),
            pltpu.VMEM((2, tok, width), BF16),
            pltpu.VMEM((chips - 1, tok, width), BF16),
        ]

    @staticmethod
    def semaphores(n):
        chips = n // 2
        kind = pltpu.SemaphoreType.DMA
        return [
            kind((chips,)),
            kind((chips,)),
            kind((chips, PIECES)),
            kind((chips, PIECES)),
            kind((2,)),
        ]

    def swap(self, i):
        ring = self.ring
        there = ring.at(ring.pos + ring.sign * (1 + i) + 2 * ring.chips, True)
        return remote(
            self.parts.at[there],
            self.mate_in.at[i],
            self.swap_send.at[i],
            self.swap_recv.at[i],
            {"seq": ring.mate},
        )

    def load(self, i):
        ring = self.ring
        here = ring.at(ring.pos - ring.sign * (1 + i) + 2 * ring.chips)
        slot = lax.rem(i, 2)
        return pltpu.make_async_copy(
            self.parts.at[here], self.near.at[slot], self.load_sem.at[slot]
        )

    def hop(self, i, s):
        rows = pl.ds(s * self.piece, self.piece)
        return remote(
            self.going.at[lax.rem(i, 2), rows],
            self.coming.at[i, rows],
            self.send.at[i, s],
            self.recv.at[i, s],
            {"seq": self.ring.onward},
        )

    def begin(self):
        self.load(0).start()
        self.swap(0).start()
        self.swap(1).start()

    def step(self, i):
        self.load(i).wait()
        self.load(i + 1).start()
        self.swap(i).wait_recv()

        @pl.when(i + 2 <= self.last)
        def _():
            self.swap(i + 2).start()

        slot = lax.rem(i, 2)

        @pl.when(i >= 2)
        def _():
            for s in range(PIECES):
                self.hop(i - 2, s).wait_send()

        for s in range(PIECES):
            rows = pl.ds(s * self.piece, self.piece)
            value = self.near[slot, rows].astype(F32) + self.mate_in[i, rows].astype(F32)
            self.going[slot, rows] = value.astype(BF16)

            @pl.when(i > 0)
            def _():
                self.hop(i - 1, s).wait_recv()
                total = self.near[slot, rows].astype(F32) + self.mate_in[i, rows].astype(F32)
                total = total + self.coming[i - 1, rows].astype(F32)
                self.going[slot, rows] = total.astype(BF16)

            self.hop(i, s).start()

    def close(self, finish):
        last = self.last
        self.load(last).wait()
        self.swap(last).wait_recv()
        for s in range(PIECES):
            rows = pl.ds(s * self.piece, self.piece)
            self.hop(last - 1, s).wait_recv()
            value = self.near[last % 2, rows].astype(F32) + self.mate_in[last, rows].astype(F32)
            finish(rows, value + self.coming[last - 1, rows].astype(F32))
            self.hop(last - 2, s).wait_send()
            self.hop(last - 1, s).wait_send()

        def body(i, carry):
            self.swap(i).wait_send()
            return carry

        lax.fori_loop(0, last + 1, body, 0)


def first_kernel(n, f, *refs):
    own, w_qkv, small, routes, w_out, w_gate, w_up = refs[:7]
    hidden_all, mixed, w_head, router, gains, routes_all, gate_near, up_near, out_all = refs[7:16]
    near, small_all, out_rows, by_head, small_rows = refs[16:21]
    sems, out_sems, small_sems = refs[21:26], refs[26:31], refs[31:36]
    send, recv, beside_send, beside_recv, keep = refs[36:41]
    wide_send, wide_recv, row_send, row_recv, out_sem = refs[41:]
    ring = Ring(n, f)
    experts = router.shape[0]
    tok, width = own.shape
    rows = small.shape[0]
    hops = ring.chips - 1
    piece = width // ring.chips
    head = width // n
    for h in range(n):
        for k in range(3):
            start = k * width + h * head
            by_head[h, :, k * head : (k + 1) * head] = w_qkv[:, start : start + head]
    greet(ring, True, True)
    gather = Gather(ring, own, near, sems)
    gather_out = Gather(ring, out_rows, out_all, out_sems)
    gather_small = Gather(ring, small_rows, small_all, small_sems)
    out_mine = pl.ds(pl.multiple_of(ring.mine * rows, rows), rows)

    def push(kind, step):
        there = ring.peer(step)
        source, target = [
            (by_head.at[there], w_head.at[ring.me, ring.mine]),
            (small, small),
            (routes, routes_all.at[ring.me]),
        ][kind]
        return remote(
            source, target, send.at[kind, step], recv.at[kind, step], {"seq": there}
        )

    def aside(kind, step, over, first):
        origin = lax.rem(ring.me + n - step, n)
        block = w_head.at[origin, ring.mine]
        source = by_head.at[ring.me] if first else block
        return remote(
            source,
            block,
            beside_send.at[kind, step, over],
            beside_recv.at[kind, step, over],
            {"fsdp": ring.beside(over)},
        )

    def row(over, kind=0):
        return remote(
            [w_out, small][kind],
            [out_rows, small_rows][kind].at[out_mine],
            row_send.at[kind, over],
            row_recv.at[kind, over],
            {"fsdp": ring.beside(over)},
        )

    def wide(part, over):
        kind, part = divmod(part, ring.chips)
        these = pl.ds(part * piece, piece)
        return remote(
            [w_gate, w_up][kind].at[these],
            [gate_near, up_near][kind].at[over - 1, these],
            wide_send.at[kind, part, over],
            wide_recv.at[kind, part, over],
            {"fsdp": ring.beside(over)},
        )

    half_parts = ring.chips + ring.chips * UPPER // 8

    gather.begin()
    for over in range(1, f):
        row(over, 1).start()
        row(over).start()
    copies = [
        pltpu.make_async_copy(by_head.at[ring.me], w_head.at[ring.me, ring.mine], keep.at[0]),
        pltpu.make_async_copy(small, small_rows.at[out_mine], keep.at[1]),
        pltpu.make_async_copy(routes, routes_all.at[ring.me], keep.at[2]),
        pltpu.make_async_copy(w_out, out_rows.at[out_mine], keep.at[3]),
    ]
    for copy in copies:
        copy.start()

    def each_1(step, carry):
        for kind in (0, 2):
            push(kind, step).start()
        return carry

    lax.fori_loop(1, n, each_1, 0)
    for over in range(1, f):
        aside(0, 0, over, True).start()
        wide(0, over).start()
    copies[1].wait()
    for over in range(1, f):
        row(over, 1).wait_recv()
    gather_small.begin()
    each = -(-(n - 1) // 3)
    parts = 1

    def widen(parts):
        if parts < half_parts:
            for over in range(1, f):
                wide(parts, over).start()
        return parts + 1

    for i in range(hops):
        gather.pass_on(i)
        gather_small.pass_on(i)
        if 2 <= i < 5:
            for step in range((i - 2) * each + 1, min((i - 1) * each, n - 1) + 1):
                for kind in (0,):
                    push(kind, step).wait_recv()
                    for over in range(1, f):
                        aside(kind, step, over, False).start()
        parts = widen(parts)
        while i >= 4 and parts < half_parts:
            parts = widen(parts)
        if i == hops - 2:
            copies[3].wait()
            for over in range(1, f):
                row(over).wait_recv()
            gather_out.begin()
    gather.finish()
    gather_small.finish()
    copies[0].wait()
    copies[2].wait()

    def each_2(step, carry):
        push(2, step).wait_recv()
        for kind in (0, 2):
            push(kind, step).wait_send()
        return carry

    lax.fori_loop(1, n, each_2, 0)

    def each_3(step, carry):
        for over in range(1, f):
            aside(0, step, over, False).wait()
        return carry

    lax.fori_loop(0, n, each_3, 0)

    lanes = lax.broadcasted_iota(jnp.int32, (32, small.shape[1]), 1)
    places = lax.broadcasted_iota(jnp.int32, (32, small.shape[1]), 0)
    chosen = jnp.where(lanes == places, 1.0, 0.0).astype(BF16)
    for c in range(n):
        for x in range(f):
            start = (c * f + x) * rows
            flipped = dot(chosen, small_all[c, x * rows : (x + 1) * rows], BY_LAST)
            router[:, start : start + rows] = flipped[0:experts, :].astype(BF16)
            gains[:, start : start + rows] = flipped[experts : experts + 8, :]

    def out(c):
        return pltpu.make_async_copy(near.at[c], hidden_all.at[c], out_sem.at[c])

    def project(c, carry):
        value = near[c].astype(F32)
        inverse = lax.rsqrt(jnp.mean(value * value, -1, keepdims=True) + EPS)
        near[c] = (value * inverse * gains[0:1, :]).astype(BF16)
        out(c).start()
        here = pl.ds(pl.multiple_of(c * tok, tok), tok)
        total = jnp.zeros((tok, w_head.shape[3]), F32)
        for k in range(n):
            for x in range(f):
                start = (k * f + x) * rows
                if (k * f + x) % (256 // rows):
                    continue
                wide_rows = 256 // rows
                if wide_rows <= f:
                    right = w_head[k, x : x + wide_rows]
                else:
                    right = w_head[k : k + wide_rows // f]
                right = right.reshape(256, w_head.shape[3])
                total = total + dot(near[c, :, start : start + 256], right, MATMUL)
        mixed[here, :] = total
        return carry

    while parts < half_parts:
        parts = widen(parts)

    def second_phase(i, carry):
        lax.fori_loop(n * i // hops, n * (i + 1) // hops, project, 0)
        gather_out.pass_on(i)
        return carry

    lax.fori_loop(0, hops, second_phase, 0)
    for c in range(n):
        out(c).wait()
    gather_out.finish()
    for over in range(1, f):
        row(over).wait_send()
        row(over, 1).wait_send()
        for part in range(half_parts):
            wide(part, over).wait()


def first_gather(n, f, own, w_qkv, small, routes, w_out, w_gate, w_up):
    tok, width = own.shape
    experts = n
    by_head = jax.ShapeDtypeStruct((n, w_qkv.shape[0], 3 * width // n), BF16)
    kind = pltpu.SemaphoreType.DMA
    shape = jax.ShapeDtypeStruct
    return pl.pallas_call(
        partial(first_kernel, n, f),
        out_shape=[
            shape((n, tok, width), BF16),
            shape((n * tok, by_head.shape[2]), F32),
            shape((n, f) + by_head.shape[1:], BF16),
            shape((experts, width), BF16),
            shape((8, width), F32),
            shape((n,) + routes.shape, jnp.int32),
            shape((max(f - 1, 1),) + w_gate.shape, BF16),
            shape((max(f - 1, 1), w_up.shape[0] * UPPER // 8, w_up.shape[1]), BF16),
            shape((n, f * w_out.shape[0], w_out.shape[1]), BF16),
        ],
        in_specs=[VMEM] * 5 + [ANY] * 2,
        out_specs=[ANY] + [VMEM] * 4 + [ANY] * 4,
        scratch_shapes=[
            pltpu.VMEM((n, tok, width), BF16),
            pltpu.VMEM((n, f * small.shape[0], small.shape[1]), BF16),
            pltpu.VMEM((f * w_out.shape[0], w_out.shape[1]), BF16),
            pltpu.VMEM(by_head.shape, BF16),
            pltpu.VMEM((f * small.shape[0], small.shape[1]), BF16),
        ]
        + Gather.semaphores(n)
        + Gather.semaphores(n)
        + Gather.semaphores(n)
        + [kind((3, n)), kind((3, n)), kind((2, n, f)), kind((2, n, f)), kind((4,))]
        + [kind((2, n // 2, f)), kind((2, n // 2, f)), kind((2, f)), kind((2, f)), kind((n,))],
        compiler_params=pltpu.CompilerParams(
            collective_id=0, has_side_effects=True, vmem_limit_bytes=67_000_000
        ),
        name="first_gather",
    )(own, w_qkv, small, routes, w_out, w_gate, w_up)


def blocks_of(length):
    block = min(512, length)
    return block, length // block


def across_lanes(value):
    ones = jnp.ones((8, value.shape[1]), F32)
    total = lax.dot_general(
        ones, value, BY_LAST, precision=lax.Precision.HIGHEST, preferred_element_type=F32
    )
    return total[0:1, :]


def to_column(table, index, lanes):
    rows = lax.broadcasted_iota(jnp.int32, (table.shape[0], lanes), 0)
    chosen = jnp.where(rows == index, 1.0, 0.0)
    return lax.dot_general(
        table, chosen, BY_FIRST, precision=lax.Precision.HIGHEST, preferred_element_type=F32
    )


def half_turn(value, first_sign):
    half = value.shape[1] // 2
    lanes = lax.broadcasted_iota(jnp.int32, value.shape, 1)
    sign = jnp.where(lanes < half, first_sign, -first_sign)
    return pltpu.roll(value, half, 1) * sign


def set_angles(n, tables, starts, cosine, sine):
    tok = tables.shape[1]

    def angles(c, carry):
        here = pl.ds(pl.multiple_of(c * tok, tok), tok)
        cosine[here, :] = starts[0, c] * tables[0] - starts[1, c] * tables[1]
        sine[here, :] = starts[1, c] * tables[0] + starts[0, c] * tables[1]
        return carry

    lax.fori_loop(0, n, angles, 0)


class Spread:
    def __init__(self, ring, block, out, sems):
        self.ring, self.block, self.out = ring, block, out
        self.send, self.recv, self.keep = sems

    @staticmethod
    def semaphores(n):
        kind = pltpu.SemaphoreType.DMA
        return [kind((n,)), kind((n,)), kind((1,))]

    def push(self, step):
        return remote(
            self.block,
            self.out.at[self.ring.me],
            self.send.at[step],
            self.recv.at[step],
            {"seq": self.ring.peer(step)},
        )

    def local(self):
        return pltpu.make_async_copy(self.block, self.out.at[self.ring.me], self.keep.at[0])

    def begin(self):

        def each_4(step, carry):
            self.push(step).start()
            return carry

        lax.fori_loop(1, self.ring.n, each_4, 0)
        self.local().start()

    def finish(self):

        def each_5(step, carry):
            self.push(step).wait()
            return carry

        lax.fori_loop(1, self.ring.n, each_5, 0)
        self.local().wait()

    def total(self):
        total = self.out[0]
        for device in range(1, self.ring.n):
            total = total + self.out[device]
        return total


def attention_kernel(n, f, factor, *refs):
    mixed, tables, starts, gains, upstream, w_up, w_down = refs[:7]
    q_ref, k_ref, v_ref, out_ref, exact_ref, sums_ref, squares = refs[7:14]
    upstream_all, by_token, up_rest, down_near = refs[14:18]
    partial_sums, arrived, cosine, sine = refs[18:22]
    sems, walk_sems = refs[22:25], refs[25:30]
    deal_send, deal_recv, deal_keep, wide_send, wide_recv = refs[30:]
    ring = Ring(n, f)
    length, head = q_ref.shape
    width = head * n
    block, count = blocks_of(length)
    greet(ring, True, True)
    rest = up_rest.shape[1]
    later = pl.ds(w_up.shape[0] - rest, rest)

    def wide(kind, over):
        return remote(
            [w_up.at[later], w_down.at[pl.ds(0, down_near.shape[1])]][kind],
            [up_rest, down_near][kind].at[over - 1],
            wide_send.at[kind, over],
            wide_recv.at[kind, over],
            {"fsdp": ring.beside(over)},
        )

    for over in range(1, f):
        wide(0, over).start()
        wide(1, over).start()
    walk = Gather(ring, upstream, upstream_all, walk_sems)
    last = walk.last
    mine = pl.ds(pl.multiple_of(ring.me * head, head), head)

    def deal(there):
        these = pl.ds(pl.multiple_of(there * tok, tok), tok)
        return remote(
            out_ref.at[these],
            by_token.at[:, mine],
            deal_send.at[there],
            deal_recv.at[ring.me],
            {"seq": there},
        )

    def dealt(origin):
        return remote(
            out_ref.at[pl.ds(0, tok)],
            by_token.at[:, pl.ds(pl.multiple_of(origin * head, head), head)],
            deal_send.at[origin],
            deal_recv.at[origin],
            {"seq": origin},
        )

    tok = tables.shape[1]

    def measure(b, carry):
        here = pl.ds(pl.multiple_of(b * block, block), block)
        for kind in (0, 1):
            raw = mixed[here, kind * head : (kind + 1) * head]
            partial_sums[pl.ds(kind * count + b, 1), :] = across_lanes(raw * raw)
        v_ref[here, :] = mixed[here, 2 * head :].astype(BF16)
        return carry

    lax.fori_loop(0, count, measure, 0)
    spread = Spread(ring, partial_sums, arrived, sems)
    spread.begin()
    walk.begin()

    set_angles(n, tables, starts, cosine, sine)
    spread.finish()
    squares[...] = spread.total()
    walk.pass_on(0)

    def prepare(b, carry):
        here = pl.ds(pl.multiple_of(b * block, block), block)
        for kind, target in ((0, q_ref), (1, k_ref)):
            inverse = lax.rsqrt(to_column(squares[...], kind * count + b, head) / width + EPS)
            raw = mixed[here, kind * head : (kind + 1) * head]
            normed = raw * inverse * gains[kind + 1 : kind + 2, mine]
            turned = half_turn(normed, -1.0)
            target[here, :] = (normed * cosine[here, :] + turned * sine[here, :]).astype(BF16)
        return carry

    lax.fori_loop(0, count, prepare, 0)
    rows = lax.broadcasted_iota(jnp.int32, (block, block), 0)
    cols = lax.broadcasted_iota(jnp.int32, (block, block), 1)

    def outer(i, carry):
        here = pl.ds(pl.multiple_of(i * block, block), block)
        part = q_ref[here, :]

        def inner(j, state, masked):
            top, total, acc = state
            there = pl.ds(pl.multiple_of(j * block, block), block)
            scores = dot(part, k_ref[there, :], BY_LAST) * factor
            if masked:
                scores = jnp.where(cols <= rows, scores, NEG)
            new = jnp.maximum(top, jnp.max(scores, -1, keepdims=True))
            scale = jnp.exp(top - new)
            expd = jnp.exp(scores - new)
            total = total * scale + jnp.sum(expd, -1, keepdims=True)
            acc = acc * scale + dot(expd.astype(BF16), v_ref[there, :], MATMUL)
            return new, total, acc

        state = (
            jnp.full((block, 1), NEG, F32),
            jnp.zeros((block, 1), F32),
            jnp.zeros((block, head), F32),
        )
        state = lax.fori_loop(0, i, lambda j, s: inner(j, s, False), state)
        top, total, acc = inner(i, state, True)
        exact = acc / total
        exact_ref[here, :] = exact
        out_ref[here, :] = exact.astype(BF16)
        column = jnp.broadcast_to(top + jnp.log(total), (block, 128))
        sums_ref[:, here] = jnp.transpose(column)[0:8, :]

        for r in range(block // tok):
            there = i * (block // tok) + r

            @pl.when(there != ring.me)
            def _():
                deal(there).start()

        @pl.when((i > 0) & (i < last))
        def _():
            walk.pass_on(i)

        return carry

    lax.fori_loop(0, count, outer, 0)
    these = pl.ds(pl.multiple_of(ring.me * tok, tok), tok)
    local = pltpu.make_async_copy(out_ref.at[these], by_token.at[:, mine], deal_keep.at[0])
    local.start()
    for i in range(count, last):
        walk.pass_on(i)
    walk.finish()

    def each_6(step, carry):
        deal(ring.peer(step)).wait_send()
        dealt(ring.peer(step)).wait_recv()
        return carry

    lax.fori_loop(1, n, each_6, 0)
    local.wait()
    for over in range(1, f):
        wide(0, over).wait()
        wide(1, over).wait()


def attention(n, f, mixed, tables, starts, gains, upstream, w_up, w_down, factor):
    length, head = mixed.shape[0], mixed.shape[1] // 3
    block, count = blocks_of(length)
    shape = jax.ShapeDtypeStruct
    return pl.pallas_call(
        partial(attention_kernel, n, f, factor),
        out_shape=[
            shape((length, head), BF16),
            shape((length, head), BF16),
            shape((length, head), BF16),
            shape((length, head), BF16),
            shape((length, head), F32),
            shape((8, length), F32),
            shape((2 * count, block), F32),
            shape((n,) + upstream.shape, BF16),
            shape((length // n, head * n), BF16),
            shape((max(f - 1, 1), w_up.shape[0] - w_up.shape[0] * UPPER // 8, w_up.shape[1]), BF16),
            shape((max(f - 1, 1), w_down.shape[0] * DOWN // 8, w_down.shape[1]), BF16),
        ],
        in_specs=[VMEM] * 5 + [ANY] * 2,
        out_specs=[VMEM] * 7 + [ANY, VMEM, ANY, ANY],
        scratch_shapes=[
            pltpu.VMEM((2 * count, block), F32),
            pltpu.VMEM((n, 2 * count, block), F32),
            pltpu.VMEM((length, head), F32),
            pltpu.VMEM((length, head), F32),
        ]
        + Spread.semaphores(n)
        + Gather.semaphores(n)
        + [pltpu.SemaphoreType.DMA((n,)), pltpu.SemaphoreType.DMA((n,))]
        + [pltpu.SemaphoreType.DMA((1,))]
        + [pltpu.SemaphoreType.DMA((2, f)), pltpu.SemaphoreType.DMA((2, f))],
        compiler_params=pltpu.CompilerParams(
            collective_id=5, has_side_effects=True, vmem_limit_bytes=67_000_000
        ),
        cost_estimate=pl.CostEstimate(
            flops=2 * length * length * head,
            transcendentals=length * length // 2,
            bytes_accessed=8 * length * head,
        ),
        name="attention",
    )(mixed, tables, starts, gains, upstream, w_up, w_down)


def attention_back_kernel(n, f, factor, *refs):
    q_ref, k_ref, v_ref, by_token, sums_ref, exact, mixed, tables, starts, gains, squares = refs[:11]
    d_attn, attended, own_hidden, d_logits = refs[11:15]
    far = refs[15:19]
    d_mixed, gain_head, qkv_part, proj, router, first_in, second_in = refs[19:26]
    dq_ref, dk_ref, dv_ref, delta, partial_sums, arrived, d_attn_all, first, d_ref = refs[26:35]
    cosine, sine = refs[35:37]
    near = refs[37:41]
    rows_in, d_gate, d_up, hidden = near
    walk_sems, spread_sems = refs[41:46], refs[46:49]
    load_sem, first_send, first_recv, deal_send, deal_recv, deal_keep = refs[49:]
    ring = Ring(n, f)
    length, head = q_ref.shape
    width = head * n
    units = first_in.shape[2]
    block, count = blocks_of(length)
    loads = [
        pltpu.make_async_copy(
            source.at[:, units:] if k in (1, 2) else source, target, load_sem.at[k]
        )
        for k, (source, target) in enumerate(zip(far, near))
    ]
    for load in loads:
        load.start()
    greet(ring, True, True)
    tok = d_attn.shape[0]
    here_rows = pl.ds(pl.multiple_of(ring.me * tok, tok), tok)
    mine = pl.ds(pl.multiple_of(ring.me * head, head), head)

    def deal(step):
        there = ring.peer(step)
        return remote(
            by_token.at[:, pl.ds(pl.multiple_of(there * head, head), head)],
            d_ref.at[here_rows],
            deal_send.at[step],
            deal_recv.at[step],
            {"seq": there},
        )

    local = pltpu.make_async_copy(
        by_token.at[:, pl.ds(pl.multiple_of(ring.me * head, head), head)],
        d_ref.at[here_rows],
        deal_keep.at[0],
    )

    def each_7(step, carry):
        deal(step).start()
        return carry

    lax.fori_loop(1, n, each_7, 0)
    local.start()
    walk = Gather(ring, d_attn, d_attn_all, walk_sems)
    walk.begin()
    last = walk.last
    tiles = ring.chips
    size = width // tiles

    def send_first(kind, at, j):
        these = pl.ds(pl.multiple_of(at * size, size), size)
        tile = kind * tiles + at
        return remote(
            first.at[tile, j],
            [first_in, second_in][kind].at[j, these],
            first_send.at[tile, j],
            first_recv.at[tile, j],
            {"fsdp": ring.beside(f - 1 - j)},
        )

    set_angles(n, tables, starts, cosine, sine)
    for load in loads[:3]:
        load.wait()

    def early(kind, right):
        def body(at, carry):
            these = pl.ds(pl.multiple_of(at * size, size), size)
            for j in range(f - 1):
                part = slice(j * units, (j + 1) * units)
                value = dot(rows_in[:, these], right[:, part], BY_FIRST)
                first[kind * tiles + at, j] = value.astype(BF16)
                send_first(kind, at, j).start()
            return carry

        lax.fori_loop(0, EARLY if kind else tiles, body, 0)

    early(0, d_gate)
    early(1, d_up)

    def each_8(step, carry):
        deal(step).wait()
        return carry

    lax.fori_loop(1, n, each_8, 0)
    local.wait()
    dq_ref[...] = jnp.zeros_like(dq_ref)

    def measure(b, carry):
        here = pl.ds(pl.multiple_of(b * block, block), block)
        value = across_lanes(d_ref[here, :].astype(F32) * exact[here, :])
        delta[:, here] = jnp.broadcast_to(value, (8, block))
        return carry

    lax.fori_loop(0, count, measure, 0)
    rows = lax.broadcasted_iota(jnp.int32, (block, block), 0)
    cols = lax.broadcasted_iota(jnp.int32, (block, block), 1)

    def outer(j, carry):
        there = pl.ds(pl.multiple_of(j * block, block), block)
        keys = k_ref[there, :]
        values = v_ref[there, :]

        def inner(i, state, masked):
            d_keys, d_values = state
            here = pl.ds(pl.multiple_of(i * block, block), block)
            part = q_ref[here, :]
            d_part = d_ref[here, :]
            scores = dot(keys, part, BY_LAST) * factor
            if masked:
                scores = jnp.where(rows <= cols, scores, NEG)
            probs = jnp.exp(scores - sums_ref[0:1, here])
            d_probs = dot(values, d_part, BY_LAST)
            d_scores = (probs * (d_probs - delta[0:1, here])).astype(BF16)
            d_values = d_values + dot(probs.astype(BF16), d_part, MATMUL)
            d_keys = d_keys + dot(d_scores, part, MATMUL)
            dq_ref[here, :] += dot(d_scores, keys, BY_FIRST)
            return d_keys, d_values

        zero = jnp.zeros((block, head), F32)
        state = inner(j, (zero, zero), True)
        state = lax.fori_loop(j + 1, count, lambda i, s: inner(i, s, False), state)
        dk_ref[there, :] = state[0]
        dv_ref[there, :] = state[1]

        @pl.when((j >= 1) & (j < last + 1))
        def _():
            walk.pass_on(j - 1)

        return carry

    lax.fori_loop(0, count, outer, 0)

    def unturn(b, carry):
        here = pl.ds(pl.multiple_of(b * block, block), block)
        for kind, source in ((0, dq_ref), (1, dk_ref)):
            grad = (source[here, :] * factor).astype(BF16).astype(F32)
            grad = grad * cosine[here, :] + half_turn(grad * sine[here, :], 1.0)
            source[here, :] = grad
            raw = mixed[here, kind * head : (kind + 1) * head]
            partial_sums[pl.ds(kind * count + b, 1), :] = across_lanes(
                raw * gains[kind + 1 : kind + 2, mine] * grad
            )
        return carry

    lax.fori_loop(0, count, unturn, 0)
    spread = Spread(ring, partial_sums, arrived, spread_sems)
    spread.begin()
    walk.pass_on(count - 1)
    loads[3].wait()
    spread.finish()
    total = spread.total()
    gain_head[...] = jnp.zeros_like(gain_head)

    def close(b, carry):
        here = pl.ds(pl.multiple_of(b * block, block), block)
        for kind, source in ((0, dq_ref), (1, dk_ref)):
            index = kind * count + b
            inverse = lax.rsqrt(to_column(squares[...], index, head) / width + EPS)
            inner = to_column(total, index, head) / width
            raw = mixed[here, kind * head : (kind + 1) * head]
            grad = source[here, :]
            value = inverse * gains[kind + 1 : kind + 2, mine] * grad
            value = value - raw * (inverse * inverse * inverse) * inner
            d_mixed[here, kind * head : (kind + 1) * head] = value.astype(BF16)
            gain_head[kind + 2 : kind + 3, :] += jnp.sum(raw * inverse * grad, 0, keepdims=True)
        d_mixed[here, 2 * head :] = dv_ref[here, :].astype(BF16)
        return carry

    lax.fori_loop(0, count, close, 0)
    walk.pass_on(count)
    chunks, beside, rows_each = qkv_part.shape[1], qkv_part.shape[0], qkv_part.shape[2]
    span = width // chunks

    def weigh(c, carry):
        these = pl.ds(pl.multiple_of(c * span, span), span)
        value = dot(hidden[:, these], d_mixed[...], BY_FIRST).astype(BF16)
        for x in range(beside):
            qkv_part[x, c] = value[x * rows_each : (x + 1) * rows_each]
        return carry

    lax.fori_loop(0, chunks, weigh, 0)
    for i in range(count + 1, last):
        walk.pass_on(i)
    router[...] = jnp.zeros_like(router)

    def route(c, carry):
        router[...] += dot(d_logits[c], own_hidden[c], MATMUL)
        return carry

    lax.fori_loop(0, n, route, 0)
    walk.finish()
    group = block // tok
    tile = min(512, width)

    def project(c, carry):
        left = attended[pl.ds(pl.multiple_of(c * block, block), block), :]
        for start in range(0, width, tile):
            cols = slice(start, start + tile)
            right = d_attn_all[pl.ds(c * group, group), :, cols].reshape(block, tile)
            value = dot(left, right, BY_FIRST)

            @pl.when(c == 0)
            def _():
                proj[:, cols] = value

            @pl.when(c > 0)
            def _():
                proj[:, cols] = proj[:, cols] + value

        return carry

    lax.fori_loop(0, count, project, 0)
    for at in range(tiles + EARLY):
        for j in range(f - 1):
            send_first(at // tiles, at % tiles, j).wait()


def attention_back(
    n, f, queries, keys, values, by_token, sums, exact, mixed, tables, starts, gains, squares,
    d_attn, attended, own_hidden, d_logits, rows_in, d_gate, d_up, hidden, rows, factor
):
    length, head = queries.shape
    tok, width = d_attn.shape
    block, count = blocks_of(length)
    experts = d_logits.shape[1]
    shape = jax.ShapeDtypeStruct
    kind = pltpu.SemaphoreType.DMA
    flat, every = d_gate.shape
    units = every // f
    tiles = n // 2
    grad = shape((max(f - 1, 1), width, units), BF16)
    return pl.pallas_call(
        partial(attention_back_kernel, n, f, factor),
        out_shape=[
            shape((length, 3 * head), BF16),
            shape((8, head), F32),
            shape((f, n, rows, 3 * head), BF16),
            shape((head, width), F32),
            shape((experts, head), F32),
            grad,
            grad,
        ],
        in_specs=[VMEM] * 15 + [ANY] * 4,
        out_specs=[VMEM] * 5 + [ANY] * 2,
        scratch_shapes=[pltpu.VMEM((length, head), F32)] * 3
        + [
            pltpu.VMEM((8, length), F32),
            pltpu.VMEM((2 * count, block), F32),
            pltpu.VMEM((n, 2 * count, block), F32),
            pltpu.VMEM((n, tok, width), BF16),
            pltpu.VMEM((tiles + EARLY, max(f - 1, 1), width // tiles, units), BF16),
            pltpu.VMEM((length, head), BF16),
            pltpu.VMEM((length, head), F32),
            pltpu.VMEM((length, head), F32),
            pltpu.VMEM(rows_in.shape, BF16),
            pltpu.VMEM((flat, every - units), BF16),
            pltpu.VMEM((flat, every - units), BF16),
            pltpu.VMEM(hidden.shape, BF16),
        ]
        + Gather.semaphores(n)
        + Spread.semaphores(n)
        + [kind((4,))]
        + [kind((tiles + EARLY, max(f - 1, 1))), kind((tiles + EARLY, max(f - 1, 1)))]
        + [kind((n,)), kind((n,)), kind((1,))],
        compiler_params=pltpu.CompilerParams(
            collective_id=6, has_side_effects=True, vmem_limit_bytes=67_000_000
        ),
        name="attention_back",
    )(
        queries, keys, values, by_token, sums, exact, mixed, tables, starts, gains, squares,
        d_attn, attended, own_hidden, d_logits, rows_in, d_gate, d_up, hidden
    )


def core_kernel(n, f, *refs):
    by_token, w_out, tokens, upstream, gain, router, routes, routes_all, upstream_all = refs[:9]
    shards_in = refs[9 : 8 + 4 * f]
    refs = refs[8 + 4 * f :]
    d_middle, middle, d_attn, d_by_token, d_logits_all, gain_two = refs[:6]
    own_hidden, rows_out, d_out, inner_out, d_gate_out, d_up_out, moe_out = refs[6:13]
    refs = refs[13:]
    w_near, w_gate, w_up, w_down, d_logits, arrived, outgoing, weights_in = refs[:8]
    refs = refs[8:]
    ring_in, mate_near, d_mate_in, coming, going, d_mate_out, own, lift = refs[:8]
    refs = refs[8:]
    rows_now, lifted, d_now, inner_now, d_gate_now, d_up_now, moe_now, d_weight, places = refs[:9]
    refs = refs[9:]
    hop_send, hop_recv, share_send, share_recv, swap_send, swap_recv = refs[:6]
    sum_send, sum_recv, send, recv, keep, load_sem, lift_sem, stage_sem, own_sem = refs[6:15]
    down_send, down_recv = refs[15:]
    ring = Ring(n, f)
    tok, width = tokens.shape
    head = width // n
    chips = ring.chips
    last = chips - 1
    capacity = rows_now.shape[1] // 2
    hidden_units = w_gate.shape[1]
    piece = tok // PIECES
    sign = 1 - 2 * ring.core
    onward = ring.at(ring.pos + sign + chips)
    local_units = hidden_units // f

    loads = [pltpu.make_async_copy(w_out, w_near, keep.at[0])]
    half_width = width * UPPER // 8
    soon = width * DOWN // 8
    sources = []
    for j in range(f):
        cols = slice(j * local_units, (j + 1) * local_units)
        sources.append((w_gate.at[:, cols], 0, j))
        sources.append((w_down.at[pl.ds(0, soon), cols] if j else w_down.at[:, cols], 2, j))
        if j:
            sources.append((w_up.at[pl.ds(0, half_width), cols], 1, j))
            sources.append((w_up.at[pl.ds(half_width, width - half_width), cols], 3, j))
        else:
            sources.append((w_up.at[:, cols], 1, j))
    for source, (target, kind, j) in zip(shards_in, sources):
        loads.append(pltpu.make_async_copy(source, target, load_sem.at[kind, j]))
    for load in loads:
        load.start()

    def chunk_of(i, other):
        return ring.at(
            ring.pos + (sign * (1 + i) if other else -sign * (1 + i)) + 2 * chips, other
        )

    def lift_copy(i, other):
        slot = lax.rem(i, 2)
        return pltpu.make_async_copy(
            upstream_all.at[chunk_of(i, other)],
            lift.at[slot, other],
            lift_sem.at[slot, other],
        )

    lift_copy(0, 0).start()
    lift_copy(0, 1).start()
    greet(ring, True, True)

    def down_rest(over):
        rows = pl.ds(soon, width - soon)
        return remote(
            shards_in[1].at[rows],
            w_down.at[rows, over * local_units : (over + 1) * local_units],
            down_send.at[over],
            down_recv.at[over],
            {"fsdp": ring.beside(over)},
        )

    for over in range(1, f):
        down_rest(over).start()

    mine = pl.ds(pl.multiple_of(ring.me * head, head), head)

    before = lax.broadcasted_iota(jnp.int32, (tok, tok), 0)
    after = lax.broadcasted_iota(jnp.int32, (tok, tok), 1)
    earlier = jnp.where(before < after, 1.0, 0.0).astype(BF16)

    def stand(c, carry):
        here = jnp.where(routes_all[c] == ring.me, 1.0, 0.0)
        here = jnp.sum(here, 0, keepdims=True)
        count = dot(jnp.broadcast_to(here, (8, tok)).astype(BF16), earlier, MATMUL)
        places[c] = jnp.where(jnp.broadcast_to(here, (8, tok)) > 0.5, count, -1.0)
        return carry

    lax.fori_loop(0, n, stand, 0)
    loads[0].wait()
    tile = min(512, width)
    squares = jnp.zeros((tok, 1), F32)
    for start in range(0, width, tile):
        cols = slice(start, start + tile)
        value = tokens[:, cols].astype(F32) + dot(by_token[...], w_near[:, cols], MATMUL)
        middle[:, cols] = value
        squares = squares + jnp.sum(value * value, -1, keepdims=True)
    inverse = lax.rsqrt(squares / width + EPS)
    ring_in[last] = (middle[...] * inverse * gain[...]).astype(BF16)

    def hop(i, s):
        rows = pl.ds(s * piece, piece)
        source = lax.rem(i + last, chips)
        return remote(
            ring_in.at[source, rows],
            ring_in.at[i, rows],
            hop_send.at[i, s],
            hop_recv.at[i, s],
            {"seq": onward},
        )

    def share(i, s):
        rows = pl.ds(s * piece, piece)
        return remote(
            ring_in.at[i, rows],
            mate_near.at[i, rows],
            share_send.at[i, s],
            share_recv.at[i, s],
            {"seq": ring.mate},
        )

    for s in range(PIECES):
        hop(0, s).start()
    for s in range(PIECES):
        share(last, s).start()

    logits = dot(router[...], ring_in[last], BY_LAST)
    expd = jnp.exp(logits - jnp.max(logits, 0, keepdims=True))
    gate = expd / jnp.sum(expd, 0, keepdims=True)
    experts = lax.broadcasted_iota(jnp.int32, gate.shape, 0)
    named = jnp.zeros(gate.shape, F32)
    for k in range(routes.shape[0]):
        named = named + jnp.where(routes[k : k + 1, :] == experts, 1.0, 0.0)
    weights = gate * named
    for e in range(n):
        outgoing[e] = jnp.broadcast_to(weights[e : e + 1, :], (8, tok))

    def push(there):
        return remote(
            outgoing.at[there],
            weights_in.at[ring.me],
            send.at[1, there],
            recv.at[1, ring.me],
            {"seq": there},
        )

    def pushed(origin):
        return remote(
            outgoing.at[origin],
            weights_in.at[origin],
            send.at[1, origin],
            recv.at[1, origin],
            {"seq": origin},
        )

    def each_9(step, carry):
        push(ring.peer(step)).start()
        return carry

    lax.fori_loop(1, n, each_9, 0)
    weights_in[ring.me] = outgoing[ring.me]
    for load in loads[1:]:
        load.wait()
    for over in range(1, f):
        down_rest(over).wait_recv()

    def swap(i):
        return remote(
            d_mate_out.at[lax.rem(i, 2)],
            d_mate_in.at[i],
            swap_send.at[i],
            swap_recv.at[i],
            {"seq": ring.mate},
        )

    def sum_hop(i, s):
        rows = pl.ds(s * piece, piece)
        return remote(
            going.at[lax.rem(i, 2), rows],
            coming.at[i, rows],
            sum_send.at[i, s],
            sum_recv.at[i, s],
            {"seq": onward},
        )

    def sum_step(i):
        swap(i).wait_recv()

        @pl.when(i >= 2)
        def _():
            for s in range(PIECES):
                sum_hop(i - 2, s).wait_send()

        for s in range(PIECES):
            rows = pl.ds(s * piece, piece)

            @pl.when(i > 0)
            def _():
                sum_hop(i - 1, s).wait_recv()
                own[rows, :] = own[rows, :] + coming[i - 1, rows].astype(F32)

            value = own[rows, :] + d_mate_in[i, rows].astype(F32)
            going[lax.rem(i, 2), rows] = value.astype(BF16)
            sum_hop(i, s).start()

    def give(kind, target, other, slot):
        chunk = target
        source, sink = [
            (rows_now, rows_out),
            (d_now, d_out),
            (inner_now, inner_out),
            (d_gate_now, d_gate_out),
            (d_up_now, d_up_out),
            (moe_now, moe_out),
        ][kind]
        size = tok if kind == 5 else capacity
        return pltpu.make_async_copy(
            source.at[slot, pl.ds(other * size, size)],
            sink.at[chunk],
            stage_sem.at[slot, kind, other],
        )

    def keep_hidden(i, other):
        return pltpu.make_async_copy(
            (mate_near if other else ring_in).at[i, :, mine],
            own_hidden.at[chunk_of(i, other)],
            own_sem.at[other, i],
        )

    def report(there, slot, other):
        return remote(
            d_weight.at[slot, other],
            arrived.at[ring.me],
            send.at[2, there],
            recv.at[2, ring.me],
            {"seq": there},
        )

    def reported(origin):
        return remote(
            d_weight.at[0, 0],
            arrived.at[origin],
            send.at[2, origin],
            recv.at[2, origin],
            {"seq": origin},
        )

    def pass_on(i):
        for s in range(PIECES):
            hop(i, s).wait_recv()

            @pl.when(i < last - 1)
            def _():
                hop(i + 1, s).start()

            share(i, s).start()

    def work(i):
        slot = lax.rem(i, 2)
        chunks = (chunk_of(i, 0), chunk_of(i, 1))
        for s in range(PIECES):
            share(i, s).wait_recv()
        keep_hidden(i, 0).start()
        keep_hidden(i, 1).start()
        for other in (0, 1):
            lift_copy(i, other).wait()

        @pl.when(i < last)
        def _():
            lift_copy(i + 1, 0).start()
            lift_copy(i + 1, 1).start()
            pushed(chunks[0]).wait_recv()

        pushed(chunks[1]).wait_recv()

        @pl.when(i >= 2)
        def _():
            for kind in range(6):
                for other in (0, 1):
                    give(kind, chunks[other], other, slot).wait()
            swap(i - 2).wait_send()
            for other in (0, 1):
                report(chunk_of(i - 2, other), slot, other).wait_send()

        slots = lax.broadcasted_iota(jnp.int32, (capacity, tok), 0).astype(F32)
        picks, rates = [], []
        for other in (0, 1):
            rows = slice(other * capacity, (other + 1) * capacity)
            where = slots == jnp.broadcast_to(places[chunks[other], 0:1, :], (capacity, tok))
            pick = jnp.where(where, 1.0, 0.0)
            low = pick.astype(BF16)
            source = mate_near.at[i] if other else ring_in.at[i]
            share_of = weights_in[chunks[other], 0:1, :]
            rate = jnp.sum(jnp.where(where, share_of, 0.0), -1, keepdims=True)
            for start in range(0, width, tile):
                cols = slice(start, start + tile)
                rows_now[slot, rows, cols] = dot(low, source[:, cols], MATMUL).astype(BF16)
                picked = dot(low, lift[slot, other, :, cols], MATMUL)
                lifted[rows, cols] = picked.astype(BF16)
                d_now[slot, rows, cols] = (rate * picked).astype(BF16)
            picks.append((low, where))
            rates.append(rate)
        rate = jnp.concatenate(rates, 0)
        unit = min(256, hidden_units)
        for start in range(0, hidden_units, unit):
            cols = slice(start, start + unit)
            gate_act = dot(rows_now[slot], w_gate[:, cols], MATMUL)
            up_act = dot(rows_now[slot], w_up[:, cols], MATMUL)
            d_inner = dot(d_now[slot], w_down[:, cols], MATMUL)
            sigma = 1.0 / (1.0 + jnp.exp(-gate_act))
            silu = gate_act * sigma
            inner_now[slot, :, cols] = (silu * up_act).astype(BF16)
            d_gate_now[slot, :, cols] = (
                d_inner * up_act * sigma * (1.0 + gate_act * (1.0 - sigma))
            ).astype(BF16)
            d_up_now[slot, :, cols] = (d_inner * silu).astype(BF16)
        inner_product = jnp.zeros((2 * capacity, 1), F32)
        for start in range(0, width, tile):
            cols = slice(start, start + tile)
            produced = dot(inner_now[slot], w_down[cols, :], BY_LAST)
            produced = produced.astype(BF16).astype(F32)
            inner_product = inner_product + jnp.sum(
                produced * lifted[:, cols].astype(F32), -1, keepdims=True
            )
            scaled = (rate * produced).astype(BF16)
            d_rows = dot(d_gate_now[slot], w_gate[cols, :], BY_LAST)
            d_rows = (d_rows + dot(d_up_now[slot], w_up[cols, :], BY_LAST)).astype(BF16)
            for other in (0, 1):
                rows = slice(other * capacity, (other + 1) * capacity)
                low = picks[other][0]
                moe_now[slot, other * tok : (other + 1) * tok, cols] = dot(
                    low, scaled[rows], BY_FIRST
                ).astype(BF16)
                spread_rows = dot(low, d_rows[rows], BY_FIRST)
                if other:
                    d_mate_out[slot, :, cols] = spread_rows.astype(BF16)
                else:
                    own[:, cols] = spread_rows
        swap(i).start()
        for kind in range(6):
            for other in (0, 1):
                give(kind, chunks[other], other, slot).start()
        for other in (0, 1):
            rows = slice(other * capacity, (other + 1) * capacity)
            value = jnp.sum(
                jnp.where(picks[other][1], inner_product[rows], 0.0), 0, keepdims=True
            )
            d_weight[slot, other] = jnp.broadcast_to(value, (8, tok))
        report(chunks[1], slot, 1).start()

        @pl.when(i < last)
        def _():
            report(chunks[0], slot, 0).start()

    def body(i, carry):
        @pl.when(i < last)
        def _():
            pass_on(i)

        @pl.when(i > 0)
        def _():
            sum_step(i - 1)

        work(i)
        return carry

    lax.fori_loop(0, chips, body, 0)
    arrived[ring.me] = d_weight[last % 2, 0]

    def each_10(step, carry):
        reported(ring.peer(step)).wait_recv()
        return carry

    lax.fori_loop(1, n, each_10, 0)
    gate_back = jnp.concatenate([arrived[e, 0:1, :] for e in range(n)], 0)
    gate_back = gate * (gate_back - jnp.sum(gate * gate_back, 0, keepdims=True))
    d_logits[...] = gate_back.astype(BF16)

    def publish(step):
        return remote(
            d_logits,
            d_logits_all.at[ring.me],
            send.at[4, step],
            recv.at[4, step],
            {"seq": ring.peer(step)},
        )

    kept = pltpu.make_async_copy(d_logits, d_logits_all.at[ring.me], keep.at[1])
    swap(last).wait_recv()
    for s in range(PIECES):
        rows = pl.ds(s * piece, piece)
        sum_hop(last - 1, s).wait_recv()
        value = own[rows, :] + d_mate_in[last, rows].astype(F32)
        own[rows, :] = value + coming[last - 1, rows].astype(F32)
    d_hidden = own[...] + dot(gate_back.astype(BF16), router[...], BY_FIRST)
    value = middle[...]
    inner = jnp.mean(value * gain[...] * d_hidden, -1, keepdims=True)
    gain_two[...] = jnp.sum(value * inverse * d_hidden, 0, keepdims=True)
    d_value = inverse * gain[...] * d_hidden - value * (inverse * inverse * inverse) * inner
    d_value = upstream[...].astype(F32) + d_value
    d_middle[...] = d_value
    d_attn[...] = d_value.astype(BF16)
    for start in range(0, width, tile):
        cols = slice(start, start + tile)
        d_by_token[:, cols] = dot(d_attn[...], w_near[cols, :], BY_LAST).astype(BF16)

    def each_11(step, carry):
        publish(step).start()
        return carry

    lax.fori_loop(1, n, each_11, 0)
    kept.start()

    for over in range(1, f):
        down_rest(over).wait_send()
    for s in range(PIECES):
        share(last, s).wait_send()

    def settle(i, carry):
        for s in range(PIECES):
            hop(i, s).wait_send()
            share(i, s).wait_send()
        for other in (0, 1):
            keep_hidden(i, other).wait()
        return carry

    lax.fori_loop(0, last, settle, 0)
    for other in (0, 1):
        keep_hidden(last, other).wait()
    for s in range(PIECES):
        sum_hop(last - 2, s).wait_send()
        sum_hop(last - 1, s).wait_send()
    for i in (last - 1, last):
        swap(i).wait_send()
        for other in (0, 1):
            for kind in range(6):
                give(kind, chunk_of(i, other), other, i % 2).wait()
            if other or i < last:
                report(chunk_of(i, other), i % 2, other).wait_send()

    def each_12(step, carry):
        push(ring.peer(step)).wait_send()
        return carry

    lax.fori_loop(1, n, each_12, 0)

    def each_13(step, carry):
        publish(step).wait()
        return carry

    lax.fori_loop(1, n, each_13, 0)
    kept.wait()


def core_stage(
    n, f, by_token, w_out, tokens, upstream, gain, router, routes, routes_all, upstream_all, halves
):
    tok, width = tokens.shape
    experts = router.shape[0]
    units = f * halves[0].shape[1]
    capacity = min(tok, 5 * tok * TOPK // (4 * experts))
    chips = n // 2
    kind = pltpu.SemaphoreType.DMA
    shape = jax.ShapeDtypeStruct
    rows = 2 * capacity
    return pl.pallas_call(
        partial(core_kernel, n, f),
        out_shape=[
            shape((tok, width), F32),
            shape((tok, width), F32),
            shape((tok, width), BF16),
            shape((tok, width), BF16),
            shape((n, experts, tok), BF16),
            shape((1, width), F32),
            shape((n, tok, width // n), BF16),
            shape((n, capacity, width), BF16),
            shape((n, capacity, width), BF16),
            shape((n, capacity, units), BF16),
            shape((n, capacity, units), BF16),
            shape((n, capacity, units), BF16),
            shape((n, tok, width), BF16),
        ],
        in_specs=[VMEM, ANY] + [VMEM] * 6 + [ANY] * (4 * f),
        out_specs=[VMEM] * 4 + [ANY, VMEM] + [ANY] * 7,
        scratch_shapes=[
            pltpu.VMEM((width, width), BF16),
            pltpu.VMEM((width, units), BF16),
            pltpu.VMEM((width, units), BF16),
            pltpu.VMEM((width, units), BF16),
            pltpu.VMEM((experts, tok), BF16),
            pltpu.VMEM((n, 8, tok), F32),
            pltpu.VMEM((n, 8, tok), F32),
            pltpu.VMEM((n, 8, tok), F32),
            pltpu.VMEM((chips, tok, width), BF16),
            pltpu.VMEM((chips, tok, width), BF16),
            pltpu.VMEM((chips, tok, width), BF16),
            pltpu.VMEM((chips - 1, tok, width), BF16),
            pltpu.VMEM((2, tok, width), BF16),
            pltpu.VMEM((2, tok, width), BF16),
            pltpu.VMEM((tok, width), F32),
            pltpu.VMEM((2, 2, tok, width), BF16),
            pltpu.VMEM((2, rows, width), BF16),
            pltpu.VMEM((rows, width), BF16),
            pltpu.VMEM((2, rows, width), BF16),
            pltpu.VMEM((2, rows, units), BF16),
            pltpu.VMEM((2, rows, units), BF16),
            pltpu.VMEM((2, rows, units), BF16),
            pltpu.VMEM((2, 2 * tok, width), BF16),
            pltpu.VMEM((2, 2, 8, tok), F32),
            pltpu.VMEM((n, 8, tok), F32),
            kind((chips, PIECES)),
            kind((chips, PIECES)),
            kind((chips, PIECES)),
            kind((chips, PIECES)),
            kind((chips,)),
            kind((chips,)),
            kind((chips, PIECES)),
            kind((chips, PIECES)),
            kind((5, n)),
            kind((5, n)),
            kind((2,)),
            kind((4, f)),
            kind((2, 2)),
            kind((2, 6, 2)),
            kind((2, chips)),
            kind((f,)),
            kind((f,)),
        ],
        compiler_params=pltpu.CompilerParams(
            collective_id=1, has_side_effects=True, vmem_limit_bytes=67_000_000
        ),
        name="core_stage",
    )(by_token, w_out, tokens, upstream, gain, router, routes, routes_all, upstream_all, *halves)


def last_kernel(n, f, *refs):
    d_mixed, w_head, qkv_part, tokens, gain, d_middle, gain_two, gain_head = refs[:8]
    middle, proj, router, moe_part = refs[8:12]
    far_refs = refs[12:17]
    d_inputs, qkv_out, gains_out, second_in, third_in, grads_out, result = refs[17:24]
    proj_out, router_out = refs[24:26]
    beside_rows, summed, qkv_rows, gain_rows, gain_in, gain_side, stage, far_stage = refs[26:34]
    proj_low, proj_in, router_low = refs[34:37]
    near_refs = refs[37:42]
    rows_in, d_in, d_gate, d_up, inner_in = near_refs
    buffers, fold_sems = refs[42:47], refs[47:51]
    stored_buffers, stored_sems = refs[51:55], refs[55:60]
    side_send, side_recv, send, recv, keep, stage_sem, load_sem, far_send, far_recv = refs[60:]
    ring = Ring(n, f)
    _, width = tokens.shape
    slice_width = width // n
    units = grads_out.shape[2]
    chips = ring.chips
    size = width // chips
    loads = [
        pltpu.make_async_copy(source.at[:, :units] if k == 2 else source, target, load_sem.at[k])
        for k, (source, target) in enumerate(zip(far_refs, near_refs))
    ]
    greet(ring, True, True)

    def side(step):
        there = ring.beside(step)
        return remote(
            qkv_part.at[there],
            beside_rows.at[step - 1],
            side_send.at[0, step],
            side_recv.at[0, step],
            {"fsdp": there},
        )

    for step in range(1, f):
        side(step).start()

    def proj_side(step):
        there = ring.beside(step)
        return remote(
            proj_low.at[there],
            proj_in.at[step - 1],
            side_send.at[3, step],
            side_recv.at[3, step],
            {"fsdp": there},
        )

    def router_side(step):
        return remote(
            router_low.at[0],
            router_low.at[step],
            side_send.at[4, step],
            side_recv.at[4, step],
            {"fsdp": ring.beside(step)},
        )

    for x in range(f):
        proj_low[x] = proj[x].astype(BF16)
    router_low[0] = router[...].astype(BF16)
    for step in range(1, f):
        proj_side(step).start()
        router_side(step).start()

    def part(chunk, target):
        tile = min(512, width)
        for start in range(0, width, tile):
            cols = slice(start, start + tile)
            target[:, cols] = dot(d_mixed[chunk], w_head[cols, :], BY_LAST).astype(target.dtype)

    fold = Fold(ring, part, buffers, fold_sems)

    def finish(rows, value):
        d_inputs[rows, :] = value

    def store(i, which):
        these = pl.ds(pl.multiple_of(i * size, size), size)
        slot = lax.rem(i, 2)
        return pltpu.make_async_copy(
            stage.at[slot, which], grads_out.at[which, these], stage_sem.at[slot, which]
        )

    def filler(i):
        these = pl.ds(pl.multiple_of(i * size, size), size)
        slot = lax.rem(i, 2)
        pairs = ((rows_in, d_gate), (rows_in, d_up), (d_in, inner_in))
        for which, (left, right) in enumerate(pairs):

            @pl.when(i >= 2)
            def _():
                store(i - 2, which).wait()

            stage[slot, which] = dot(left[:, these], right[:, :units], BY_FIRST).astype(BF16)
            store(i, which).start()
        afar(i)

    def far(kind, i, j):
        these = pl.ds(pl.multiple_of(i * size, size), size)
        return remote(
            far_stage.at[lax.rem(i, 2), kind, j],
            [second_in, third_in][kind].at[j, these],
            far_send.at[kind, i, j],
            far_recv.at[kind, i, j],
            {"fsdp": ring.beside(f - 1 - j)},
        )

    def afar(i):
        these = pl.ds(pl.multiple_of(i * size, size), size)
        slot = lax.rem(i, 2)

        def make(kind, first_tile, left, right):
            @pl.when(i >= first_tile + 2)
            def _():
                for j in range(f - 1):
                    far(kind, i - 2, j).wait_send()

            @pl.when(i >= first_tile)
            def _():
                for j in range(f - 1):
                    part = slice((j + 1) * units, (j + 2) * units)
                    value = dot(left[:, these], right[:, part], BY_FIRST)
                    far_stage[slot, kind, j] = value.astype(BF16)
                    far(kind, i, j).start()

        make(0, EARLY, rows_in, d_up)
        make(1, 0, d_in, inner_in)

    def push(step):
        there = ring.peer(step)
        return remote(
            summed.at[there],
            qkv_rows.at[ring.me],
            send.at[0, step],
            recv.at[0, step],
            {"seq": there},
        )

    local = pltpu.make_async_copy(summed.at[ring.me], qkv_rows.at[ring.me], keep.at[0])

    stored = Stored(ring, moe_part, stored_buffers, stored_sems)

    def before(i):
        @pl.when(i == 0)
        def _():
            stored.begin()
            for load in loads:
                load.start()

    def spread_qkv():
        for step in range(1, f):
            side(step).wait_recv()

        def add(block, carry):
            value = qkv_part[ring.mine, block].astype(F32)
            for step in range(1, f):
                value = value + beside_rows[step - 1, block].astype(F32)
            summed[block] = value.astype(BF16)
            return carry

        lax.fori_loop(0, n, add, 0)

        def each_14(step, carry):
            push(step).start()
            return carry

        lax.fori_loop(1, n, each_14, 0)
        local.start()

    def after(i):
        stored.step(i)

        @pl.when(i == 0)
        def _():
            for load in loads:
                load.wait()

    fold.run(finish, filler, before, after)

    def settle(rows, value):
        result[rows, :] = (middle[rows, :] + value).astype(BF16)

    stored.close(settle)
    value = tokens[...].astype(F32)
    grad = d_inputs[...]
    inverse = lax.rsqrt(jnp.mean(value * value, -1, keepdims=True) + EPS)
    inner = jnp.mean(value * gain[...] * grad, -1, keepdims=True)
    gain_rows[...] = jnp.zeros_like(gain_rows)
    gain_rows[0:1, :] = jnp.sum(value * inverse * grad, 0, keepdims=True)
    gain_rows[1:2, :] = gain_two[...]

    def gains(step):
        there = ring.peer(step)
        cols = pl.ds(pl.multiple_of(there * slice_width, slice_width), slice_width)
        return remote(
            gain_rows.at[:, cols],
            gain_in.at[ring.me],
            send.at[1, step],
            recv.at[1, step],
            {"seq": there},
        )

    mine = pl.ds(pl.multiple_of(ring.me * slice_width, slice_width), slice_width)
    kept = pltpu.make_async_copy(gain_rows.at[:, mine], gain_in.at[ring.me], keep.at[1])

    def each_15(step, carry):
        gains(step).start()
        return carry

    lax.fori_loop(1, n, each_15, 0)
    kept.start()
    spread_qkv()
    d_value = inverse * gain[...] * grad - value * (inverse * inverse * inverse) * inner
    d_inputs[...] = d_middle[...] + d_value

    def each_16(step, carry):
        gains(step).wait()
        return carry

    lax.fori_loop(1, n, each_16, 0)
    kept.wait()
    total = gain_head[...]
    for device in range(n):
        total = total + gain_in[device]
    gain_side[0] = total

    def sums(step):
        return remote(
            gain_side.at[0],
            gain_side.at[step],
            side_send.at[1, step],
            side_recv.at[1, step],
            {"fsdp": ring.beside(step)},
        )

    for step in range(1, f):
        sums(step).start()
    proj_total = proj[ring.mine]
    router_total = router[...]
    for step in range(1, f):
        proj_side(step).wait()
        router_side(step).wait()
        proj_total = proj_total + proj_in[step - 1].astype(F32)
        router_total = router_total + router_low[step].astype(F32)
    proj_out[...] = proj_total
    router_out[...] = router_total
    fold.close()
    for i in (chips - 2, chips - 1):
        for which in range(3):
            store(i, which).wait()
    for step in range(1, f):
        side(step).wait_send()

    def each_17(step, carry):
        push(step).wait()
        return carry

    lax.fori_loop(1, n, each_17, 0)
    local.wait()
    piece = qkv_rows.shape[2] // 3
    for h in range(n):
        for k in range(3):
            start = k * width + h * piece
            qkv_out[:, start : start + piece] = qkv_rows[
                h, :, k * piece : (k + 1) * piece
            ].astype(F32)
    for step in range(1, f):
        sums(step).wait()
        total = total + gain_side[step]
    gains_out[...] = total
    for j in range(f - 1):
        for kind, first_tile in ((0, EARLY), (1, 0)):
            for i in range(first_tile, chips):
                far(kind, i, j).wait_recv()
                if i >= chips - 2:
                    far(kind, i, j).wait_send()


def last_stage(
    n, f, d_mixed, w_head, qkv_part, tokens, gain, d_middle, gain_two, gain_head,
    middle, proj, router, moe_part, rows_in, d_in, d_gate, d_up, inner_in, second
):
    tok, width = tokens.shape
    rows, across = qkv_part.shape[2:]
    units = second.shape[2]
    kind = pltpu.SemaphoreType.DMA
    shape = jax.ShapeDtypeStruct
    return pl.pallas_call(
        partial(last_kernel, n, f),
        out_shape=[
            shape((tok, width), F32),
            shape((rows, n * across), F32),
            shape((8, width // n), F32),
            shape(second.shape, BF16),
            shape(second.shape, BF16),
            shape((3, width, units), BF16),
            shape((tok, width), BF16),
            shape((rows, width), F32),
            shape(router.shape, F32),
        ],
        in_specs=[VMEM] * 11 + [ANY] * 6,
        out_specs=[VMEM] * 3 + [ANY] * 3 + [VMEM] * 3,
        scratch_shapes=[
            pltpu.VMEM((max(f - 1, 1), n, rows, across), BF16),
            pltpu.VMEM((n, rows, across), BF16),
            pltpu.VMEM((n, rows, across), BF16),
            pltpu.VMEM((8, width), F32),
            pltpu.VMEM((n, 8, width // n), F32),
            pltpu.VMEM((f, 8, width // n), F32),
            pltpu.VMEM((2, 3, 2 * width // n, units), BF16),
            pltpu.VMEM((2, 2, max(f - 1, 1), 2 * width // n, units), BF16),
            pltpu.VMEM(proj.shape, BF16),
            pltpu.VMEM((max(f - 1, 1),) + proj.shape[1:], BF16),
            pltpu.VMEM((f,) + router.shape, BF16),
            pltpu.VMEM(rows_in.shape, BF16),
            pltpu.VMEM(rows_in.shape, BF16),
            pltpu.VMEM((rows_in.shape[0], units), BF16),
            pltpu.VMEM(d_up.shape, BF16),
            pltpu.VMEM(inner_in.shape, BF16),
        ]
        + Fold.buffers(n, tok, width)
        + Fold.semaphores(n)
        + Stored.buffers(n, tok, width)
        + Stored.semaphores(n)
        + [kind((5, f)), kind((5, f)), kind((2, n)), kind((2, n)), kind((2,)), kind((2, 3))]
        + [kind((5,))]
        + [kind((2, n // 2, max(f - 1, 1))), kind((2, n // 2, max(f - 1, 1)))],
        compiler_params=pltpu.CompilerParams(
            collective_id=4, has_side_effects=True, vmem_limit_bytes=67_000_000
        ),
        name="last_stage",
    )(
        d_mixed, w_head, qkv_part, tokens, gain, d_middle, gain_two, gain_head,
        middle, proj, router, moe_part, rows_in, d_in, d_gate, d_up, inner_in
    )


def angles_of(n, tok, head_size):
    half = head_size // 2
    freqs = 10000.0 ** (-jnp.arange(half, dtype=F32) / half)
    inside = jnp.arange(tok, dtype=jnp.int32)
    starts = jnp.arange(n, dtype=jnp.int32) * tok
    angles = jnp.concatenate([inside, starts]).astype(F32)[:, None] * freqs[None, :]
    both = jnp.stack([jnp.cos(angles), jnp.sin(angles)])
    both = jnp.concatenate([both, both], -1)
    return both[:, :tok], both[:, tok:, None, :]


def shards(n, f, inputs, routes, w_qkv, w_out, w_router, norm_gains, w_gate, w_up, w_down, cotangent):
    tokens_low = inputs[0]
    upstream_low = cotangent[0]
    local_routes = routes[0].T
    mine = lax.axis_index("fsdp")
    tok, width = tokens_low.shape
    length = tok * n
    head_size = width // HEADS
    across = 3 * head_size
    rows = w_qkv.shape[0]
    experts = n * w_gate.shape[0]
    capacity = min(tok, 5 * tok * TOPK // (4 * experts))
    factor = head_size ** (-0.5)

    small = jnp.concatenate([w_router, norm_gains], 1)
    small = jnp.pad(small, ((0, 0), (0, 128 - small.shape[1])))
    (
        hidden_one,
        mixed,
        w_head,
        router,
        gains,
        routes_all,
        gate_near,
        up_near,
        w_out_all,
    ) = first_gather(n, f, tokens_low, w_qkv, small, local_routes, w_out, w_gate[0], w_up[0])
    w_out_all = w_out_all.reshape(width, width)
    hidden_one = hidden_one.reshape(length, width)
    w_head = w_head.reshape(width, across)
    tables, starts = angles_of(n, tok, head_size)
    (
        queries,
        keys,
        values,
        attended,
        exact,
        sums,
        squares,
        upstream_all,
        by_token,
        up_rest,
        down_near,
    ) = attention(n, f, mixed, tables, starts, gains, upstream_low, w_up[0], w_down[0], factor)
    halves = [w_gate[0], w_down[0], w_up[0]]
    for j in range(f - 1):
        halves += [gate_near[j], down_near[j], up_near[j], up_rest[j]]

    (
        d_middle,
        middle,
        d_attn,
        d_attended,
        d_logits_all,
        gain_two,
        own_hidden,
        expert_rows,
        d_produced,
        inner,
        d_gate,
        d_up,
        moe_part,
    ) = core_stage(
        n,
        f,
        by_token,
        w_out_all,
        tokens_low,
        upstream_low,
        gains[3:4],
        router,
        local_routes,
        routes_all,
        upstream_all,
        halves,
    )
    flat = n * capacity
    units = w_gate.shape[2]
    expert_rows = expert_rows.reshape(flat, width)
    d_produced = d_produced.reshape(flat, width)
    inner, d_gate, d_up = (v.reshape(flat, f * units) for v in (inner, d_gate, d_up))
    d_mixed, gain_head, qkv_part, proj, router_part, first, second = attention_back(
        n,
        f,
        queries,
        keys,
        values,
        d_attended,
        sums,
        exact,
        mixed,
        tables,
        starts,
        gains,
        squares,
        d_attn,
        attended,
        own_hidden,
        d_logits_all,
        expert_rows,
        d_gate,
        d_up,
        hidden_one,
        rows,
        factor,
    )
    (
        grad_inputs,
        grad_qkv,
        gains_own,
        second_rest,
        third,
        grads_own,
        result,
        grad_proj,
        grad_router,
    ) = last_stage(
        n,
        f,
        d_mixed.reshape(n, tok, across),
        w_head,
        qkv_part,
        tokens_low,
        gains[0:1],
        d_middle,
        gain_two,
        gain_head,
        middle,
        proj.reshape(f, rows, width),
        router_part,
        moe_part,
        expert_rows,
        d_produced,
        d_gate,
        d_up,
        inner,
        second,
    )
    grad_router = lax.dynamic_slice_in_dim(grad_router, mine * rows, rows, 1).T
    split = EARLY * (width // (n // 2))
    grads = []
    for which in range(3):
        total = grads_own[which].astype(F32)
        for j in range(f - 1):
            if which == 1:
                late = jnp.arange(width)[:, None] >= split
                part = jnp.where(late, second_rest[j], second[j])
            else:
                part = (first if which == 0 else third)[j]
            total = total + part.astype(F32)
        grads.append(total[None])
    gains_out = jnp.stack([gains_own[0], gains_own[2], gains_own[3], gains_own[1]], 1)
    grad_gains = lax.dynamic_slice_in_dim(gains_out, mine * rows, rows, 0)
    return (
        result[None],
        grad_inputs[None],
        grad_qkv,
        grad_proj,
        grad_router,
        grad_gains,
        *grads,
    )


def solution(mesh):
    tokens = P("fsdp", "seq", None)
    split = P(("seq", "fsdp"), None)
    expert = P("seq", None, "fsdp")
    return jax.shard_map(
        partial(shards, mesh.shape["seq"], mesh.shape["fsdp"]),
        mesh=mesh,
        in_specs=(tokens, tokens, split, split, split, split, expert, expert, expert, tokens),
        out_specs=(tokens, tokens, split, split, split, split, expert, expert, expert),
        check_vma=False,
    )
```
